256 devices in a mesh: curve: 64 (over y, z, core), sub: 4 (over x).
Axes of the slice: x: 4, y: 4, z: 8, core: 2. Of those that a mesh axis runs over, the one named last changes fastest.
Arguments:
- forcing: float32 [12, 6144, 1024], P(None, 'curve', 'sub'), may hold values from -10 to 10
- metric: float32 [6144, 1024], P('curve', 'sub'), may hold values from 0.25 to 4
- jacobian: float32 [6144, 1024], P('curve', 'sub'), may hold values from 0.5 to 2
- mode_scale: float32 [12], replicated, may hold values from 0.1 to 10
Outputs:
- solution: float32 [12, 6144, 1024], P(None, 'curve', 'sub')
- residual: float32 [12, 6144, 1024], P(None, 'curve', 'sub')
The draws below stay inside these ranges and needn't reach their ends.
All inputs are finite; a program needn't handle non-finite values.
Results may differ from the reference program's by a relative error of at most 0.0003.
Values sent between devices are 32-bit elements; how exact they have to be, the bound alone decides.
A program may use at most 64 MiB of HBM per device.

```python
import math
import jax
import jax.numpy as jnp
import numpy as np
from jax import lax

NP = 4
MODES = 12
ITERS = 3
EBX = 24
NX = 6144
NY = 1024


def draw_forcing(key, part):
    noise_key, scale_key = jax.random.split(jax.random.fold_in(key, 7))
    regions = NX // (NP * EBX)
    region_scale = jnp.exp(jax.random.uniform(scale_key, (regions,), jnp.float32, math.log(0.3), math.log(3.0)))
    per_row = jnp.repeat(region_scale, NP * EBX)
    base = jax.random.normal(noise_key, (MODES, NX, NY), jnp.float32)
    return jnp.clip(base * per_row[None, :, None], -10.0, 10.0)


def block_scale(key, extent, cuts, low, high):
    level, own = 1.0, jax.random.fold_in(key, 6)
    for axis_at, blocks in cuts:
        steps = jnp.exp(jax.random.uniform(jax.random.fold_in(own, axis_at), (blocks,), jnp.float32, low / len(cuts), high / len(cuts)))
        level = level * jnp.repeat(steps, extent[axis_at] // blocks).reshape([-1 if axis == axis_at else 1 for axis in range(len(extent))])
    return level


def setup_inputs(seed: int = 0) -> dict:
    key_list = jax.random.split(jax.random.key(seed), 5)
    forcing = draw_forcing(jax.random.fold_in(key_list[4], 71), 0)
    metric = jnp.clip(jnp.exp(math.log(4.0) - 2.7725887 * jax.random.uniform(key_list[1], (NX, NY), jnp.float32) ** block_scale(key_list[1], (NX, NY), ((0, 64), (1, 4)), -0.2, 0.2)), 0.25, 4.0)
    jacobian = jnp.clip(jnp.exp(math.log(2.0) - 1.3862944 * jax.random.uniform(key_list[2], (NX, NY), jnp.float32) ** block_scale(key_list[2], (NX, NY), ((0, 64), (1, 4)), -0.2, 0.2)), 0.5, 2.0)
    mode_scale = jnp.clip(jnp.exp(jax.random.uniform(key_list[3], (MODES,), jnp.float32, math.log(0.1), math.log(10.0))), 0.1, 10.0)
    return {"forcing": forcing, "metric": metric, "jacobian": jacobian, "mode_scale": mode_scale}


def gll_tables():
    points = np.array([-1.0, -1.0 / math.sqrt(5.0), 1.0 / math.sqrt(5.0), 1.0])
    weights = np.array([1.0 / 6.0, 5.0 / 6.0, 5.0 / 6.0, 1.0 / 6.0])
    factor = np.array([np.prod([points[j] - points[m] for m in range(4) if m != j]) for j in range(4)])
    slopes = np.zeros((4, 4))
    for i in range(4):
        for j in range(4):
            if i != j:
                slopes[i, j] = factor[i] / (factor[j] * (points[i] - points[j]))
        slopes[i, i] = sum((1.0 / (points[i] - points[m]) for m in range(4) if m != i))
    return (slopes, weights)

def line_tables(count):
    phase = jnp.arange(count, dtype=jnp.int32) % 4
    on_edge = (phase == 0) | (phase == 3)
    line_w = jnp.where(on_edge, jnp.float32(1.0 / 6.0), jnp.float32(5.0 / 6.0))
    line_mult = jnp.where(on_edge, jnp.float32(2.0), jnp.float32(1.0))
    return (line_w, line_mult)

def assemble(values):
    for axis_dim in (0, 1):
        phase = lax.broadcasted_iota(jnp.int32, values.shape, axis_dim) % 4
        values = values + jnp.where(phase == 3, jnp.roll(values, -1, axis_dim), 0.0) + jnp.where(phase == 0, jnp.roll(values, 1, axis_dim), 0.0)
    return values

def apply_local(values, scale, slopes, mass_w, flux_w):
    row_count, col_count = values.shape
    shape4 = (row_count // 4, 4, col_count // 4, 4)
    blocks = values.reshape(shape4)
    hp = lax.Precision.HIGHEST
    grad_x = jnp.einsum('ak,xkyb->xayb', slopes, blocks, precision=hp)
    grad_y = jnp.einsum('bk,xayk->xayb', slopes, blocks, precision=hp)
    weight4 = flux_w.reshape(shape4)
    lap = jnp.einsum('ka,xkyb->xayb', slopes, weight4 * grad_x, precision=hp) + jnp.einsum('kb,xayk->xayb', slopes, weight4 * grad_y, precision=hp)
    return mass_w * values + scale * lap.reshape(row_count, col_count)

def diag_terms(flux_w, slopes):
    row_count, col_count = flux_w.shape
    shape4 = (row_count // 4, 4, col_count // 4, 4)
    weight4 = flux_w.reshape(shape4)
    hp = lax.Precision.HIGHEST
    squared = slopes * slopes
    terms = jnp.einsum('ka,xkyb->xayb', squared, weight4, precision=hp) + jnp.einsum('kb,xayk->xayb', squared, weight4, precision=hp)
    return terms.reshape(row_count, col_count)

def reference(forcing, metric, jacobian, mode_scale):
    slopes = jnp.asarray(gll_tables()[0], jnp.float32)
    row_w, row_mult = line_tables(metric.shape[0])
    col_w, col_mult = line_tables(metric.shape[1])
    grid_w = row_w[:, None] * col_w[None, :]
    inv_count = 1.0 / (row_mult[:, None] * col_mult[None, :])
    mass_w = jacobian * grid_w
    flux_w = metric * grid_w
    mass_diag = assemble(mass_w)
    lap_diag = assemble(diag_terms(flux_w, slopes))

    def solve_mode(member):
        source, scale = member
        rhs = assemble(source * mass_w)
        precond = mass_diag + scale * lap_diag
        solution = jnp.zeros_like(rhs)
        residual = rhs
        zvec = residual / precond
        direction = zvec
        rho_now = jnp.sum(residual * zvec * inv_count)
        for iteration in range(ITERS):
            image = assemble(apply_local(direction, scale, slopes, mass_w, flux_w))
            step_len = rho_now / jnp.sum(direction * image * inv_count)
            solution = solution + step_len * direction
            residual = residual - step_len * image
            zvec = residual / precond
            rho_next = jnp.sum(residual * zvec * inv_count)
            direction = zvec + rho_next / rho_now * direction
            rho_now = rho_next
        return (solution, residual)
    solution, residual = lax.map(solve_mode, (forcing, mode_scale))
    return (solution, residual)
```

```python
import functools
import math

import jax
import jax.numpy as jnp
import numpy as np
from jax import lax
from jax.experimental import pallas as pl
from jax.experimental.pallas import tpu as pltpu
from jax.sharding import PartitionSpec as P

ITERS = 3
GROUPS = 2
UNROLL = True
MESH = pl.DeviceIdType.MESH
LANES = 128
f32 = jnp.float32
bf16 = jnp.bfloat16


def gll_tables():
    points = np.array([-1.0, -1.0 / math.sqrt(5.0), 1.0 / math.sqrt(5.0), 1.0])
    weights = np.array([1.0 / 6.0, 5.0 / 6.0, 5.0 / 6.0, 1.0 / 6.0])
    factor = np.array(
        [np.prod([points[j] - points[m] for m in range(4) if m != j]) for j in range(4)]
    )
    slopes = np.zeros((4, 4))
    for i in range(4):
        for j in range(4):
            if i != j:
                slopes[i, j] = factor[i] / (factor[j] * (points[i] - points[j]))
        slopes[i, i] = sum((1.0 / (points[i] - points[m]) for m in range(4) if m != i))
    return (slopes, weights)


SLOPES, WEIGHTS = gll_tables()


def combo(coefs, parts):
    total = None
    for c, v in zip(coefs, parts):
        if abs(c) < 1e-12:
            continue
        term = v * f32(c)
        total = term if total is None else total + term
    return total


PRODUCTS = 6
FIELD = 16


def planes(nc, ns):
    depth = 8 if nc % 16 == 0 else 2
    return nc // (2 * depth), depth, 2, ns


def kernel(
    nc, ns, modes, groups,
    scale_hbm, forcing_ref, metric_ref, jac_ref, grad_hbm, div_hbm,
    r0, r1, r2, u2, invp, coef,
    z, w, mass, flux, zcat, gout, sums,
    row_tx, row_rx, col_tx, col_rx, cor_rx, near_tx, near_rx, far_tx, far_rx,
    source, factors, grad_ref, div_ref, scale_ref,
    htx_sem, hrx_sem, atx_sem, arx_sem, in_sem, table_sem,
):
    rows, cols = metric_ref.shape
    q = rows // 4
    half = cols - LANES
    tiles = cols // LANES
    per = modes // groups
    loads, sources = [], []
    for c in range(tiles):
        cut = pl.ds(c * LANES, LANES)
        loads += [
            pltpu.make_async_copy(jac_ref.at[:, cut], factors.at[0, c], in_sem.at[0, c]),
            pltpu.make_async_copy(metric_ref.at[:, cut], factors.at[1, c], in_sem.at[1, c]),
        ]
        sources.append(
            pltpu.make_async_copy(forcing_ref.at[:, :, cut], source.at[c], in_sem.at[2, c]))
    div_load = pltpu.make_async_copy(div_hbm, div_ref, table_sem.at[0])
    grad_load = pltpu.make_async_copy(grad_hbm, grad_ref, table_sem.at[1])
    scale_load = pltpu.make_async_copy(scale_hbm, scale_ref, table_sem.at[2])
    for copy in loads + sources + [div_load, scale_load, grad_load]:
        copy.start()

    me_c, me_s = lax.axis_index("curve"), lax.axis_index("sub")
    up, down = lax.rem(me_c + nc - 1, nc), lax.rem(me_c + 1, nc)
    left, right = lax.rem(me_s + ns - 1, ns), lax.rem(me_s + 1, ns)

    ny, nz, nk, nx = planes(nc, ns)
    core, chip = lax.rem(me_c, nk), me_c // nk
    at_z, at_y = lax.rem(chip, nz), chip // nz
    subs = [me_s if dx == 0 else lax.rem(me_s + dx, nx) for dx in range(nx)]
    near, far = [], []
    for dy in range(ny):
        y = at_y if dy == 0 else lax.rem(at_y + dy, ny)
        for dk in range(nk):
            k = core if dk == 0 else 1 - core
            c = (y * nz + at_z) * nk + k
            near += [(c, subs[dx]) for dx in range(nx)]
    for dz in range(nz):
        far.append(((at_y * nz + lax.rem(at_z + dz, nz)) * nk + core, me_s))
    near, far = near[1:], far[1:]

    barrier = pltpu.get_barrier_semaphore()
    greeted = [
        (up, left), (up, right), (down, left), (down, right), (up, me_s), (down, me_s),
        (me_c, left), (me_c, right)] + near + far
    for where in greeted:
        pl.semaphore_signal(barrier, inc=1, device_id=where, device_id_type=MESH)

    lane_full = lax.broadcasted_iota(jnp.int32, (q, cols), 1)
    lane = lax.broadcasted_iota(jnp.int32, (q, LANES), 1)
    row_at = lax.broadcasted_iota(jnp.int32, (q, cols), 0)
    phase = lane_full % 4
    on_edge = (phase == 0) | (phase == 3)
    take_next = (phase == 3) & (lane_full != cols - 1)
    take_prev = (phase == 0) & (lane_full != 0)

    def load(ref, m):
        return [ref[m, p * q:(p + 1) * q, :] for p in range(4)]

    def save(ref, m, parts):
        for p in range(4):
            ref[m, p * q:(p + 1) * q, :] = parts[p]

    def load2(ref):
        return [ref[p * q:(p + 1) * q, :] for p in range(4)]

    def pack(k, m, slot, h, tops):
        lo, hi = tops
        row_tx[k, 0, pl.ds(slot, 1), :] = h[0][0:1, :]
        row_tx[k, 1, pl.ds(slot, 1), :] = h[3][q - 1:q, :]
        t0 = h[0] + jnp.where(row_at == 0, 0.0, pltpu.roll(h[3], 1, 0))
        t3 = h[3] + jnp.where(row_at == q - 1, 0.0, pltpu.roll(h[0], q - 1, 0))
        t = [t0, h[1], h[2], t3]
        save(w, m, t)
        for p in range(4):
            at = 4 * slot + p
            lo = jnp.where(lane == at, pltpu.roll(t[p][:, :LANES], at, 1), lo)
            hi = jnp.where(lane == at, pltpu.roll(t[p][:, half:], at + 1, 1), hi)
        return lo, hi

    def halo_copies(k):
        plan = [
            (col_tx.at[k, 0, pl.ds(0, 1)], cor_rx.at[k, 3], (up, left)),
            (col_tx.at[k, 1, pl.ds(0, 1)], cor_rx.at[k, 2], (up, right)),
            (col_tx.at[k, 0, pl.ds(q - 1, 1)], cor_rx.at[k, 1], (down, left)),
            (col_tx.at[k, 1, pl.ds(q - 1, 1)], cor_rx.at[k, 0], (down, right)),
            (row_tx.at[k, 0], row_rx.at[k, 1], (up, me_s)),
            (row_tx.at[k, 1], row_rx.at[k, 0], (down, me_s)),
            (col_tx.at[k, 0], col_rx.at[k, 1], (me_c, left)),
            (col_tx.at[k, 1], col_rx.at[k, 0], (me_c, right)),
        ]
        return [
            pltpu.make_async_remote_copy(
                src_ref=src, dst_ref=dst, send_sem=htx_sem.at[k, e], recv_sem=hrx_sem.at[k, e],
                device_id=where, device_id_type=MESH)
            for e, (src, dst, where) in enumerate(plan)
        ]

    def send(k, tops):
        col_tx[k, 0], col_tx[k, 1] = tops
        for copy in halo_copies(k):
            copy.start()

    def arrive(k):
        for copy in halo_copies(k):
            copy.wait_recv()
        ph = lax.broadcasted_iota(jnp.int32, (1, LANES), 1) % 4
        edge_row = lax.broadcasted_iota(jnp.int32, (q, LANES), 0)
        merged = []
        for side in range(2):
            above, below = cor_rx[k, side], cor_rx[k, 2 + side]
            above = jnp.where(ph == 0, pltpu.roll(above, LANES - 3, 1), 0.0)
            below = jnp.where(ph == 3, pltpu.roll(below, 3, 1), 0.0)
            c = col_rx[k, side]
            c = c + jnp.where(edge_row == 0, above, 0.0) + jnp.where(edge_row == q - 1, below, 0.0)
            merged.append(c)
        return merged

    def assembled(k, m, slot, merged):
        t = load(w, m)
        t[0] = t[0] + jnp.where(row_at == 0, row_rx[k, 0, pl.ds(slot, 1), :], 0.0)
        t[3] = t[3] + jnp.where(row_at == q - 1, row_rx[k, 1, pl.ds(slot, 1), :], 0.0)
        out = []
        for p in range(4):
            at = 4 * slot + p
            c = t[p] + jnp.where(
                take_next, pltpu.roll(t[p], cols - 1, 1),
                jnp.where(take_prev, pltpu.roll(t[p], 1, 1), 0.0))
            a = jnp.where(lane == 0, pltpu.roll(merged[0], LANES - at, 1), 0.0)
            b = jnp.where(lane == LANES - 1, pltpu.roll(merged[1], LANES - 1 - at, 1), 0.0)
            pieces = [c[:, e * LANES:(e + 1) * LANES] for e in range(tiles)]
            pieces[0] = pieces[0] + a
            pieces[-1] = pieces[-1] + b
            out.append(jnp.concatenate(pieces, axis=1))
        return out

    edge_w, mid_w = f32(1.0 / 6.0), f32(5.0 / 6.0)
    col_w = jnp.where(on_edge, edge_w, mid_w)
    mw, fw = [], []
    for copy in loads:
        copy.wait()
    for p in range(4):
        grid_w = col_w * (edge_w if p in (0, 3) else mid_w)
        mw.append(strided([factors.at[0, c] for c in range(tiles)], p, q) * grid_w)
        fw.append(strided([factors.at[1, c] for c in range(tiles)], p, q) * grid_w)
        mass[p * q:(p + 1) * q, :] = mw[p]
        flux[p * q:(p + 1) * q, :] = fw[p]
    zero = jnp.zeros((q, LANES), f32)
    tops = pack(0, modes, per, mw, (zero, zero))
    div_load.wait()
    table = div_ref[:cols, :].astype(f32) + div_ref[2 * cols:, :].astype(f32)
    by_cols = jnp.dot(flux[...], table * table, precision=lax.Precision.HIGHEST,
                      preferred_element_type=f32)
    squared = SLOPES * SLOPES
    lap = [combo(squared[:, a], fw) + by_cols[a * q:(a + 1) * q, :] for a in range(4)]
    tops = pack(0, modes + 1, per + 1, lap, tops)
    for copy in sources:
        copy.wait()
    for g in range(groups):

        def start_body(slot, carry, g=g):
            m = g * per + slot
            h = [strided([source.at[c, m] for c in range(tiles)], p, q)
                 * mass[p * q:(p + 1) * q, :] for p in range(4)]
            return pack(g, m, slot, h, carry)

        tops = lax.fori_loop(0, per, start_body, tops if g == 0 else (zero, zero), unroll=UNROLL)
        if g == 0:
            pl.semaphore_wait(barrier, len(greeted))
        send(g, tops)
    scale_load.wait()
    grad_load.wait()

    def fill(g, slot, parts):
        v = jnp.concatenate(parts, axis=0)
        top = v.astype(bf16)
        at = pl.ds(pl.multiple_of(slot * rows, rows), rows)
        zcat[g, at, :cols] = top
        zcat[g, at, cols:] = (v - top.astype(f32)).astype(bf16)

    def multiply(g, table_ref):
        gout[...] = (
            jnp.dot(zcat[g], table_ref[:2 * cols, :], preferred_element_type=f32)
            + jnp.dot(zcat[g, :, :cols], table_ref[2 * cols:, :], preferred_element_type=f32))

    def total_rows(parts):
        return jnp.sum((parts[0] + parts[3]) + (parts[1] + parts[2]), axis=0, keepdims=True)

    def shared_rows(parts):
        line = (parts[0] + parts[3]) * 0.5 + (parts[1] + parts[2])
        return jnp.sum(jnp.where(on_edge, line * 0.5, line), axis=0, keepdims=True)

    def finish(g, k, base):
        multiply(g, div_ref)

        def third(slot, carry):
            m = base + slot
            h = [u + gout[pl.ds(pl.multiple_of(slot * rows + p * q, q), q), :]
                 for p, u in enumerate(load(w, m))]
            if k < ITERS - 1:
                zh = [u * v for u, v in zip(load(z, m), h)]
                sums[2 * k + 1, pl.ds(m, 1), :] = total_rows(zh)
            return pack((k + 1) * groups + g, m, slot, h, carry)

        tops = lax.fori_loop(0, per, third, (zero, zero), unroll=UNROLL)
        send((k + 1) * groups + g, tops)

    for it in range(ITERS):
        for g in range(groups):
            base = g * per
            k = it * groups + g
            merged = arrive(k)
            if it == 0 and g == 0:
                for e in range(2):
                    save(w, modes + e, assembled(k, modes + e, per + e, merged))

            def first(slot, carry, it=it, g=g, k=k, base=base, merged=merged):
                m = base + slot
                uu = assembled(k, m, slot, merged)
                if it == 0:
                    rr = uu
                    inv = [1.0 / (u + scale_ref[m] * v)
                           for u, v in zip(load(w, modes), load(w, modes + 1))]
                    save(invp, m, inv)
                    save(r0, m, rr)
                elif it == 1:
                    rr = [u - v for u, v in zip(uu, load(r0, m))]
                    inv = load(invp, m)
                    save(r1, m, rr)
                else:
                    rr = [2.0 * (u - v) - s for u, v, s in zip(uu, load(r1, m), load(r0, m))]
                    inv = load(invp, m)
                    save(r2, m, rr)
                zz = [u * v for u, v in zip(rr, inv)]
                fill(g, slot, zz)
                sums[2 * it, pl.ds(m, 1), :] = shared_rows([u * v for u, v in zip(uu, zz)])
                f = load2(flux)
                gx = [combo(SLOPES[a], zz) for a in range(4)]
                fg = [f[a] * gx[a] * scale_ref[m] for a in range(4)]
                mz = [u * v for u, v in zip(load2(mass), zz)]
                if it < ITERS - 1:
                    save(z, m, zz)
                else:
                    sums[2 * it + 1, pl.ds(m, 1), :] = total_rows(
                        [u * v + s * t for u, v, s, t in zip(mz, zz, fg, gx)])
                save(w, m, [mz[a] + combo(SLOPES[:, a], fg) for a in range(4)])
                return carry

            lax.fori_loop(0, per, first, 0, unroll=UNROLL)
            multiply(g, grad_ref)

            def second(slot, carry, it=it, g=g, base=base):
                m = base + slot
                grad = [gout[pl.ds(pl.multiple_of(slot * rows + p * q, q), q), :]
                        for p in range(4)]
                fy = [u * v * scale_ref[m] for u, v in zip(load2(flux), grad)]
                if it == ITERS - 1:
                    e = 2 * it + 1
                    sums[e, pl.ds(m, 1), :] = sums[e, pl.ds(m, 1), :] + total_rows(
                        [u * v for u, v in zip(fy, grad)])
                fill(g, slot, fy)
                return carry

            lax.fori_loop(0, per, second, 0, unroll=UNROLL)
            if it < ITERS - 1:
                finish(g, it, base)

    high = lax.broadcasted_iota(jnp.int32, (FIELD, LANES), 0)
    wide = lax.broadcasted_iota(jnp.int32, (FIELD, LANES), 1)
    picks = [(wide == e * FIELD + high) & (high < modes) for e in range(PRODUCTS)]
    spread = jnp.zeros((FIELD, LANES), f32)
    for e in range(PRODUCTS):
        part = jnp.sum(sums[e], axis=1, keepdims=True)
        spread = spread + jnp.where(picks[e], part, 0.0)
    line = jnp.sum(spread, axis=0, keepdims=True)

    def share(stage, line, tx, rx, peers):
        tx[...] = line
        rx[0] = line
        for j, where in enumerate(peers):
            pltpu.make_async_remote_copy(
                src_ref=tx, dst_ref=rx.at[j + 1], send_sem=atx_sem.at[stage],
                recv_sem=arx_sem.at[stage], device_id=where, device_id_type=MESH).start()

    def gather(stage, rx):
        got = rx.at[pl.ds(1, rx.shape[0] - 1)]
        pltpu.make_async_copy(got, got, arx_sem.at[stage]).wait()
        return jnp.sum(rx[...], axis=0)

    share(0, line, near_tx, near_rx, near)
    for g in range(groups):
        finish(g, ITERS - 1, g * per)
    share(1, gather(0, near_rx), far_tx, far_rx, far)
    for g in range(groups):
        k = ITERS * groups + g
        merged = arrive(k)

        def last(slot, carry, g=g, k=k, merged=merged):
            m = g * per + slot
            save(u2, m, assembled(k, m, slot, merged))
            return carry

        lax.fori_loop(0, per, last, 0, unroll=UNROLL)

    total = gather(1, far_rx)
    pad = (high[:, :1] >= modes).astype(f32)
    n0, p00, p01, p11, p12, p22 = [
        jnp.broadcast_to(
            jnp.sum(jnp.where(pick, total, 0.0), axis=1, keepdims=True), (FIELD, LANES))
        for pick in picks]
    pad = jnp.broadcast_to(pad, (FIELD, LANES))
    p00, p11, p22 = p00 + pad, p11 + pad, p22 + 2.0 * pad
    b0 = n0
    b1 = p00 - n0
    b2 = 2.0 * (p01 - b1) - n0
    p02 = 2.0 * p11 - p00
    i0 = 1.0 / p00
    l1, l2 = p01 * i0, p02 * i0
    d1 = p11 - l1 * p01
    t2 = p12 - l2 * p01
    i1 = 1.0 / d1
    l3 = t2 * i1
    d2 = p22 - l2 * p02 - l3 * t2
    y1 = b1 - l1 * b0
    y2 = b2 - l2 * b0 - l3 * y1
    c2 = y2 / d2
    c1 = y1 * i1 - l3 * c2
    c0 = b0 * i0 - l1 * c1 - l2 * c2
    for e, c in enumerate((c0, c1, c2, 1.0 - c0 - 0.5 * c1, c0 + c1, 0.5 * c1)):
        coef[e] = c

    for k in range((ITERS + 1) * groups):
        for copy in halo_copies(k):
            copy.wait_send()
    for stage, rx in enumerate((near_rx, far_rx)):
        sent = rx.at[pl.ds(1, rx.shape[0] - 1)]
        pltpu.make_async_copy(sent, sent, atx_sem.at[stage]).wait()


def node_order(r0, r1, r2, u2, invp, coef, sol_ref, res_ref, sol_buf, res_buf, sem):
    modes, rows, cols = r0.shape
    q, tiles = rows // 4, cols // LANES

    def stores(m):
        return [
            pltpu.make_async_copy(
                buf.at[c, m], out.at[m, :, pl.ds(c * LANES, LANES)], sem.at[k, c, m])
            for k, (buf, out) in enumerate(((sol_buf, sol_ref), (res_buf, res_ref)))
            for c in range(tiles)
        ]

    def body(m, carry):
        c0, c1, c2, e0, e1, e2 = [coef[e, pl.ds(m, 1), :] for e in range(6)]
        for c in range(tiles):
            for p in range(4):
                at = (m, slice(p * q, (p + 1) * q), slice(c * LANES, (c + 1) * LANES))
                a0, a1, a2 = r0[at], r1[at], r2[at]
                sol_buf[c, m, pl.ds(p, q, stride=4), :] = invp[at] * (c0 * a0 + c1 * a1 + c2 * a2)
                res_buf[c, m, pl.ds(p, q, stride=4), :] = (
                    e0 * a0 - e1 * a1 - e2 * a2 - c2 * u2[at])
        for copy in stores(m):
            copy.start()
        return carry

    lax.fori_loop(0, modes, body, 0)

    def drain(m, carry):
        for copy in stores(m):
            copy.wait()
        return carry

    lax.fori_loop(0, modes, drain, 0)


def strided(refs, p, q):
    return jnp.concatenate([ref[pl.ds(p, q, stride=4), :] for ref in refs], axis=1)


def stack_table(table):
    top = table.astype(bf16)
    low = (table - top.astype(np.float32)).astype(bf16)
    return np.concatenate([top, top, low], axis=0)


def shards(nc, ns, forcing, metric, jacobian, mode_scale):
    modes, rows, cols = forcing.shape
    block = np.kron(np.eye(cols // 4), SLOPES).astype(np.float32)
    grad, div = stack_table(block.T), stack_table(block)
    q, tiles = rows // 4, cols // LANES
    groups = GROUPS if modes % GROUPS == 0 else 1
    per = modes // groups
    slots = -(-(per + 2) // 8) * 8
    vm = pl.BlockSpec(memory_space=pltpu.VMEM)
    hbm = pl.BlockSpec(memory_space=pltpu.HBM)
    rounds = (ITERS + 1) * groups
    ny, nz, nk, nx = planes(nc, ns)
    field = pltpu.VMEM((modes, rows, cols), f32)
    split = pltpu.VMEM((tiles, modes, rows, LANES), f32)
    table = pltpu.VMEM(grad.shape, bf16)
    line = pltpu.VMEM((1, LANES), f32)
    shape = jax.ShapeDtypeStruct(forcing.shape, f32)
    kept = pl.pallas_call(
        functools.partial(kernel, nc, ns, modes, groups),
        out_shape=[shape] * 5 + [jax.ShapeDtypeStruct((6, FIELD, LANES), f32)],
        in_specs=[hbm] * 6,
        out_specs=[vm] * 6,
        scratch_shapes=[
            field,
            pltpu.VMEM((modes + 2, rows, cols), f32),
            pltpu.VMEM((rows, cols), f32),
            pltpu.VMEM((rows, cols), f32),
            pltpu.VMEM((groups, per * rows, 2 * cols), bf16),
            pltpu.VMEM((per * rows, cols), f32),
            pltpu.VMEM((PRODUCTS, FIELD, cols), f32),
            pltpu.VMEM((rounds, 2, slots, cols), f32),
            pltpu.VMEM((rounds, 2, slots, cols), f32),
            pltpu.VMEM((rounds, 2, q, LANES), f32),
            pltpu.VMEM((rounds, 2, q, LANES), f32),
            pltpu.VMEM((rounds, 4, 1, LANES), f32),
            line,
            pltpu.VMEM((ny * nk * nx, 1, LANES), f32),
            line,
            pltpu.VMEM((nz, 1, LANES), f32),
            split,
            pltpu.VMEM((2, tiles, rows, LANES), f32),
            table, table,
            pltpu.SMEM((modes,), f32),
            pltpu.SemaphoreType.DMA((rounds, 8)),
            pltpu.SemaphoreType.DMA((rounds, 8)),
            pltpu.SemaphoreType.DMA((2,)),
            pltpu.SemaphoreType.DMA((2,)),
            pltpu.SemaphoreType.DMA((3, tiles)),
            pltpu.SemaphoreType.DMA((3,)),
        ],
        compiler_params=pltpu.CompilerParams(
            collective_id=0, has_side_effects=True, vmem_limit_bytes=41943040),
    )(*[pltpu.with_memory_space_constraint(v, pltpu.HBM) for v in (mode_scale, forcing, metric, jacobian, jnp.asarray(grad), jnp.asarray(div))])
    return pl.pallas_call(
        node_order,
        out_shape=[shape] * 2,
        in_specs=[vm] * 6,
        out_specs=[hbm, hbm],
        scratch_shapes=[split, split, pltpu.SemaphoreType.DMA((2, tiles, modes))],
        compiler_params=pltpu.CompilerParams(vmem_limit_bytes=16 * 1024 * 1024),
    )(*kept)


def solution(mesh):
    placed = (P(None, "curve", "sub"), P("curve", "sub"), P("curve", "sub"), P())
    return jax.shard_map(
        functools.partial(shards, mesh.shape["curve"], mesh.shape["sub"]),
        mesh=mesh,
        in_specs=placed,
        out_specs=(P(None, "curve", "sub"), P(None, "curve", "sub")),
        check_vma=False,
    )
```

```python
import functools
import math

import jax
import jax.numpy as jnp
import numpy as np
from jax import lax
from jax.experimental import pallas as pl
from jax.experimental.pallas import tpu as pltpu
from jax.sharding import PartitionSpec as P

ITERS = 3
GROUPS = 3
UNROLL = True
MESH = pl.DeviceIdType.MESH
LANES = 128
f32 = jnp.float32
bf16 = jnp.bfloat16


def gll_tables():
    points = np.array([-1.0, -1.0 / math.sqrt(5.0), 1.0 / math.sqrt(5.0), 1.0])
    weights = np.array([1.0 / 6.0, 5.0 / 6.0, 5.0 / 6.0, 1.0 / 6.0])
    factor = np.array(
        [np.prod([points[j] - points[m] for m in range(4) if m != j]) for j in range(4)]
    )
    slopes = np.zeros((4, 4))
    for i in range(4):
        for j in range(4):
            if i != j:
                slopes[i, j] = factor[i] / (factor[j] * (points[i] - points[j]))
        slopes[i, i] = sum((1.0 / (points[i] - points[m]) for m in range(4) if m != i))
    return (slopes, weights)


SLOPES, WEIGHTS = gll_tables()


def combo(coefs, parts):
    total = None
    for c, v in zip(coefs, parts):
        if abs(c) < 1e-12:
            continue
        term = v * f32(c)
        total = term if total is None else total + term
    return total


PRODUCTS = 6
FIELD = 16


def planes(nc, ns):
    depth = 8 if nc % 16 == 0 else 2
    return nc // (2 * depth), depth, 2, ns


def kernel(
    nc, ns, modes, groups,
    scale_hbm, forcing_ref, metric_ref, jac_ref, grad_hbm, div_hbm,
    r0, r1, r2, u2, invp, coef,
    z, w, mass, flux, zcat, gout, sums,
    row_tx, row_rx, col_tx, col_rx, cor_rx, near_tx, near_rx, far_tx, far_rx,
    source, factors, grad_ref, div_ref, scale_ref,
    htx_sem, hrx_sem, atx_sem, arx_sem, in_sem, table_sem,
):
    rows, cols = metric_ref.shape
    q = rows // 4
    half = cols - LANES
    tiles = cols // LANES
    per = modes // groups
    loads, sources = [], []
    for c in range(tiles):
        cut = pl.ds(c * LANES, LANES)
        loads += [
            pltpu.make_async_copy(jac_ref.at[:, cut], factors.at[0, c], in_sem.at[0, c]),
            pltpu.make_async_copy(metric_ref.at[:, cut], factors.at[1, c], in_sem.at[1, c]),
        ]
        sources.append(
            pltpu.make_async_copy(forcing_ref.at[:, :, cut], source.at[c], in_sem.at[2, c]))
    div_load = pltpu.make_async_copy(div_hbm, div_ref, table_sem.at[0])
    grad_load = pltpu.make_async_copy(grad_hbm, grad_ref, table_sem.at[1])
    scale_load = pltpu.make_async_copy(scale_hbm, scale_ref, table_sem.at[2])
    for copy in loads + sources + [div_load, scale_load, grad_load]:
        copy.start()

    me_c, me_s = lax.axis_index("curve"), lax.axis_index("sub")
    up, down = lax.rem(me_c + nc - 1, nc), lax.rem(me_c + 1, nc)
    left, right = lax.rem(me_s + ns - 1, ns), lax.rem(me_s + 1, ns)

    ny, nz, nk, nx = planes(nc, ns)
    core, chip = lax.rem(me_c, nk), me_c // nk
    at_z, at_y = lax.rem(chip, nz), chip // nz
    subs = [me_s if dx == 0 else lax.rem(me_s + dx, nx) for dx in range(nx)]
    near, far = [], []
    for dy in range(ny):
        y = at_y if dy == 0 else lax.rem(at_y + dy, ny)
        for dk in range(nk):
            k = core if dk == 0 else 1 - core
            c = (y * nz + at_z) * nk + k
            near += [(c, subs[dx]) for dx in range(nx)]
    for dz in range(nz):
        far.append(((at_y * nz + lax.rem(at_z + dz, nz)) * nk + core, me_s))
    near, far = near[1:], far[1:]

    barrier = pltpu.get_barrier_semaphore()
    greeted = [
        (up, left), (up, right), (down, left), (down, right), (up, me_s), (down, me_s),
        (me_c, left), (me_c, right)] + near + far
    for where in greeted:
        pl.semaphore_signal(barrier, inc=1, device_id=where, device_id_type=MESH)

    lane_full = lax.broadcasted_iota(jnp.int32, (q, cols), 1)
    lane = lax.broadcasted_iota(jnp.int32, (q, LANES), 1)
    row_at = lax.broadcasted_iota(jnp.int32, (q, cols), 0)
    phase = lane_full % 4
    on_edge = (phase == 0) | (phase == 3)
    take_next = (phase == 3) & (lane_full != cols - 1)
    take_prev = (phase == 0) & (lane_full != 0)

    def load(ref, m):
        return [ref[m, p * q:(p + 1) * q, :] for p in range(4)]

    def save(ref, m, parts):
        for p in range(4):
            ref[m, p * q:(p + 1) * q, :] = parts[p]

    def load2(ref):
        return [ref[p * q:(p + 1) * q, :] for p in range(4)]

    def pack(k, m, slot, h, tops):
        lo, hi = tops
        row_tx[k, 0, pl.ds(slot, 1), :] = h[0][0:1, :]
        row_tx[k, 1, pl.ds(slot, 1), :] = h[3][q - 1:q, :]
        t0 = h[0] + jnp.where(row_at == 0, 0.0, pltpu.roll(h[3], 1, 0))
        t3 = h[3] + jnp.where(row_at == q - 1, 0.0, pltpu.roll(h[0], q - 1, 0))
        t = [t0, h[1], h[2], t3]
        save(w, m, t)
        for p in range(4):
            at = 4 * slot + p
            lo = jnp.where(lane == at, pltpu.roll(t[p][:, :LANES], at, 1), lo)
            hi = jnp.where(lane == at, pltpu.roll(t[p][:, half:], at + 1, 1), hi)
        return lo, hi

    def halo_copies(k):
        plan = [
            (col_tx.at[k, 0, pl.ds(0, 1)], cor_rx.at[k, 3], (up, left)),
            (col_tx.at[k, 1, pl.ds(0, 1)], cor_rx.at[k, 2], (up, right)),
            (col_tx.at[k, 0, pl.ds(q - 1, 1)], cor_rx.at[k, 1], (down, left)),
            (col_tx.at[k, 1, pl.ds(q - 1, 1)], cor_rx.at[k, 0], (down, right)),
            (row_tx.at[k, 0], row_rx.at[k, 1], (up, me_s)),
            (row_tx.at[k, 1], row_rx.at[k, 0], (down, me_s)),
            (col_tx.at[k, 0], col_rx.at[k, 1], (me_c, left)),
            (col_tx.at[k, 1], col_rx.at[k, 0], (me_c, right)),
        ]
        return [
            pltpu.make_async_remote_copy(
                src_ref=src, dst_ref=dst, send_sem=htx_sem.at[k, e], recv_sem=hrx_sem.at[k, e],
                device_id=where, device_id_type=MESH)
            for e, (src, dst, where) in enumerate(plan)
        ]

    def send(k, tops):
        col_tx[k, 0], col_tx[k, 1] = tops
        for copy in halo_copies(k):
            copy.start()

    def arrive(k):
        for copy in halo_copies(k):
            copy.wait_recv()
        ph = lax.broadcasted_iota(jnp.int32, (1, LANES), 1) % 4
        edge_row = lax.broadcasted_iota(jnp.int32, (q, LANES), 0)
        merged = []
        for side in range(2):
            above, below = cor_rx[k, side], cor_rx[k, 2 + side]
            above = jnp.where(ph == 0, pltpu.roll(above, LANES - 3, 1), 0.0)
            below = jnp.where(ph == 3, pltpu.roll(below, 3, 1), 0.0)
            c = col_rx[k, side]
            c = c + jnp.where(edge_row == 0, above, 0.0) + jnp.where(edge_row == q - 1, below, 0.0)
            merged.append(c)
        return merged

    def assembled(k, m, slot, merged):
        t = load(w, m)
        t[0] = t[0] + jnp.where(row_at == 0, row_rx[k, 0, pl.ds(slot, 1), :], 0.0)
        t[3] = t[3] + jnp.where(row_at == q - 1, row_rx[k, 1, pl.ds(slot, 1), :], 0.0)
        out = []
        for p in range(4):
            at = 4 * slot + p
            c = t[p] + jnp.where(
                take_next, pltpu.roll(t[p], cols - 1, 1),
                jnp.where(take_prev, pltpu.roll(t[p], 1, 1), 0.0))
            a = jnp.where(lane == 0, pltpu.roll(merged[0], LANES - at, 1), 0.0)
            b = jnp.where(lane == LANES - 1, pltpu.roll(merged[1], LANES - 1 - at, 1), 0.0)
            pieces = [c[:, e * LANES:(e + 1) * LANES] for e in range(tiles)]
            pieces[0] = pieces[0] + a
            pieces[-1] = pieces[-1] + b
            out.append(jnp.concatenate(pieces, axis=1))
        return out

    edge_w, mid_w = f32(1.0 / 6.0), f32(5.0 / 6.0)
    col_w = jnp.where(on_edge, edge_w, mid_w)
    mw, fw = [], []
    for copy in loads:
        copy.wait()
    for p in range(4):
        grid_w = col_w * (edge_w if p in (0, 3) else mid_w)
        mw.append(strided([factors.at[0, c] for c in range(tiles)], p, q) * grid_w)
        fw.append(strided([factors.at[1, c] for c in range(tiles)], p, q) * grid_w)
        mass[p * q:(p + 1) * q, :] = mw[p]
        flux[p * q:(p + 1) * q, :] = fw[p]
    zero = jnp.zeros((q, LANES), f32)
    tops = pack(0, modes, per, mw, (zero, zero))
    div_load.wait()
    table = div_ref[:cols, :].astype(f32) + div_ref[2 * cols:, :].astype(f32)
    by_cols = jnp.dot(flux[...], table * table, precision=lax.Precision.HIGHEST,
                      preferred_element_type=f32)
    squared = SLOPES * SLOPES
    lap = [combo(squared[:, a], fw) + by_cols[a * q:(a + 1) * q, :] for a in range(4)]
    tops = pack(0, modes + 1, per + 1, lap, tops)
    for copy in sources:
        copy.wait()
    for g in range(groups):

        def start_body(slot, carry, g=g):
            m = g * per + slot
            h = [strided([source.at[c, m] for c in range(tiles)], p, q)
                 * mass[p * q:(p + 1) * q, :] for p in range(4)]
            return pack(g, m, slot, h, carry)

        tops = lax.fori_loop(0, per, start_body, tops if g == 0 else (zero, zero), unroll=UNROLL)
        if g == 0:
            pl.semaphore_wait(barrier, len(greeted))
        send(g, tops)
    scale_load.wait()
    grad_load.wait()

    def fill(g, slot, parts):
        v = jnp.concatenate(parts, axis=0)
        top = v.astype(bf16)
        at = pl.ds(pl.multiple_of(slot * rows, rows), rows)
        zcat[g, at, :cols] = top
        zcat[g, at, cols:] = (v - top.astype(f32)).astype(bf16)

    def multiply(g, table_ref):
        gout[...] = (
            jnp.dot(zcat[g], table_ref[:2 * cols, :], preferred_element_type=f32)
            + jnp.dot(zcat[g, :, :cols], table_ref[2 * cols:, :], preferred_element_type=f32))

    def total_rows(parts):
        return jnp.sum((parts[0] + parts[3]) + (parts[1] + parts[2]), axis=0, keepdims=True)

    def shared_rows(parts):
        line = (parts[0] + parts[3]) * 0.5 + (parts[1] + parts[2])
        return jnp.sum(jnp.where(on_edge, line * 0.5, line), axis=0, keepdims=True)

    def finish(g, k, base):
        multiply(g, div_ref)

        def third(slot, carry):
            m = base + slot
            h = [u + gout[pl.ds(pl.multiple_of(slot * rows + p * q, q), q), :]
                 for p, u in enumerate(load(w, m))]
            if k < ITERS - 1:
                zh = [u * v for u, v in zip(load(z, m), h)]
                sums[2 * k + 1, pl.ds(m, 1), :] = total_rows(zh)
            return pack((k + 1) * groups + g, m, slot, h, carry)

        tops = lax.fori_loop(0, per, third, (zero, zero), unroll=UNROLL)
        send((k + 1) * groups + g, tops)

    for it in range(ITERS):
        for g in range(groups):
            base = g * per
            k = it * groups + g
            merged = arrive(k)
            if it == 0 and g == 0:
                for e in range(2):
                    save(w, modes + e, assembled(k, modes + e, per + e, merged))

            def first(slot, carry, it=it, g=g, k=k, base=base, merged=merged):
                m = base + slot
                uu = assembled(k, m, slot, merged)
                if it == 0:
                    rr = uu
                    inv = [1.0 / (u + scale_ref[m] * v)
                           for u, v in zip(load(w, modes), load(w, modes + 1))]
                    save(invp, m, inv)
                    save(r0, m, rr)
                elif it == 1:
                    rr = [u - v for u, v in zip(uu, load(r0, m))]
                    inv = load(invp, m)
                    save(r1, m, rr)
                else:
                    rr = [2.0 * (u - v) - s for u, v, s in zip(uu, load(r1, m), load(r0, m))]
                    inv = load(invp, m)
                    save(r2, m, rr)
                zz = [u * v for u, v in zip(rr, inv)]
                fill(g, slot, zz)
                sums[2 * it, pl.ds(m, 1), :] = shared_rows([u * v for u, v in zip(uu, zz)])
                f = load2(flux)
                gx = [combo(SLOPES[a], zz) for a in range(4)]
                fg = [f[a] * gx[a] * scale_ref[m] for a in range(4)]
                mz = [u * v for u, v in zip(load2(mass), zz)]
                if it < ITERS - 1:
                    save(z, m, zz)
                else:
                    sums[2 * it + 1, pl.ds(m, 1), :] = total_rows(
                        [u * v + s * t for u, v, s, t in zip(mz, zz, fg, gx)])
                save(w, m, [mz[a] + combo(SLOPES[:, a], fg) for a in range(4)])
                return carry

            lax.fori_loop(0, per, first, 0, unroll=UNROLL)
            multiply(g, grad_ref)

            def second(slot, carry, it=it, g=g, base=base):
                m = base + slot
                grad = [gout[pl.ds(pl.multiple_of(slot * rows + p * q, q), q), :]
                        for p in range(4)]
                fy = [u * v * scale_ref[m] for u, v in zip(load2(flux), grad)]
                if it == ITERS - 1:
                    e = 2 * it + 1
                    sums[e, pl.ds(m, 1), :] = sums[e, pl.ds(m, 1), :] + total_rows(
                        [u * v for u, v in zip(fy, grad)])
                fill(g, slot, fy)
                return carry

            lax.fori_loop(0, per, second, 0, unroll=UNROLL)
            if it < ITERS - 1:
                finish(g, it, base)

    high = lax.broadcasted_iota(jnp.int32, (FIELD, LANES), 0)
    wide = lax.broadcasted_iota(jnp.int32, (FIELD, LANES), 1)
    picks = [(wide == e * FIELD + high) & (high < modes) for e in range(PRODUCTS)]
    spread = jnp.zeros((FIELD, LANES), f32)
    for e in range(PRODUCTS):
        part = jnp.sum(sums[e], axis=1, keepdims=True)
        spread = spread + jnp.where(picks[e], part, 0.0)
    line = jnp.sum(spread, axis=0, keepdims=True)

    def share(stage, line, tx, rx, peers):
        tx[...] = line
        rx[0] = line
        for j, where in enumerate(peers):
            pltpu.make_async_remote_copy(
                src_ref=tx, dst_ref=rx.at[j + 1], send_sem=atx_sem.at[stage],
                recv_sem=arx_sem.at[stage], device_id=where, device_id_type=MESH).start()

    def gather(stage, rx):
        got = rx.at[pl.ds(1, rx.shape[0] - 1)]
        pltpu.make_async_copy(got, got, arx_sem.at[stage]).wait()
        return jnp.sum(rx[...], axis=0)

    share(0, line, near_tx, near_rx, near)
    for g in range(groups):
        finish(g, ITERS - 1, g * per)
    share(1, gather(0, near_rx), far_tx, far_rx, far)
    for g in range(groups):
        k = ITERS * groups + g
        merged = arrive(k)

        def last(slot, carry, g=g, k=k, merged=merged):
            m = g * per + slot
            save(u2, m, assembled(k, m, slot, merged))
            return carry

        lax.fori_loop(0, per, last, 0, unroll=UNROLL)

    total = gather(1, far_rx)
    pad = (high[:, :1] >= modes).astype(f32)
    n0, p00, p01, p11, p12, p22 = [
        jnp.broadcast_to(
            jnp.sum(jnp.where(pick, total, 0.0), axis=1, keepdims=True), (FIELD, LANES))
        for pick in picks]
    pad = jnp.broadcast_to(pad, (FIELD, LANES))
    p00, p11, p22 = p00 + pad, p11 + pad, p22 + 2.0 * pad
    b0 = n0
    b1 = p00 - n0
    b2 = 2.0 * (p01 - b1) - n0
    p02 = 2.0 * p11 - p00
    i0 = 1.0 / p00
    l1, l2 = p01 * i0, p02 * i0
    d1 = p11 - l1 * p01
    t2 = p12 - l2 * p01
    i1 = 1.0 / d1
    l3 = t2 * i1
    d2 = p22 - l2 * p02 - l3 * t2
    y1 = b1 - l1 * b0
    y2 = b2 - l2 * b0 - l3 * y1
    c2 = y2 / d2
    c1 = y1 * i1 - l3 * c2
    c0 = b0 * i0 - l1 * c1 - l2 * c2
    for e, c in enumerate((c0, c1, c2, 1.0 - c0 - 0.5 * c1, c0 + c1, 0.5 * c1)):
        coef[e] = c

    for k in range((ITERS + 1) * groups):
        for copy in halo_copies(k):
            copy.wait_send()
    for stage, rx in enumerate((near_rx, far_rx)):
        sent = rx.at[pl.ds(1, rx.shape[0] - 1)]
        pltpu.make_async_copy(sent, sent, atx_sem.at[stage]).wait()


def node_order(r0, r1, r2, u2, invp, coef, sol_ref, res_ref, sol_buf, res_buf, sem):
    modes, rows, cols = r0.shape
    q, tiles = rows // 4, cols // LANES

    def stores(m):
        return [
            pltpu.make_async_copy(
                buf.at[c, m], out.at[m, :, pl.ds(c * LANES, LANES)], sem.at[k, c, m])
            for k, (buf, out) in enumerate(((sol_buf, sol_ref), (res_buf, res_ref)))
            for c in range(tiles)
        ]

    def body(m, carry):
        c0, c1, c2, e0, e1, e2 = [coef[e, pl.ds(m, 1), :] for e in range(6)]
        for c in range(tiles):
            for p in range(4):
                at = (m, slice(p * q, (p + 1) * q), slice(c * LANES, (c + 1) * LANES))
                a0, a1, a2 = r0[at], r1[at], r2[at]
                sol_buf[c, m, pl.ds(p, q, stride=4), :] = invp[at] * (c0 * a0 + c1 * a1 + c2 * a2)
                res_buf[c, m, pl.ds(p, q, stride=4), :] = (
                    e0 * a0 - e1 * a1 - e2 * a2 - c2 * u2[at])
        for copy in stores(m):
            copy.start()
        return carry

    lax.fori_loop(0, modes, body, 0)

    def drain(m, carry):
        for copy in stores(m):
            copy.wait()
        return carry

    lax.fori_loop(0, modes, drain, 0)


def strided(refs, p, q):
    return jnp.concatenate([ref[pl.ds(p, q, stride=4), :] for ref in refs], axis=1)


def stack_table(table):
    top = table.astype(bf16)
    low = (table - top.astype(np.float32)).astype(bf16)
    return np.concatenate([top, top, low], axis=0)


def shards(nc, ns, forcing, metric, jacobian, mode_scale):
    modes, rows, cols = forcing.shape
    block = np.kron(np.eye(cols // 4), SLOPES).astype(np.float32)
    grad, div = stack_table(block.T), stack_table(block)
    q, tiles = rows // 4, cols // LANES
    groups = GROUPS if modes % GROUPS == 0 else 1
    per = modes // groups
    slots = -(-(per + 2) // 8) * 8
    vm = pl.BlockSpec(memory_space=pltpu.VMEM)
    hbm = pl.BlockSpec(memory_space=pltpu.HBM)
    rounds = (ITERS + 1) * groups
    ny, nz, nk, nx = planes(nc, ns)
    field = pltpu.VMEM((modes, rows, cols), f32)
    split = pltpu.VMEM((tiles, modes, rows, LANES), f32)
    table = pltpu.VMEM(grad.shape, bf16)
    line = pltpu.VMEM((1, LANES), f32)
    shape = jax.ShapeDtypeStruct(forcing.shape, f32)
    kept = pl.pallas_call(
        functools.partial(kernel, nc, ns, modes, groups),
        out_shape=[shape] * 5 + [jax.ShapeDtypeStruct((6, FIELD, LANES), f32)],
        in_specs=[hbm] * 6,
        out_specs=[vm] * 6,
        scratch_shapes=[
            field,
            pltpu.VMEM((modes + 2, rows, cols), f32),
            pltpu.VMEM((rows, cols), f32),
            pltpu.VMEM((rows, cols), f32),
            pltpu.VMEM((groups, per * rows, 2 * cols), bf16),
            pltpu.VMEM((per * rows, cols), f32),
            pltpu.VMEM((PRODUCTS, FIELD, cols), f32),
            pltpu.VMEM((rounds, 2, slots, cols), f32),
            pltpu.VMEM((rounds, 2, slots, cols), f32),
            pltpu.VMEM((rounds, 2, q, LANES), f32),
            pltpu.VMEM((rounds, 2, q, LANES), f32),
            pltpu.VMEM((rounds, 4, 1, LANES), f32),
            line,
            pltpu.VMEM((ny * nk * nx, 1, LANES), f32),
            line,
            pltpu.VMEM((nz, 1, LANES), f32),
            split,
            pltpu.VMEM((2, tiles, rows, LANES), f32),
            table, table,
            pltpu.SMEM((modes,), f32),
            pltpu.SemaphoreType.DMA((rounds, 8)),
            pltpu.SemaphoreType.DMA((rounds, 8)),
            pltpu.SemaphoreType.DMA((2,)),
            pltpu.SemaphoreType.DMA((2,)),
            pltpu.SemaphoreType.DMA((3, tiles)),
            pltpu.SemaphoreType.DMA((3,)),
        ],
        compiler_params=pltpu.CompilerParams(
            collective_id=0, has_side_effects=True, vmem_limit_bytes=41943040),
    )(*[pltpu.with_memory_space_constraint(v, pltpu.HBM) for v in (mode_scale, forcing, metric, jacobian, jnp.asarray(grad), jnp.asarray(div))])
    return pl.pallas_call(
        node_order,
        out_shape=[shape] * 2,
        in_specs=[vm] * 6,
        out_specs=[hbm, hbm],
        scratch_shapes=[split, split, pltpu.SemaphoreType.DMA((2, tiles, modes))],
        compiler_params=pltpu.CompilerParams(vmem_limit_bytes=16 * 1024 * 1024),
    )(*kept)


def solution(mesh):
    placed = (P(None, "curve", "sub"), P("curve", "sub"), P("curve", "sub"), P())
    return jax.shard_map(
        functools.partial(shards, mesh.shape["curve"], mesh.shape["sub"]),
        mesh=mesh,
        in_specs=placed,
        out_specs=(P(None, "curve", "sub"), P(None, "curve", "sub")),
        check_vma=False,
    )
```

```python
import functools
import math

import jax
import jax.numpy as jnp
import numpy as np
from jax import lax
from jax.experimental import pallas as pl
from jax.experimental.pallas import tpu as pltpu
from jax.sharding import PartitionSpec as P

ITERS = 3
GROUPS = 2
UNROLL = True
MESH = pl.DeviceIdType.MESH
LANES = 128
f32 = jnp.float32
bf16 = jnp.bfloat16


def gll_tables():
    points = np.array([-1.0, -1.0 / math.sqrt(5.0), 1.0 / math.sqrt(5.0), 1.0])
    weights = np.array([1.0 / 6.0, 5.0 / 6.0, 5.0 / 6.0, 1.0 / 6.0])
    factor = np.array(
        [np.prod([points[j] - points[m] for m in range(4) if m != j]) for j in range(4)]
    )
    slopes = np.zeros((4, 4))
    for i in range(4):
        for j in range(4):
            if i != j:
                slopes[i, j] = factor[i] / (factor[j] * (points[i] - points[j]))
        slopes[i, i] = sum((1.0 / (points[i] - points[m]) for m in range(4) if m != i))
    return (slopes, weights)


SLOPES, WEIGHTS = gll_tables()


def combo(coefs, parts):
    total = None
    for c, v in zip(coefs, parts):
        if abs(c) < 1e-12:
            continue
        term = v * f32(c)
        total = term if total is None else total + term
    return total


PRODUCTS = 6
FIELD = 16


def planes(nc, ns):
    depth = 8 if nc % 16 == 0 else 2
    return nc // (2 * depth), depth, 2, ns


def kernel(
    nc, ns, modes, groups,
    scale_hbm, forcing_ref, metric_ref, jac_ref, grad_hbm, div_hbm,
    r0, r1, r2, u2, invp, coef,
    z, w, mass, flux, zcat, gout, sums,
    row_tx, row_rx, col_tx, col_rx, cor_tx, cor_rx, near_tx, near_rx, far_tx, far_rx,
    source, factors, grad_ref, div_ref, scale_ref,
    htx_sem, hrx_sem, atx_sem, arx_sem, in_sem, table_sem,
):
    rows, cols = metric_ref.shape
    q = rows // 4
    half = cols - LANES
    tiles = cols // LANES
    per = modes // groups
    slots = row_tx.shape[2]
    loads, sources = [], []
    for c in range(tiles):
        cut = pl.ds(c * LANES, LANES)
        loads += [
            pltpu.make_async_copy(jac_ref.at[:, cut], factors.at[0, c], in_sem.at[0, c]),
            pltpu.make_async_copy(metric_ref.at[:, cut], factors.at[1, c], in_sem.at[1, c]),
        ]
        sources.append(
            pltpu.make_async_copy(forcing_ref.at[:, :, cut], source.at[c], in_sem.at[2, c]))
    div_load = pltpu.make_async_copy(div_hbm, div_ref, table_sem.at[0])
    grad_load = pltpu.make_async_copy(grad_hbm, grad_ref, table_sem.at[1])
    scale_load = pltpu.make_async_copy(scale_hbm, scale_ref, table_sem.at[2])
    for copy in loads + sources + [div_load, scale_load, grad_load]:
        copy.start()

    me_c, me_s = lax.axis_index("curve"), lax.axis_index("sub")
    up, down = lax.rem(me_c + nc - 1, nc), lax.rem(me_c + 1, nc)
    left, right = lax.rem(me_s + ns - 1, ns), lax.rem(me_s + 1, ns)

    ny, nz, nk, nx = planes(nc, ns)
    core, chip = lax.rem(me_c, nk), me_c // nk
    at_z, at_y = lax.rem(chip, nz), chip // nz
    subs = [me_s if dx == 0 else lax.rem(me_s + dx, nx) for dx in range(nx)]
    near, far = [], []
    for dy in range(ny):
        y = at_y if dy == 0 else lax.rem(at_y + dy, ny)
        for dk in range(nk):
            k = core if dk == 0 else 1 - core
            c = (y * nz + at_z) * nk + k
            near += [(c, subs[dx]) for dx in range(nx)]
    for dz in range(nz):
        far.append(((at_y * nz + lax.rem(at_z + dz, nz)) * nk + core, me_s))
    near, far = near[1:], far[1:]

    barrier = pltpu.get_barrier_semaphore()
    greeted = [
        (up, left), (up, right), (down, left), (down, right), (up, me_s), (down, me_s),
        (me_c, left), (me_c, right)] + near + far
    for where in greeted:
        pl.semaphore_signal(barrier, inc=1, device_id=where, device_id_type=MESH)

    lane_full = lax.broadcasted_iota(jnp.int32, (q, cols), 1)
    lane = lax.broadcasted_iota(jnp.int32, (q, LANES), 1)
    row_at = lax.broadcasted_iota(jnp.int32, (q, cols), 0)
    phase = lane_full % 4
    on_edge = (phase == 0) | (phase == 3)
    take_next = (phase == 3) & (lane_full != cols - 1)
    take_prev = (phase == 0) & (lane_full != 0)

    def load(ref, m):
        return [ref[m, p * q:(p + 1) * q, :] for p in range(4)]

    def save(ref, m, parts):
        for p in range(4):
            ref[m, p * q:(p + 1) * q, :] = parts[p]

    def load2(ref):
        return [ref[p * q:(p + 1) * q, :] for p in range(4)]

    def pack(k, m, slot, h, tops):
        lo, hi = tops
        row_tx[k, 0, pl.ds(slot, 1), :] = h[0][0:1, :]
        row_tx[k, 1, pl.ds(slot, 1), :] = h[3][q - 1:q, :]
        t0 = h[0] + jnp.where(row_at == 0, 0.0, pltpu.roll(h[3], 1, 0))
        t3 = h[3] + jnp.where(row_at == q - 1, 0.0, pltpu.roll(h[0], q - 1, 0))
        t = [t0, h[1], h[2], t3]
        save(w, m, t)
        for p in range(4):
            at = 4 * slot + p
            lo = jnp.where(lane == at, pltpu.roll(t[p][:, :LANES], at, 1), lo)
            hi = jnp.where(lane == at, pltpu.roll(t[p][:, half:], at + 1, 1), hi)
        return lo, hi

    def early(k):
        return groups <= k < ITERS * groups

    def halo_copies(k):
        if early(k):
            corners = [cor_tx.at[k, pl.ds(2 * e, 1)] for e in range(4)]
        else:
            corners = [col_tx.at[k, e % 2, pl.ds(0 if e < 2 else q - 1, 1)] for e in range(4)]
        plan = [
            (corners[0], cor_rx.at[k, 3], (up, left)),
            (corners[1], cor_rx.at[k, 2], (up, right)),
            (corners[2], cor_rx.at[k, 1], (down, left)),
            (corners[3], cor_rx.at[k, 0], (down, right)),
            (row_tx.at[k, 0], row_rx.at[k, 1], (up, me_s)),
            (row_tx.at[k, 1], row_rx.at[k, 0], (down, me_s)),
            (col_tx.at[k, 0], col_rx.at[k, 1], (me_c, left)),
            (col_tx.at[k, 1], col_rx.at[k, 0], (me_c, right)),
        ]
        return [
            pltpu.make_async_remote_copy(
                src_ref=src, dst_ref=dst, send_sem=htx_sem.at[k, e], recv_sem=hrx_sem.at[k, e],
                device_id=where, device_id_type=MESH)
            for e, (src, dst, where) in enumerate(plan)
        ]

    def send(k, tops):
        col_tx[k, 0], col_tx[k, 1] = tops
        for copy in halo_copies(k)[4 if early(k) else 0:]:
            copy.start()

    def arrive(k):
        for copy in halo_copies(k):
            copy.wait_recv()
        ph = lax.broadcasted_iota(jnp.int32, (1, LANES), 1) % 4
        edge_row = lax.broadcasted_iota(jnp.int32, (q, LANES), 0)
        merged = []
        for side in range(2):
            above, below = cor_rx[k, side], cor_rx[k, 2 + side]
            above = jnp.where(ph == 0, pltpu.roll(above, LANES - 3, 1), 0.0)
            below = jnp.where(ph == 3, pltpu.roll(below, 3, 1), 0.0)
            c = col_rx[k, side]
            c = c + jnp.where(edge_row == 0, above, 0.0) + jnp.where(edge_row == q - 1, below, 0.0)
            merged.append(c)
        return merged

    def assembled(k, m, slot, merged):
        t = load(w, m)
        t[0] = t[0] + jnp.where(row_at == 0, row_rx[k, 0, pl.ds(slot, 1), :], 0.0)
        t[3] = t[3] + jnp.where(row_at == q - 1, row_rx[k, 1, pl.ds(slot, 1), :], 0.0)
        out = []
        for p in range(4):
            at = 4 * slot + p
            c = t[p] + jnp.where(
                take_next, pltpu.roll(t[p], cols - 1, 1),
                jnp.where(take_prev, pltpu.roll(t[p], 1, 1), 0.0))
            a = jnp.where(lane == 0, pltpu.roll(merged[0], LANES - at, 1), 0.0)
            b = jnp.where(lane == LANES - 1, pltpu.roll(merged[1], LANES - 1 - at, 1), 0.0)
            pieces = [c[:, e * LANES:(e + 1) * LANES] for e in range(tiles)]
            pieces[0] = pieces[0] + a
            pieces[-1] = pieces[-1] + b
            out.append(jnp.concatenate(pieces, axis=1))
        return out

    edge_w, mid_w = f32(1.0 / 6.0), f32(5.0 / 6.0)
    col_w = jnp.where(on_edge, edge_w, mid_w)
    mw, fw = [], []
    for copy in loads:
        copy.wait()
    for p in range(4):
        grid_w = col_w * (edge_w if p in (0, 3) else mid_w)
        mw.append(strided([factors.at[0, c] for c in range(tiles)], p, q) * grid_w)
        fw.append(strided([factors.at[1, c] for c in range(tiles)], p, q) * grid_w)
        mass[p * q:(p + 1) * q, :] = mw[p]
        flux[p * q:(p + 1) * q, :] = fw[p]
    zero = jnp.zeros((q, LANES), f32)
    tops = pack(0, modes, per, mw, (zero, zero))
    div_load.wait()
    table = div_ref[:cols, :].astype(f32) + div_ref[2 * cols:, :].astype(f32)
    by_cols = jnp.dot(flux[...], table * table, precision=lax.Precision.HIGHEST,
                      preferred_element_type=f32)
    squared = SLOPES * SLOPES
    lap = [combo(squared[:, a], fw) + by_cols[a * q:(a + 1) * q, :] for a in range(4)]
    tops = pack(0, modes + 1, per + 1, lap, tops)
    for copy in sources:
        copy.wait()
    for g in range(groups):

        def start_body(slot, carry, g=g):
            m = g * per + slot
            h = [strided([source.at[c, m] for c in range(tiles)], p, q)
                 * mass[p * q:(p + 1) * q, :] for p in range(4)]
            return pack(g, m, slot, h, carry)

        tops = lax.fori_loop(0, per, start_body, tops if g == 0 else (zero, zero), unroll=UNROLL)
        if g == 0:
            pl.semaphore_wait(barrier, len(greeted))
        send(g, tops)
    scale_load.wait()
    grad_load.wait()

    at_lane = lax.broadcasted_iota(jnp.int32, (1, LANES), 1)
    of_four = at_lane % 4
    tall = lax.broadcasted_iota(jnp.int32, (slots, LANES), 0)
    flat = lax.broadcasted_iota(jnp.int32, (slots, LANES), 1)
    low_half = tall < 4

    def coefs(values):
        line = jnp.zeros((1, LANES), f32)
        for e, value in enumerate(values):
            line = jnp.where(of_four == e, f32(value), line)
        return line

    def corner_weights(g):
        scale = jnp.zeros((1, LANES), f32)
        for slot in range(per):
            scale = jnp.where(at_lane // 4 == slot, scale_ref[g * per + slot], scale)
        lines = []
        for tb in range(2):
            er, cr = (0, 0) if tb == 0 else (q - 1, 3)
            for side in range(2):
                cc, edge, start = (0, 0, 0) if side == 0 else (3, cols - 1, cols - 4)
                sx = jnp.zeros((1, LANES), f32)
                sy = jnp.zeros((1, LANES), f32)
                own = jnp.zeros((1, 1), f32)
                for e in range(4):
                    fx = flux[e * q + er:e * q + er + 1, edge:edge + 1]
                    fy = flux[cr * q + er:cr * q + er + 1, start + e:start + e + 1]
                    sx = sx + fx * coefs(SLOPES[e, cr] * SLOPES[e])
                    sy = sy + fy * coefs(SLOPES[e, cc] * SLOPES[e])
                    own = own + fy * f32(SLOPES[e, cc] * SLOPES[e, cc])
                here = mass[cr * q + er:cr * q + er + 1, edge:edge + 1]
                lines += [
                    scale * sx + jnp.where(of_four == cr, here + scale * own, 0.0),
                    jnp.where(of_four == cc, 0.0, scale * sy)]
        return scale, jnp.concatenate(lines, axis=0)

    def gathered_rows(x):
        left = x[:, :LANES]
        left = left + jnp.where(flat == 3, pltpu.roll(left, LANES - 1, 1), 0.0)
        right = x[:, half:]
        right = right + jnp.where(flat == LANES - 4, pltpu.roll(right, 1, 1), 0.0)
        left = pltpu.roll(jnp.where(flat < 4, left, 0.0), 0, 1, stride=4, stride_axis=0)
        right = pltpu.roll(
            jnp.where(flat >= LANES - 4, right, 0.0), 4, 1, stride=4, stride_axis=0)
        return [jnp.sum(v, axis=0, keepdims=True) for v in (left, right)]

    def corner_values(k, merged):
        lines = []
        for tb in range(2):
            er, cr = (0, 0) if tb == 0 else (q - 1, 3)
            halo = row_rx[k, tb]
            rows_here = gathered_rows(row_tx[k, tb] + halo)
            for side in range(2):
                edge = 0 if side == 0 else cols - 1
                place = flat == 4 * tall + cr
                extra = jnp.sum(
                    jnp.where(place, halo[:, edge:edge + 1], 0.0), axis=0, keepdims=True)
                col = col_tx[k, side, er:er + 1, :] + merged[side][er:er + 1, :] + extra
                lines += [col, rows_here[side]]
        return jnp.concatenate(lines, axis=0)

    def send_corners(k, weights, v):
        h = weights * v
        fore = h + pltpu.roll(h, LANES - 1, 1)
        fore = fore + pltpu.roll(fore, LANES - 2, 1)
        back = h + pltpu.roll(h, 1, 1)
        back = back + pltpu.roll(back, 2, 1)
        h = jnp.where(low_half, fore, back)
        cor_tx[k] = h + pltpu.roll(h, slots - 1, 0)
        for copy in halo_copies(k)[:4]:
            copy.start()

    def repeat(x, slot):
        x = jnp.where(flat // 4 == slot, x, 0.0)
        x = pltpu.roll(x, LANES - 4 * slot, 1)
        for step in (4, 8, 16):
            x = x + pltpu.roll(x, step, 1)
        return x

    assert slots == 8
    corner = [corner_weights(g) for g in range(groups)]
    corner_r, corner_inv, shared_diag = [None] * groups, [None] * groups, []

    def corner_step(it, g, k, merged):
        u = corner_values(k, merged)
        scale, weights = corner[g]
        if it == 0:
            if g == 0:
                shared_diag.extend([repeat(u, per), repeat(u, per + 1)])
            used = flat < 4 * per
            u = jnp.where(used, u, 0.0)
            corner_r[g] = u
            corner_inv[g] = jnp.where(used, 1.0 / jnp.where(
                used, shared_diag[0] + scale * shared_diag[1], 1.0), 0.0)
            r = u
        else:
            r = jnp.where(flat < 4 * per, u, 0.0) - corner_r[g]
        send_corners(k + groups, weights, r * corner_inv[g])

    def fill(g, slot, parts):
        v = jnp.concatenate(parts, axis=0)
        top = v.astype(bf16)
        at = pl.ds(pl.multiple_of(slot * rows, rows), rows)
        zcat[g, at, :cols] = top
        zcat[g, at, cols:] = (v - top.astype(f32)).astype(bf16)

    def multiply(g, table_ref):
        gout[...] = (
            jnp.dot(zcat[g], table_ref[:2 * cols, :], preferred_element_type=f32)
            + jnp.dot(zcat[g, :, :cols], table_ref[2 * cols:, :], preferred_element_type=f32))

    def total_rows(parts):
        return jnp.sum((parts[0] + parts[3]) + (parts[1] + parts[2]), axis=0, keepdims=True)

    def shared_rows(parts):
        line = (parts[0] + parts[3]) * 0.5 + (parts[1] + parts[2])
        return jnp.sum(jnp.where(on_edge, line * 0.5, line), axis=0, keepdims=True)

    def finish(g, k, base):
        multiply(g, div_ref)

        def third(slot, carry):
            m = base + slot
            h = [u + gout[pl.ds(pl.multiple_of(slot * rows + p * q, q), q), :]
                 for p, u in enumerate(load(w, m))]
            if k < ITERS - 1:
                zh = [u * v for u, v in zip(load(z, m), h)]
                sums[2 * k + 1, pl.ds(m, 1), :] = total_rows(zh)
            return pack((k + 1) * groups + g, m, slot, h, carry)

        tops = lax.fori_loop(0, per, third, (zero, zero), unroll=UNROLL)
        send((k + 1) * groups + g, tops)

    for it in range(ITERS):
        for g in range(groups):
            base = g * per
            k = it * groups + g
            merged = arrive(k)
            if it < ITERS - 1:
                corner_step(it, g, k, merged)
            if it == 0 and g == 0:
                for e in range(2):
                    save(w, modes + e, assembled(k, modes + e, per + e, merged))

            def first(slot, carry, it=it, g=g, k=k, base=base, merged=merged):
                m = base + slot
                uu = assembled(k, m, slot, merged)
                if it == 0:
                    rr = uu
                    inv = [1.0 / (u + scale_ref[m] * v)
                           for u, v in zip(load(w, modes), load(w, modes + 1))]
                    save(invp, m, inv)
                    save(r0, m, rr)
                elif it == 1:
                    rr = [u - v for u, v in zip(uu, load(r0, m))]
                    inv = load(invp, m)
                    save(r1, m, rr)
                else:
                    rr = [2.0 * (u - v) - s for u, v, s in zip(uu, load(r1, m), load(r0, m))]
                    inv = load(invp, m)
                    save(r2, m, rr)
                zz = [u * v for u, v in zip(rr, inv)]
                fill(g, slot, zz)
                sums[2 * it, pl.ds(m, 1), :] = shared_rows([u * v for u, v in zip(uu, zz)])
                f = load2(flux)
                gx = [combo(SLOPES[a], zz) for a in range(4)]
                fg = [f[a] * gx[a] * scale_ref[m] for a in range(4)]
                mz = [u * v for u, v in zip(load2(mass), zz)]
                if it < ITERS - 1:
                    save(z, m, zz)
                else:
                    sums[2 * it + 1, pl.ds(m, 1), :] = total_rows(
                        [u * v + s * t for u, v, s, t in zip(mz, zz, fg, gx)])
                save(w, m, [mz[a] + combo(SLOPES[:, a], fg) for a in range(4)])
                return carry

            lax.fori_loop(0, per, first, 0, unroll=UNROLL)
            multiply(g, grad_ref)

            def second(slot, carry, it=it, g=g, base=base):
                m = base + slot
                grad = [gout[pl.ds(pl.multiple_of(slot * rows + p * q, q), q), :]
                        for p in range(4)]
                fy = [u * v * scale_ref[m] for u, v in zip(load2(flux), grad)]
                if it == ITERS - 1:
                    e = 2 * it + 1
                    sums[e, pl.ds(m, 1), :] = sums[e, pl.ds(m, 1), :] + total_rows(
                        [u * v for u, v in zip(fy, grad)])
                fill(g, slot, fy)
                return carry

            lax.fori_loop(0, per, second, 0, unroll=UNROLL)
            if it < ITERS - 1:
                finish(g, it, base)

    high = lax.broadcasted_iota(jnp.int32, (FIELD, LANES), 0)
    wide = lax.broadcasted_iota(jnp.int32, (FIELD, LANES), 1)
    picks = [(wide == e * FIELD + high) & (high < modes) for e in range(PRODUCTS)]
    spread = jnp.zeros((FIELD, LANES), f32)
    for e in range(PRODUCTS):
        part = jnp.sum(sums[e], axis=1, keepdims=True)
        spread = spread + jnp.where(picks[e], part, 0.0)
    line = jnp.sum(spread, axis=0, keepdims=True)

    def share(stage, line, tx, rx, peers):
        tx[...] = line
        rx[0] = line
        for j, where in enumerate(peers):
            pltpu.make_async_remote_copy(
                src_ref=tx, dst_ref=rx.at[j + 1], send_sem=atx_sem.at[stage],
                recv_sem=arx_sem.at[stage], device_id=where, device_id_type=MESH).start()

    def gather(stage, rx):
        got = rx.at[pl.ds(1, rx.shape[0] - 1)]
        pltpu.make_async_copy(got, got, arx_sem.at[stage]).wait()
        return jnp.sum(rx[...], axis=0)

    share(0, line, near_tx, near_rx, near)
    for g in range(groups):
        finish(g, ITERS - 1, g * per)
    share(1, gather(0, near_rx), far_tx, far_rx, far)
    for g in range(groups):
        k = ITERS * groups + g
        merged = arrive(k)

        def last(slot, carry, g=g, k=k, merged=merged):
            m = g * per + slot
            save(u2, m, assembled(k, m, slot, merged))
            return carry

        lax.fori_loop(0, per, last, 0, unroll=UNROLL)

    total = gather(1, far_rx)
    pad = (high[:, :1] >= modes).astype(f32)
    n0, p00, p01, p11, p12, p22 = [
        jnp.broadcast_to(
            jnp.sum(jnp.where(pick, total, 0.0), axis=1, keepdims=True), (FIELD, LANES))
        for pick in picks]
    pad = jnp.broadcast_to(pad, (FIELD, LANES))
    p00, p11, p22 = p00 + pad, p11 + pad, p22 + 2.0 * pad
    b0 = n0
    b1 = p00 - n0
    b2 = 2.0 * (p01 - b1) - n0
    p02 = 2.0 * p11 - p00
    i0 = 1.0 / p00
    l1, l2 = p01 * i0, p02 * i0
    d1 = p11 - l1 * p01
    t2 = p12 - l2 * p01
    i1 = 1.0 / d1
    l3 = t2 * i1
    d2 = p22 - l2 * p02 - l3 * t2
    y1 = b1 - l1 * b0
    y2 = b2 - l2 * b0 - l3 * y1
    c2 = y2 / d2
    c1 = y1 * i1 - l3 * c2
    c0 = b0 * i0 - l1 * c1 - l2 * c2
    for e, c in enumerate((c0, c1, c2, 1.0 - c0 - 0.5 * c1, c0 + c1, 0.5 * c1)):
        coef[e] = c

    for k in range((ITERS + 1) * groups):
        for copy in halo_copies(k):
            copy.wait_send()
    for stage, rx in enumerate((near_rx, far_rx)):
        sent = rx.at[pl.ds(1, rx.shape[0] - 1)]
        pltpu.make_async_copy(sent, sent, atx_sem.at[stage]).wait()


def node_order(r0, r1, r2, u2, invp, coef, sol_ref, res_ref, sol_buf, res_buf, sem):
    modes, rows, cols = r0.shape
    q, tiles = rows // 4, cols // LANES

    def stores(m):
        return [
            pltpu.make_async_copy(
                buf.at[c, m], out.at[m, :, pl.ds(c * LANES, LANES)], sem.at[k, c, m])
            for k, (buf, out) in enumerate(((sol_buf, sol_ref), (res_buf, res_ref)))
            for c in range(tiles)
        ]

    def body(m, carry):
        c0, c1, c2, e0, e1, e2 = [coef[e, pl.ds(m, 1), :] for e in range(6)]
        for c in range(tiles):
            for p in range(4):
                at = (m, slice(p * q, (p + 1) * q), slice(c * LANES, (c + 1) * LANES))
                a0, a1, a2 = r0[at], r1[at], r2[at]
                sol_buf[c, m, pl.ds(p, q, stride=4), :] = invp[at] * (c0 * a0 + c1 * a1 + c2 * a2)
                res_buf[c, m, pl.ds(p, q, stride=4), :] = (
                    e0 * a0 - e1 * a1 - e2 * a2 - c2 * u2[at])
        for copy in stores(m):
            copy.start()
        return carry

    lax.fori_loop(0, modes, body, 0)

    def drain(m, carry):
        for copy in stores(m):
            copy.wait()
        return carry

    lax.fori_loop(0, modes, drain, 0)


def strided(refs, p, q):
    return jnp.concatenate([ref[pl.ds(p, q, stride=4), :] for ref in refs], axis=1)


def stack_table(table):
    top = table.astype(bf16)
    low = (table - top.astype(np.float32)).astype(bf16)
    return np.concatenate([top, top, low], axis=0)


def shards(nc, ns, forcing, metric, jacobian, mode_scale):
    modes, rows, cols = forcing.shape
    block = np.kron(np.eye(cols // 4), SLOPES).astype(np.float32)
    grad, div = stack_table(block.T), stack_table(block)
    q, tiles = rows // 4, cols // LANES
    groups = GROUPS if modes % GROUPS == 0 else 1
    per = modes // groups
    slots = -(-(per + 2) // 8) * 8
    vm = pl.BlockSpec(memory_space=pltpu.VMEM)
    hbm = pl.BlockSpec(memory_space=pltpu.HBM)
    rounds = (ITERS + 1) * groups
    ny, nz, nk, nx = planes(nc, ns)
    field = pltpu.VMEM((modes, rows, cols), f32)
    split = pltpu.VMEM((tiles, modes, rows, LANES), f32)
    table = pltpu.VMEM(grad.shape, bf16)
    line = pltpu.VMEM((1, LANES), f32)
    shape = jax.ShapeDtypeStruct(forcing.shape, f32)
    kept = pl.pallas_call(
        functools.partial(kernel, nc, ns, modes, groups),
        out_shape=[shape] * 5 + [jax.ShapeDtypeStruct((6, FIELD, LANES), f32)],
        in_specs=[hbm] * 6,
        out_specs=[vm] * 6,
        scratch_shapes=[
            field,
            pltpu.VMEM((modes + 2, rows, cols), f32),
            pltpu.VMEM((rows, cols), f32),
            pltpu.VMEM((rows, cols), f32),
            pltpu.VMEM((groups, per * rows, 2 * cols), bf16),
            pltpu.VMEM((per * rows, cols), f32),
            pltpu.VMEM((PRODUCTS, FIELD, cols), f32),
            pltpu.VMEM((rounds, 2, slots, cols), f32),
            pltpu.VMEM((rounds, 2, slots, cols), f32),
            pltpu.VMEM((rounds, 2, q, LANES), f32),
            pltpu.VMEM((rounds, 2, q, LANES), f32),
            pltpu.VMEM((rounds, 8, LANES), f32),
            pltpu.VMEM((rounds, 4, 1, LANES), f32),
            line,
            pltpu.VMEM((ny * nk * nx, 1, LANES), f32),
            line,
            pltpu.VMEM((nz, 1, LANES), f32),
            split,
            pltpu.VMEM((2, tiles, rows, LANES), f32),
            table, table,
            pltpu.SMEM((modes,), f32),
            pltpu.SemaphoreType.DMA((rounds, 8)),
            pltpu.SemaphoreType.DMA((rounds, 8)),
            pltpu.SemaphoreType.DMA((2,)),
            pltpu.SemaphoreType.DMA((2,)),
            pltpu.SemaphoreType.DMA((3, tiles)),
            pltpu.SemaphoreType.DMA((3,)),
        ],
        compiler_params=pltpu.CompilerParams(
            collective_id=0, has_side_effects=True, vmem_limit_bytes=41943040),
    )(*[pltpu.with_memory_space_constraint(v, pltpu.HBM) for v in (mode_scale, forcing, metric, jacobian, jnp.asarray(grad), jnp.asarray(div))])
    return pl.pallas_call(
        node_order,
        out_shape=[shape] * 2,
        in_specs=[vm] * 6,
        out_specs=[hbm, hbm],
        scratch_shapes=[split, split, pltpu.SemaphoreType.DMA((2, tiles, modes))],
        compiler_params=pltpu.CompilerParams(vmem_limit_bytes=16 * 1024 * 1024),
    )(*kept)


def solution(mesh):
    placed = (P(None, "curve", "sub"), P("curve", "sub"), P("curve", "sub"), P())
    return jax.shard_map(
        functools.partial(shards, mesh.shape["curve"], mesh.shape["sub"]),
        mesh=mesh,
        in_specs=placed,
        out_specs=(P(None, "curve", "sub"), P(None, "curve", "sub")),
        check_vma=False,
    )
```

```python
import functools
import math

import jax
import jax.numpy as jnp
import numpy as np
from jax import lax
from jax.experimental import pallas as pl
from jax.experimental.pallas import tpu as pltpu
from jax.sharding import PartitionSpec as P

ITERS = 3
GROUPS = 2
UNROLL = True
MESH = pl.DeviceIdType.MESH
LANES = 128
f32 = jnp.float32
bf16 = jnp.bfloat16


def gll_tables():
    points = np.array([-1.0, -1.0 / math.sqrt(5.0), 1.0 / math.sqrt(5.0), 1.0])
    weights = np.array([1.0 / 6.0, 5.0 / 6.0, 5.0 / 6.0, 1.0 / 6.0])
    factor = np.array(
        [np.prod([points[j] - points[m] for m in range(4) if m != j]) for j in range(4)]
    )
    slopes = np.zeros((4, 4))
    for i in range(4):
        for j in range(4):
            if i != j:
                slopes[i, j] = factor[i] / (factor[j] * (points[i] - points[j]))
        slopes[i, i] = sum((1.0 / (points[i] - points[m]) for m in range(4) if m != i))
    return (slopes, weights)


SLOPES, WEIGHTS = gll_tables()


def combo(coefs, parts):
    total = None
    for c, v in zip(coefs, parts):
        if abs(c) < 1e-12:
            continue
        term = v * f32(c)
        total = term if total is None else total + term
    return total


PRODUCTS = 6
FIELD = 16


def planes(nc, ns):
    depth = 8 if nc % 16 == 0 else 2
    return nc // (2 * depth), depth, 2, ns


def kernel(
    nc, ns, modes, groups,
    scale_hbm, forcing_ref, metric_ref, jac_ref, grad_hbm, div_hbm,
    r0, r1, r2, u2, invp, coef,
    z, w, mass, flux, zcat, gout, sums,
    row_tx, row_rx, col_tx, col_rx, cor_tx, cor_rx, near_tx, near_rx, far_tx, far_rx,
    source, factors, grad_ref, div_ref, scale_ref,
    htx_sem, hrx_sem, atx_sem, arx_sem, in_sem, table_sem,
):
    rows, cols = metric_ref.shape
    q = rows // 4
    half = cols - LANES
    tiles = cols // LANES
    per = modes // groups
    slots = row_tx.shape[2]
    loads, sources = [], []
    for c in range(tiles):
        cut = pl.ds(c * LANES, LANES)
        loads += [
            pltpu.make_async_copy(jac_ref.at[:, cut], factors.at[0, c], in_sem.at[0, c]),
            pltpu.make_async_copy(metric_ref.at[:, cut], factors.at[1, c], in_sem.at[1, c]),
        ]
        sources.append(
            pltpu.make_async_copy(forcing_ref.at[:, :, cut], source.at[c], in_sem.at[2, c]))
    div_load = pltpu.make_async_copy(div_hbm, div_ref, table_sem.at[0])
    grad_load = pltpu.make_async_copy(grad_hbm, grad_ref, table_sem.at[1])
    scale_load = pltpu.make_async_copy(scale_hbm, scale_ref, table_sem.at[2])
    for copy in loads + sources + [div_load, scale_load, grad_load]:
        copy.start()

    me_c, me_s = lax.axis_index("curve"), lax.axis_index("sub")
    up, down = lax.rem(me_c + nc - 1, nc), lax.rem(me_c + 1, nc)
    left, right = lax.rem(me_s + ns - 1, ns), lax.rem(me_s + 1, ns)

    ny, nz, nk, nx = planes(nc, ns)
    core, chip = lax.rem(me_c, nk), me_c // nk
    at_z, at_y = lax.rem(chip, nz), chip // nz
    subs = [me_s if dx == 0 else lax.rem(me_s + dx, nx) for dx in range(nx)]
    near, far = [], []
    for dy in range(ny):
        y = at_y if dy == 0 else lax.rem(at_y + dy, ny)
        for dk in range(nk):
            k = core if dk == 0 else 1 - core
            c = (y * nz + at_z) * nk + k
            near += [(c, subs[dx]) for dx in range(nx)]
    for dz in range(nz):
        far.append(((at_y * nz + lax.rem(at_z + dz, nz)) * nk + core, me_s))
    near, far = near[1:], far[1:]

    barrier = pltpu.get_barrier_semaphore()
    greeted = [
        (up, left), (up, right), (down, left), (down, right), (up, me_s), (down, me_s),
        (me_c, left), (me_c, right)] + near + far
    for where in greeted:
        pl.semaphore_signal(barrier, inc=1, device_id=where, device_id_type=MESH)

    lane_full = lax.broadcasted_iota(jnp.int32, (q, cols), 1)
    lane = lax.broadcasted_iota(jnp.int32, (q, LANES), 1)
    row_at = lax.broadcasted_iota(jnp.int32, (q, cols), 0)
    phase = lane_full % 4
    on_edge = (phase == 0) | (phase == 3)
    take_next = (phase == 3) & (lane_full != cols - 1)
    take_prev = (phase == 0) & (lane_full != 0)

    def load(ref, m):
        return [ref[m, p * q:(p + 1) * q, :] for p in range(4)]

    def save(ref, m, parts):
        for p in range(4):
            ref[m, p * q:(p + 1) * q, :] = parts[p]

    def load2(ref):
        return [ref[p * q:(p + 1) * q, :] for p in range(4)]

    def pack(k, m, slot, h, tops):
        lo, hi = tops
        row_tx[k, 0, pl.ds(slot, 1), :] = h[0][0:1, :]
        row_tx[k, 1, pl.ds(slot, 1), :] = h[3][q - 1:q, :]
        t0 = h[0] + jnp.where(row_at == 0, 0.0, pltpu.roll(h[3], 1, 0))
        t3 = h[3] + jnp.where(row_at == q - 1, 0.0, pltpu.roll(h[0], q - 1, 0))
        t = [t0, h[1], h[2], t3]
        save(w, m, t)
        for p in range(4):
            at = 4 * slot + p
            lo = jnp.where(lane == at, pltpu.roll(t[p][:, :LANES], at, 1), lo)
            hi = jnp.where(lane == at, pltpu.roll(t[p][:, half:], at + 1, 1), hi)
        return lo, hi

    def early(k):
        return groups <= k < ITERS * groups

    def halo_copies(k):
        if early(k):
            corners = [cor_tx.at[k, pl.ds(2 * e, 1)] for e in range(4)]
        else:
            corners = [col_tx.at[k, e % 2, pl.ds(0 if e < 2 else q - 1, 1)] for e in range(4)]
        plan = [
            (corners[0], cor_rx.at[k, 3], (up, left)),
            (corners[1], cor_rx.at[k, 2], (up, right)),
            (corners[2], cor_rx.at[k, 1], (down, left)),
            (corners[3], cor_rx.at[k, 0], (down, right)),
            (row_tx.at[k, 0], row_rx.at[k, 1], (up, me_s)),
            (row_tx.at[k, 1], row_rx.at[k, 0], (down, me_s)),
            (col_tx.at[k, 0], col_rx.at[k, 1], (me_c, left)),
            (col_tx.at[k, 1], col_rx.at[k, 0], (me_c, right)),
        ]
        return [
            pltpu.make_async_remote_copy(
                src_ref=src, dst_ref=dst, send_sem=htx_sem.at[k, e], recv_sem=hrx_sem.at[k, e],
                device_id=where, device_id_type=MESH)
            for e, (src, dst, where) in enumerate(plan)
        ]

    def send(k, tops):
        col_tx[k, 0], col_tx[k, 1] = tops
        for copy in halo_copies(k)[4 if early(k) else 0:]:
            copy.start()

    def arrive(k):
        for copy in halo_copies(k):
            copy.wait_recv()
        ph = lax.broadcasted_iota(jnp.int32, (1, LANES), 1) % 4
        edge_row = lax.broadcasted_iota(jnp.int32, (q, LANES), 0)
        merged = []
        for side in range(2):
            above, below = cor_rx[k, side], cor_rx[k, 2 + side]
            above = jnp.where(ph == 0, pltpu.roll(above, LANES - 3, 1), 0.0)
            below = jnp.where(ph == 3, pltpu.roll(below, 3, 1), 0.0)
            c = col_rx[k, side]
            c = c + jnp.where(edge_row == 0, above, 0.0) + jnp.where(edge_row == q - 1, below, 0.0)
            merged.append(c)
        return merged

    def assembled(k, m, slot, merged):
        t = load(w, m)
        t[0] = t[0] + jnp.where(row_at == 0, row_rx[k, 0, pl.ds(slot, 1), :], 0.0)
        t[3] = t[3] + jnp.where(row_at == q - 1, row_rx[k, 1, pl.ds(slot, 1), :], 0.0)
        out = []
        for p in range(4):
            at = 4 * slot + p
            c = t[p] + jnp.where(
                take_next, pltpu.roll(t[p], cols - 1, 1),
                jnp.where(take_prev, pltpu.roll(t[p], 1, 1), 0.0))
            a = jnp.where(lane == 0, pltpu.roll(merged[0], LANES - at, 1), 0.0)
            b = jnp.where(lane == LANES - 1, pltpu.roll(merged[1], LANES - 1 - at, 1), 0.0)
            pieces = [c[:, e * LANES:(e + 1) * LANES] for e in range(tiles)]
            pieces[0] = pieces[0] + a
            pieces[-1] = pieces[-1] + b
            out.append(jnp.concatenate(pieces, axis=1))
        return out

    edge_w, mid_w = f32(1.0 / 6.0), f32(5.0 / 6.0)
    col_w = jnp.where(on_edge, edge_w, mid_w)
    mw, fw = [], []
    for copy in loads:
        copy.wait()
    for p in range(4):
        grid_w = col_w * (edge_w if p in (0, 3) else mid_w)
        mw.append(strided([factors.at[0, c] for c in range(tiles)], p, q) * grid_w)
        fw.append(strided([factors.at[1, c] for c in range(tiles)], p, q) * grid_w)
        mass[p * q:(p + 1) * q, :] = mw[p]
        flux[p * q:(p + 1) * q, :] = fw[p]
    zero = jnp.zeros((q, LANES), f32)
    tops = pack(0, modes, per, mw, (zero, zero))
    div_load.wait()
    table = div_ref[:cols, :].astype(f32) + div_ref[2 * cols:, :].astype(f32)
    by_cols = jnp.dot(flux[...], table * table, precision=lax.Precision.HIGHEST,
                      preferred_element_type=f32)
    squared = SLOPES * SLOPES
    lap = [combo(squared[:, a], fw) + by_cols[a * q:(a + 1) * q, :] for a in range(4)]
    tops = pack(0, modes + 1, per + 1, lap, tops)
    for copy in sources:
        copy.wait()
    for g in range(groups):

        def start_body(slot, carry, g=g):
            m = g * per + slot
            h = [strided([source.at[c, m] for c in range(tiles)], p, q)
                 * mass[p * q:(p + 1) * q, :] for p in range(4)]
            return pack(g, m, slot, h, carry)

        tops = lax.fori_loop(0, per, start_body, tops if g == 0 else (zero, zero), unroll=UNROLL)
        if g == 0:
            pl.semaphore_wait(barrier, len(greeted))
        send(g, tops)
    scale_load.wait()
    grad_load.wait()

    at_lane = lax.broadcasted_iota(jnp.int32, (1, LANES), 1)
    of_four = at_lane % 4
    tall = lax.broadcasted_iota(jnp.int32, (slots, LANES), 0)
    flat = lax.broadcasted_iota(jnp.int32, (slots, LANES), 1)
    low_half = tall < 4

    def coefs(values):
        line = jnp.zeros((1, LANES), f32)
        for e, value in enumerate(values):
            line = jnp.where(of_four == e, f32(value), line)
        return line

    def corner_weights(g):
        scale = jnp.zeros((1, LANES), f32)
        for slot in range(per):
            scale = jnp.where(at_lane // 4 == slot, scale_ref[g * per + slot], scale)
        lines = []
        for tb in range(2):
            er, cr = (0, 0) if tb == 0 else (q - 1, 3)
            for side in range(2):
                cc, edge, start = (0, 0, 0) if side == 0 else (3, cols - 1, cols - 4)
                sx = jnp.zeros((1, LANES), f32)
                sy = jnp.zeros((1, LANES), f32)
                own = jnp.zeros((1, 1), f32)
                for e in range(4):
                    fx = flux[e * q + er:e * q + er + 1, edge:edge + 1]
                    fy = flux[cr * q + er:cr * q + er + 1, start + e:start + e + 1]
                    sx = sx + fx * coefs(SLOPES[e, cr] * SLOPES[e])
                    sy = sy + fy * coefs(SLOPES[e, cc] * SLOPES[e])
                    own = own + fy * f32(SLOPES[e, cc] * SLOPES[e, cc])
                here = mass[cr * q + er:cr * q + er + 1, edge:edge + 1]
                lines += [
                    scale * sx + jnp.where(of_four == cr, here + scale * own, 0.0),
                    jnp.where(of_four == cc, 0.0, scale * sy)]
        return scale, jnp.concatenate(lines, axis=0)

    def gathered_rows(x):
        left = x[:, :LANES]
        left = left + jnp.where(flat == 3, pltpu.roll(left, LANES - 1, 1), 0.0)
        right = x[:, half:]
        right = right + jnp.where(flat == LANES - 4, pltpu.roll(right, 1, 1), 0.0)
        left = pltpu.roll(jnp.where(flat < 4, left, 0.0), 0, 1, stride=4, stride_axis=0)
        right = pltpu.roll(
            jnp.where(flat >= LANES - 4, right, 0.0), 4, 1, stride=4, stride_axis=0)
        return [jnp.sum(v, axis=0, keepdims=True) for v in (left, right)]

    def corner_values(k, merged):
        lines = []
        for tb in range(2):
            er, cr = (0, 0) if tb == 0 else (q - 1, 3)
            halo = row_rx[k, tb]
            rows_here = gathered_rows(row_tx[k, tb] + halo)
            for side in range(2):
                edge = 0 if side == 0 else cols - 1
                place = flat == 4 * tall + cr
                extra = jnp.sum(
                    jnp.where(place, halo[:, edge:edge + 1], 0.0), axis=0, keepdims=True)
                col = col_tx[k, side, er:er + 1, :] + merged[side][er:er + 1, :] + extra
                lines += [col, rows_here[side]]
        return jnp.concatenate(lines, axis=0)

    def send_corners(k, weights, v):
        h = weights * v
        fore = h + pltpu.roll(h, LANES - 1, 1)
        fore = fore + pltpu.roll(fore, LANES - 2, 1)
        back = h + pltpu.roll(h, 1, 1)
        back = back + pltpu.roll(back, 2, 1)
        h = jnp.where(low_half, fore, back)
        cor_tx[k] = h + pltpu.roll(h, slots - 1, 0)
        for copy in halo_copies(k)[:4]:
            copy.start()

    def repeat(x, slot):
        x = jnp.where(flat // 4 == slot, x, 0.0)
        x = pltpu.roll(x, LANES - 4 * slot, 1)
        for step in (4, 8, 16):
            x = x + pltpu.roll(x, step, 1)
        return x

    assert slots == 8
    corner = [corner_weights(g) for g in range(groups)]
    corner_r, corner_inv, shared_diag = [None] * groups, [None] * groups, []

    def corner_step(it, g, k, merged):
        u = corner_values(k, merged)
        scale, weights = corner[g]
        if it == 0:
            if g == 0:
                shared_diag.extend([repeat(u, per), repeat(u, per + 1)])
            used = flat < 4 * per
            u = jnp.where(used, u, 0.0)
            corner_r[g] = u
            corner_inv[g] = jnp.where(used, 1.0 / jnp.where(
                used, shared_diag[0] + scale * shared_diag[1], 1.0), 0.0)
            r = u
        else:
            r = jnp.where(flat < 4 * per, u, 0.0) - corner_r[g]
        send_corners(k + groups, weights, r * corner_inv[g])

    def fill(g, slot, parts):
        v = jnp.concatenate(parts, axis=0)
        top = v.astype(bf16)
        at = pl.ds(pl.multiple_of(slot * rows, rows), rows)
        zcat[g, at, :cols] = top
        zcat[g, at, cols:] = (v - top.astype(f32)).astype(bf16)

    def multiply(g, table_ref):
        gout[g] = (
            jnp.dot(zcat[g], table_ref[:2 * cols, :], preferred_element_type=f32)
            + jnp.dot(zcat[g, :, :cols], table_ref[2 * cols:, :], preferred_element_type=f32))

    def total_rows(parts):
        return jnp.sum((parts[0] + parts[3]) + (parts[1] + parts[2]), axis=0, keepdims=True)

    def shared_rows(parts):
        line = (parts[0] + parts[3]) * 0.5 + (parts[1] + parts[2])
        return jnp.sum(jnp.where(on_edge, line * 0.5, line), axis=0, keepdims=True)

    def taken(g, slot):
        return [gout[g, pl.ds(pl.multiple_of(slot * rows + p * q, q), q), :] for p in range(4)]

    def divergence(g, k, base):
        multiply(g, div_ref)

        def third(slot, carry):
            m = base + slot
            if k < ITERS - 1:
                own = load(w, m)
            else:
                fg = load(z, m)
                zz = [u * v for u, v in zip(load(r2, m), load(invp, m))]
                own = [t * u + combo(SLOPES[:, a], fg)
                       for a, (t, u) in enumerate(zip(load2(mass), zz))]
            h = [u + v for u, v in zip(own, taken(g, slot))]
            return pack((k + 1) * groups + g, m, slot, h, carry)

        tops = lax.fori_loop(0, per, third, (zero, zero), unroll=UNROLL)
        send((k + 1) * groups + g, tops)

    def tally(it):
        def body(m, carry):
            rr, inv, t = load((r0, r1)[it], m), load(invp, m), load(w, m)
            zz = [u * v for u, v in zip(rr, inv)]
            uu = rr if it == 0 else [u + v for u, v in zip(rr, load(r0, m))]
            sums[2 * it, pl.ds(m, 1), :] = shared_rows([u * v for u, v in zip(uu, zz)])
            zt = [u * v for u, v in zip(zz, t)]
            edge = jnp.where(row_at == q - 1, zt[3], 0.0)
            sums[2 * it + 1, pl.ds(m, 1), :] = total_rows([zt[0], zt[1], zt[2], edge])
            return carry

        lax.fori_loop(0, modes, body, 0)

    for it in range(ITERS):
        for g in range(groups):
            base = g * per
            k = it * groups + g
            merged = arrive(k)
            if it < ITERS - 1:
                corner_step(it, g, k, merged)
            if it == 0 and g == 0:
                for e in range(2):
                    save(w, modes + e, assembled(k, modes + e, per + e, merged))

            def first(slot, carry, it=it, g=g, k=k, base=base, merged=merged):
                m = base + slot
                uu = assembled(k, m, slot, merged)
                if it == 0:
                    rr = uu
                    inv = [1.0 / (u + scale_ref[m] * v)
                           for u, v in zip(load(w, modes), load(w, modes + 1))]
                    save(invp, m, inv)
                    save(r0, m, rr)
                elif it == 1:
                    rr = [u - v for u, v in zip(uu, load(r0, m))]
                    inv = load(invp, m)
                    save(r1, m, rr)
                else:
                    rr = [2.0 * (u - v) - s for u, v, s in zip(uu, load(r1, m), load(r0, m))]
                    inv = load(invp, m)
                    save(r2, m, rr)
                zz = [u * v for u, v in zip(rr, inv)]
                fill(g, slot, zz)
                f = load2(flux)
                gx = [combo(SLOPES[a], zz) for a in range(4)]
                fg = [f[a] * gx[a] * scale_ref[m] for a in range(4)]
                mz = [u * v for u, v in zip(load2(mass), zz)]
                if it < ITERS - 1:
                    save(w, m, [mz[a] + combo(SLOPES[:, a], fg) for a in range(4)])
                else:
                    save(z, m, fg)
                    sums[2 * it, pl.ds(m, 1), :] = shared_rows([u * v for u, v in zip(uu, zz)])
                    sums[2 * it + 1, pl.ds(m, 1), :] = total_rows(
                        [u * v + s * t for u, v, s, t in zip(mz, zz, fg, gx)])
                return carry

            lax.fori_loop(0, per, first, 0, unroll=UNROLL)
            multiply(g, grad_ref)

            def weigh(slot, carry, it=it, g=g, base=base):
                grad = taken(g, slot)
                fill(g, slot, [u * v * scale_ref[base + slot] for u, v in zip(load2(flux), grad)])
                return carry

            def square(slot, carry, it=it, g=g, base=base):
                m, e = base + slot, 2 * it + 1
                more = [u * v * v for u, v in zip(load2(flux), taken(g, slot))]
                sums[e, pl.ds(m, 1), :] = (
                    sums[e, pl.ds(m, 1), :] + scale_ref[m] * total_rows(more))
                return carry

            if it < ITERS - 1:
                lax.fori_loop(0, per, weigh, 0, unroll=UNROLL)
                divergence(g, it, base)
            else:
                lax.fori_loop(0, per, square, 0, unroll=UNROLL)
        if it < ITERS - 1:
            tally(it)

    high = lax.broadcasted_iota(jnp.int32, (FIELD, LANES), 0)
    wide = lax.broadcasted_iota(jnp.int32, (FIELD, LANES), 1)
    picks = [(wide == e * FIELD + high) & (high < modes) for e in range(PRODUCTS)]
    spread = jnp.zeros((FIELD, LANES), f32)
    for e in range(PRODUCTS):
        part = jnp.sum(sums[e], axis=1, keepdims=True)
        spread = spread + jnp.where(picks[e], part, 0.0)
    line = jnp.sum(spread, axis=0, keepdims=True)

    def share(stage, line, tx, rx, peers):
        tx[...] = line
        rx[0] = line
        for j, where in enumerate(peers):
            pltpu.make_async_remote_copy(
                src_ref=tx, dst_ref=rx.at[j + 1], send_sem=atx_sem.at[stage],
                recv_sem=arx_sem.at[stage], device_id=where, device_id_type=MESH).start()

    def gather(stage, rx):
        got = rx.at[pl.ds(1, rx.shape[0] - 1)]
        pltpu.make_async_copy(got, got, arx_sem.at[stage]).wait()
        return jnp.sum(rx[...], axis=0)

    share(0, line, near_tx, near_rx, near)
    for g in range(groups):

        def weigh(slot, carry, g=g):
            fill(g, slot, [u * v * scale_ref[g * per + slot]
                           for u, v in zip(load2(flux), taken(g, slot))])
            return carry

        lax.fori_loop(0, per, weigh, 0, unroll=UNROLL)
        divergence(g, ITERS - 1, g * per)
    share(1, gather(0, near_rx), far_tx, far_rx, far)
    for g in range(groups):
        k = ITERS * groups + g
        merged = arrive(k)

        def last(slot, carry, g=g, k=k, merged=merged):
            m = g * per + slot
            save(u2, m, assembled(k, m, slot, merged))
            return carry

        lax.fori_loop(0, per, last, 0, unroll=UNROLL)

    total = gather(1, far_rx)
    pad = (high[:, :1] >= modes).astype(f32)
    n0, p00, p01, p11, p12, p22 = [
        jnp.broadcast_to(
            jnp.sum(jnp.where(pick, total, 0.0), axis=1, keepdims=True), (FIELD, LANES))
        for pick in picks]
    pad = jnp.broadcast_to(pad, (FIELD, LANES))
    p00, p11, p22 = p00 + pad, p11 + pad, p22 + 2.0 * pad
    b0 = n0
    b1 = p00 - n0
    b2 = 2.0 * (p01 - b1) - n0
    p02 = 2.0 * p11 - p00
    i0 = 1.0 / p00
    l1, l2 = p01 * i0, p02 * i0
    d1 = p11 - l1 * p01
    t2 = p12 - l2 * p01
    i1 = 1.0 / d1
    l3 = t2 * i1
    d2 = p22 - l2 * p02 - l3 * t2
    y1 = b1 - l1 * b0
    y2 = b2 - l2 * b0 - l3 * y1
    c2 = y2 / d2
    c1 = y1 * i1 - l3 * c2
    c0 = b0 * i0 - l1 * c1 - l2 * c2
    for e, c in enumerate((c0, c1, c2, 1.0 - c0 - 0.5 * c1, c0 + c1, 0.5 * c1)):
        coef[e] = c

    for k in range((ITERS + 1) * groups):
        for copy in halo_copies(k):
            copy.wait_send()
    for stage, rx in enumerate((near_rx, far_rx)):
        sent = rx.at[pl.ds(1, rx.shape[0] - 1)]
        pltpu.make_async_copy(sent, sent, atx_sem.at[stage]).wait()


def node_order(r0, r1, r2, u2, invp, coef, sol_ref, res_ref, sol_buf, res_buf, sem):
    modes, rows, cols = r0.shape
    q, tiles = rows // 4, cols // LANES

    def stores(m):
        return [
            pltpu.make_async_copy(
                buf.at[c, m], out.at[m, :, pl.ds(c * LANES, LANES)], sem.at[k, c, m])
            for k, (buf, out) in enumerate(((sol_buf, sol_ref), (res_buf, res_ref)))
            for c in range(tiles)
        ]

    def body(m, carry):
        c0, c1, c2, e0, e1, e2 = [coef[e, pl.ds(m, 1), :] for e in range(6)]
        for c in range(tiles):
            for p in range(4):
                at = (m, slice(p * q, (p + 1) * q), slice(c * LANES, (c + 1) * LANES))
                a0, a1, a2 = r0[at], r1[at], r2[at]
                sol_buf[c, m, pl.ds(p, q, stride=4), :] = invp[at] * (c0 * a0 + c1 * a1 + c2 * a2)
                res_buf[c, m, pl.ds(p, q, stride=4), :] = (
                    e0 * a0 - e1 * a1 - e2 * a2 - c2 * u2[at])
        for copy in stores(m):
            copy.start()
        return carry

    lax.fori_loop(0, modes, body, 0)

    def drain(m, carry):
        for copy in stores(m):
            copy.wait()
        return carry

    lax.fori_loop(0, modes, drain, 0)


def strided(refs, p, q):
    return jnp.concatenate([ref[pl.ds(p, q, stride=4), :] for ref in refs], axis=1)


def stack_table(table):
    top = table.astype(bf16)
    low = (table - top.astype(np.float32)).astype(bf16)
    return np.concatenate([top, top, low], axis=0)


def shards(nc, ns, forcing, metric, jacobian, mode_scale):
    modes, rows, cols = forcing.shape
    block = np.kron(np.eye(cols // 4), SLOPES).astype(np.float32)
    grad, div = stack_table(block.T), stack_table(block)
    q, tiles = rows // 4, cols // LANES
    groups = GROUPS if modes % GROUPS == 0 else 1
    per = modes // groups
    slots = -(-(per + 2) // 8) * 8
    vm = pl.BlockSpec(memory_space=pltpu.VMEM)
    hbm = pl.BlockSpec(memory_space=pltpu.HBM)
    rounds = (ITERS + 1) * groups
    ny, nz, nk, nx = planes(nc, ns)
    field = pltpu.VMEM((modes, rows, cols), f32)
    split = pltpu.VMEM((tiles, modes, rows, LANES), f32)
    table = pltpu.VMEM(grad.shape, bf16)
    line = pltpu.VMEM((1, LANES), f32)
    shape = jax.ShapeDtypeStruct(forcing.shape, f32)
    kept = pl.pallas_call(
        functools.partial(kernel, nc, ns, modes, groups),
        out_shape=[shape] * 5 + [jax.ShapeDtypeStruct((6, FIELD, LANES), f32)],
        in_specs=[hbm] * 6,
        out_specs=[vm] * 6,
        scratch_shapes=[
            field,
            pltpu.VMEM((modes + 2, rows, cols), f32),
            pltpu.VMEM((rows, cols), f32),
            pltpu.VMEM((rows, cols), f32),
            pltpu.VMEM((groups, per * rows, 2 * cols), bf16),
            pltpu.VMEM((groups, per * rows, cols), f32),
            pltpu.VMEM((PRODUCTS, FIELD, cols), f32),
            pltpu.VMEM((rounds, 2, slots, cols), f32),
            pltpu.VMEM((rounds, 2, slots, cols), f32),
            pltpu.VMEM((rounds, 2, q, LANES), f32),
            pltpu.VMEM((rounds, 2, q, LANES), f32),
            pltpu.VMEM((rounds, 8, LANES), f32),
            pltpu.VMEM((rounds, 4, 1, LANES), f32),
            line,
            pltpu.VMEM((ny * nk * nx, 1, LANES), f32),
            line,
            pltpu.VMEM((nz, 1, LANES), f32),
            split,
            pltpu.VMEM((2, tiles, rows, LANES), f32),
            table, table,
            pltpu.SMEM((modes,), f32),
            pltpu.SemaphoreType.DMA((rounds, 8)),
            pltpu.SemaphoreType.DMA((rounds, 8)),
            pltpu.SemaphoreType.DMA((2,)),
            pltpu.SemaphoreType.DMA((2,)),
            pltpu.SemaphoreType.DMA((3, tiles)),
            pltpu.SemaphoreType.DMA((3,)),
        ],
        compiler_params=pltpu.CompilerParams(
            collective_id=0, has_side_effects=True, vmem_limit_bytes=41943040),
    )(*[pltpu.with_memory_space_constraint(v, pltpu.HBM) for v in (mode_scale, forcing, metric, jacobian, jnp.asarray(grad), jnp.asarray(div))])
    return pl.pallas_call(
        node_order,
        out_shape=[shape] * 2,
        in_specs=[vm] * 6,
        out_specs=[hbm, hbm],
        scratch_shapes=[split, split, pltpu.SemaphoreType.DMA((2, tiles, modes))],
        compiler_params=pltpu.CompilerParams(vmem_limit_bytes=16 * 1024 * 1024),
    )(*kept)


def solution(mesh):
    placed = (P(None, "curve", "sub"), P("curve", "sub"), P("curve", "sub"), P())
    return jax.shard_map(
        functools.partial(shards, mesh.shape["curve"], mesh.shape["sub"]),
        mesh=mesh,
        in_specs=placed,
        out_specs=(P(None, "curve", "sub"), P(None, "curve", "sub")),
        check_vma=False,
    )
```

```python
import functools
import math

import jax
import jax.numpy as jnp
import numpy as np
from jax import lax
from jax.experimental import pallas as pl
from jax.experimental.pallas import tpu as pltpu
from jax.sharding import PartitionSpec as P

ITERS = 3
GROUPS = 2
UNROLL = True
MESH = pl.DeviceIdType.MESH
LANES = 128
f32 = jnp.float32
bf16 = jnp.bfloat16


def gll_tables():
    points = np.array([-1.0, -1.0 / math.sqrt(5.0), 1.0 / math.sqrt(5.0), 1.0])
    weights = np.array([1.0 / 6.0, 5.0 / 6.0, 5.0 / 6.0, 1.0 / 6.0])
    factor = np.array(
        [np.prod([points[j] - points[m] for m in range(4) if m != j]) for j in range(4)]
    )
    slopes = np.zeros((4, 4))
    for i in range(4):
        for j in range(4):
            if i != j:
                slopes[i, j] = factor[i] / (factor[j] * (points[i] - points[j]))
        slopes[i, i] = sum((1.0 / (points[i] - points[m]) for m in range(4) if m != i))
    return (slopes, weights)


SLOPES, WEIGHTS = gll_tables()


def combo(coefs, parts):
    total = None
    for c, v in zip(coefs, parts):
        if abs(c) < 1e-12:
            continue
        term = v * f32(c)
        total = term if total is None else total + term
    return total


PRODUCTS = 6
FIELD = 16


def planes(nc, ns):
    depth = 8 if nc % 16 == 0 else 2
    return nc // (2 * depth), depth, 2, ns


def kernel(
    nc, ns, modes, groups,
    scale_hbm, forcing_ref, metric_ref, jac_ref, grad_hbm, div_hbm,
    r0, r1, r2, u2, invp, coef,
    z, w, mass, flux, zcat, gout, sums,
    row_tx, row_rx, col_tx, col_rx, cor_tx, cor_rx, near_tx, near_rx, far_tx, far_rx,
    source, factors, grad_ref, div_ref, scale_ref,
    htx_sem, hrx_sem, atx_sem, arx_sem, in_sem, table_sem,
):
    rows, cols = metric_ref.shape
    q = rows // 4
    half = cols - LANES
    tiles = cols // LANES
    per = modes // groups
    slots = row_tx.shape[2]
    loads, sources = [], []
    for c in range(tiles):
        cut = pl.ds(c * LANES, LANES)
        loads += [
            pltpu.make_async_copy(jac_ref.at[:, cut], factors.at[0, c], in_sem.at[0, c]),
            pltpu.make_async_copy(metric_ref.at[:, cut], factors.at[1, c], in_sem.at[1, c]),
        ]
        sources.append(
            pltpu.make_async_copy(forcing_ref.at[:, :, cut], source.at[c], in_sem.at[2, c]))
    div_load = pltpu.make_async_copy(div_hbm, div_ref, table_sem.at[0])
    grad_load = pltpu.make_async_copy(grad_hbm, grad_ref, table_sem.at[1])
    scale_load = pltpu.make_async_copy(scale_hbm, scale_ref, table_sem.at[2])
    for copy in loads + sources + [div_load, scale_load, grad_load]:
        copy.start()

    me_c, me_s = lax.axis_index("curve"), lax.axis_index("sub")
    up, down = lax.rem(me_c + nc - 1, nc), lax.rem(me_c + 1, nc)
    left, right = lax.rem(me_s + ns - 1, ns), lax.rem(me_s + 1, ns)

    ny, nz, nk, nx = planes(nc, ns)
    core, chip = lax.rem(me_c, nk), me_c // nk
    at_z, at_y = lax.rem(chip, nz), chip // nz
    subs = [me_s if dx == 0 else lax.rem(me_s + dx, nx) for dx in range(nx)]
    ys = [at_y if dy == 0 else lax.rem(at_y + dy, ny) for dy in range(ny)]
    zs = [at_z if dz == 0 else lax.rem(at_z + dz, nz) for dz in range(nz)]

    def ring(step, size):
        return min(step, size - step)

    plane = sorted(
        [(dy, dk, dx) for dy in range(ny) for dk in range(nk) for dx in range(nx)][1:],
        key=lambda o: -(2 * ring(o[0], ny) + o[1] + 2 * ring(o[2], nx)))
    near = [((ys[dy] * nz + at_z) * nk + (1 - core if dk else core), subs[dx])
            for dy, dk, dx in plane]
    line_z = sorted(range(1, nz), key=lambda dz: -ring(dz, nz))
    far = [((at_y * nz + zs[dz]) * nk + core, me_s) for dz in line_z]

    barrier = pltpu.get_barrier_semaphore()
    greeted = [
        (up, left), (up, right), (down, left), (down, right)]
    greeted += [((ys[dy] * nz + at_z) * nk + core, me_s) for dy in range(1, ny)]
    greeted += [((at_y * nz + zs[dz]) * nk + core, me_s)
                for dz in sorted({1, 2, nz - 1, nz - 2} - {0, nz})]
    greeted += [(up, me_s), (down, me_s), (me_c, left), (me_c, right)]
    for where in greeted:
        pl.semaphore_signal(barrier, inc=1, device_id=where, device_id_type=MESH)

    lane_full = lax.broadcasted_iota(jnp.int32, (q, cols), 1)
    lane = lax.broadcasted_iota(jnp.int32, (q, LANES), 1)
    row_at = lax.broadcasted_iota(jnp.int32, (q, cols), 0)
    phase = lane_full % 4
    on_edge = (phase == 0) | (phase == 3)
    take_next = (phase == 3) & (lane_full != cols - 1)
    take_prev = (phase == 0) & (lane_full != 0)

    def load(ref, m):
        return [ref[m, p * q:(p + 1) * q, :] for p in range(4)]

    def save(ref, m, parts):
        for p in range(4):
            ref[m, p * q:(p + 1) * q, :] = parts[p]

    def load2(ref):
        return [ref[p * q:(p + 1) * q, :] for p in range(4)]

    def pack(k, m, slot, h, tops):
        lo, hi = tops
        row_tx[k, 0, pl.ds(slot, 1), :] = h[0][0:1, :]
        row_tx[k, 1, pl.ds(slot, 1), :] = h[3][q - 1:q, :]
        t0 = h[0] + jnp.where(row_at == 0, 0.0, pltpu.roll(h[3], 1, 0))
        t3 = h[3] + jnp.where(row_at == q - 1, 0.0, pltpu.roll(h[0], q - 1, 0))
        t = [t0, h[1], h[2], t3]
        save(w, m, t)
        for p in range(4):
            at = 4 * slot + p
            lo = jnp.where(lane == at, pltpu.roll(t[p][:, :LANES], at, 1), lo)
            hi = jnp.where(lane == at, pltpu.roll(t[p][:, half:], at + 1, 1), hi)
        return lo, hi

    def early(k):
        return groups <= k < ITERS * groups

    def halo_copies(k):
        if early(k):
            corners = [cor_tx.at[k, pl.ds(2 * e, 1)] for e in range(4)]
        else:
            corners = [col_tx.at[k, e % 2, pl.ds(0 if e < 2 else q - 1, 1)] for e in range(4)]
        plan = [
            (corners[0], cor_rx.at[k, 3], (up, left)),
            (corners[1], cor_rx.at[k, 2], (up, right)),
            (corners[2], cor_rx.at[k, 1], (down, left)),
            (corners[3], cor_rx.at[k, 0], (down, right)),
            (row_tx.at[k, 0], row_rx.at[k, 1], (up, me_s)),
            (row_tx.at[k, 1], row_rx.at[k, 0], (down, me_s)),
            (col_tx.at[k, 0], col_rx.at[k, 1], (me_c, left)),
            (col_tx.at[k, 1], col_rx.at[k, 0], (me_c, right)),
        ]
        return [
            pltpu.make_async_remote_copy(
                src_ref=src, dst_ref=dst, send_sem=htx_sem.at[k, e], recv_sem=hrx_sem.at[k, e],
                device_id=where, device_id_type=MESH)
            for e, (src, dst, where) in enumerate(plan)
        ]

    def send(k, tops):
        col_tx[k, 0], col_tx[k, 1] = tops
        for copy in halo_copies(k)[4 if early(k) else 0:]:
            copy.start()

    def arrive(k):
        for copy in halo_copies(k):
            copy.wait_recv()
        ph = lax.broadcasted_iota(jnp.int32, (1, LANES), 1) % 4
        edge_row = lax.broadcasted_iota(jnp.int32, (q, LANES), 0)
        merged = []
        for side in range(2):
            above, below = cor_rx[k, side], cor_rx[k, 2 + side]
            above = jnp.where(ph == 0, pltpu.roll(above, LANES - 3, 1), 0.0)
            below = jnp.where(ph == 3, pltpu.roll(below, 3, 1), 0.0)
            c = col_rx[k, side]
            c = c + jnp.where(edge_row == 0, above, 0.0) + jnp.where(edge_row == q - 1, below, 0.0)
            merged.append(c)
        return merged

    def assembled(k, m, slot, merged):
        t = load(w, m)
        t[0] = t[0] + jnp.where(row_at == 0, row_rx[k, 0, pl.ds(slot, 1), :], 0.0)
        t[3] = t[3] + jnp.where(row_at == q - 1, row_rx[k, 1, pl.ds(slot, 1), :], 0.0)
        out = []
        for p in range(4):
            at = 4 * slot + p
            c = t[p] + jnp.where(
                take_next, pltpu.roll(t[p], cols - 1, 1),
                jnp.where(take_prev, pltpu.roll(t[p], 1, 1), 0.0))
            a = jnp.where(lane == 0, pltpu.roll(merged[0], LANES - at, 1), 0.0)
            b = jnp.where(lane == LANES - 1, pltpu.roll(merged[1], LANES - 1 - at, 1), 0.0)
            pieces = [c[:, e * LANES:(e + 1) * LANES] for e in range(tiles)]
            pieces[0] = pieces[0] + a
            pieces[-1] = pieces[-1] + b
            out.append(jnp.concatenate(pieces, axis=1))
        return out

    edge_w, mid_w = f32(1.0 / 6.0), f32(5.0 / 6.0)
    col_w = jnp.where(on_edge, edge_w, mid_w)
    mw, fw = [], []
    for copy in loads:
        copy.wait()
    for p in range(4):
        grid_w = col_w * (edge_w if p in (0, 3) else mid_w)
        mw.append(strided([factors.at[0, c] for c in range(tiles)], p, q) * grid_w)
        fw.append(strided([factors.at[1, c] for c in range(tiles)], p, q) * grid_w)
        mass[p * q:(p + 1) * q, :] = mw[p]
        flux[p * q:(p + 1) * q, :] = fw[p]
    zero = jnp.zeros((q, LANES), f32)
    tops = pack(0, modes, per, mw, (zero, zero))
    div_load.wait()
    table = div_ref[:cols, :].astype(f32) + div_ref[2 * cols:, :].astype(f32)
    by_cols = jnp.dot(flux[...], table * table, precision=lax.Precision.HIGHEST,
                      preferred_element_type=f32)
    squared = SLOPES * SLOPES
    lap = [combo(squared[:, a], fw) + by_cols[a * q:(a + 1) * q, :] for a in range(4)]
    tops = pack(0, modes + 1, per + 1, lap, tops)
    for copy in sources:
        copy.wait()
    for g in range(groups):

        def start_body(slot, carry, g=g):
            m = g * per + slot
            h = [strided([source.at[c, m] for c in range(tiles)], p, q)
                 * mass[p * q:(p + 1) * q, :] for p in range(4)]
            return pack(g, m, slot, h, carry)

        tops = lax.fori_loop(0, per, start_body, tops if g == 0 else (zero, zero), unroll=UNROLL)
        if g == 0:
            pl.semaphore_wait(barrier, len(greeted))
        send(g, tops)
    scale_load.wait()
    grad_load.wait()

    at_lane = lax.broadcasted_iota(jnp.int32, (1, LANES), 1)
    of_four = at_lane % 4
    tall = lax.broadcasted_iota(jnp.int32, (slots, LANES), 0)
    flat = lax.broadcasted_iota(jnp.int32, (slots, LANES), 1)
    low_half = tall < 4

    def coefs(values):
        line = jnp.zeros((1, LANES), f32)
        for e, value in enumerate(values):
            line = jnp.where(of_four == e, f32(value), line)
        return line

    def corner_weights(g):
        scale = jnp.zeros((1, LANES), f32)
        for slot in range(per):
            scale = jnp.where(at_lane // 4 == slot, scale_ref[g * per + slot], scale)
        lines = []
        for tb in range(2):
            er, cr = (0, 0) if tb == 0 else (q - 1, 3)
            for side in range(2):
                cc, edge, start = (0, 0, 0) if side == 0 else (3, cols - 1, cols - 4)
                sx = jnp.zeros((1, LANES), f32)
                sy = jnp.zeros((1, LANES), f32)
                own = jnp.zeros((1, 1), f32)
                for e in range(4):
                    fx = flux[e * q + er:e * q + er + 1, edge:edge + 1]
                    fy = flux[cr * q + er:cr * q + er + 1, start + e:start + e + 1]
                    sx = sx + fx * coefs(SLOPES[e, cr] * SLOPES[e])
                    sy = sy + fy * coefs(SLOPES[e, cc] * SLOPES[e])
                    own = own + fy * f32(SLOPES[e, cc] * SLOPES[e, cc])
                here = mass[cr * q + er:cr * q + er + 1, edge:edge + 1]
                lines += [
                    scale * sx + jnp.where(of_four == cr, here + scale * own, 0.0),
                    jnp.where(of_four == cc, 0.0, scale * sy)]
        return scale, jnp.concatenate(lines, axis=0)

    def gathered_rows(x):
        left = x[:, :LANES]
        left = left + jnp.where(flat == 3, pltpu.roll(left, LANES - 1, 1), 0.0)
        right = x[:, half:]
        right = right + jnp.where(flat == LANES - 4, pltpu.roll(right, 1, 1), 0.0)
        left = pltpu.roll(jnp.where(flat < 4, left, 0.0), 0, 1, stride=4, stride_axis=0)
        right = pltpu.roll(
            jnp.where(flat >= LANES - 4, right, 0.0), 4, 1, stride=4, stride_axis=0)
        return [jnp.sum(v, axis=0, keepdims=True) for v in (left, right)]

    def corner_values(k, merged):
        lines = []
        for tb in range(2):
            er, cr = (0, 0) if tb == 0 else (q - 1, 3)
            halo = row_rx[k, tb]
            rows_here = gathered_rows(row_tx[k, tb] + halo)
            for side in range(2):
                edge = 0 if side == 0 else cols - 1
                place = flat == 4 * tall + cr
                extra = jnp.sum(
                    jnp.where(place, halo[:, edge:edge + 1], 0.0), axis=0, keepdims=True)
                col = col_tx[k, side, er:er + 1, :] + merged[side][er:er + 1, :] + extra
                lines += [col, rows_here[side]]
        return jnp.concatenate(lines, axis=0)

    def send_corners(k, weights, v):
        h = weights * v
        fore = h + pltpu.roll(h, LANES - 1, 1)
        fore = fore + pltpu.roll(fore, LANES - 2, 1)
        back = h + pltpu.roll(h, 1, 1)
        back = back + pltpu.roll(back, 2, 1)
        h = jnp.where(low_half, fore, back)
        cor_tx[k] = h + pltpu.roll(h, slots - 1, 0)
        for copy in halo_copies(k)[:4]:
            copy.start()

    def repeat(x, slot):
        x = jnp.where(flat // 4 == slot, x, 0.0)
        x = pltpu.roll(x, LANES - 4 * slot, 1)
        for step in (4, 8, 16):
            x = x + pltpu.roll(x, step, 1)
        return x

    assert slots == 8
    corner = [corner_weights(g) for g in range(groups)]
    corner_r, corner_inv, shared_diag = [None] * groups, [None] * groups, []

    def corner_step(it, g, k, merged):
        u = corner_values(k, merged)
        scale, weights = corner[g]
        if it == 0:
            if g == 0:
                shared_diag.extend([repeat(u, per), repeat(u, per + 1)])
            used = flat < 4 * per
            u = jnp.where(used, u, 0.0)
            corner_r[g] = u
            corner_inv[g] = jnp.where(used, 1.0 / jnp.where(
                used, shared_diag[0] + scale * shared_diag[1], 1.0), 0.0)
            r = u
        else:
            r = jnp.where(flat < 4 * per, u, 0.0) - corner_r[g]
        send_corners(k + groups, weights, r * corner_inv[g])

    def fill(g, slot, parts):
        v = jnp.concatenate(parts, axis=0)
        top = v.astype(bf16)
        at = pl.ds(pl.multiple_of(slot * rows, rows), rows)
        zcat[g, at, :cols] = top
        zcat[g, at, cols:] = (v - top.astype(f32)).astype(bf16)

    def multiply(g, table_ref):
        gout[...] = (
            jnp.dot(zcat[g], table_ref[:2 * cols, :], preferred_element_type=f32)
            + jnp.dot(zcat[g, :, :cols], table_ref[2 * cols:, :], preferred_element_type=f32))

    def total_rows(parts):
        return jnp.sum((parts[0] + parts[3]) + (parts[1] + parts[2]), axis=0, keepdims=True)

    def shared_rows(parts):
        line = (parts[0] + parts[3]) * 0.5 + (parts[1] + parts[2])
        return jnp.sum(jnp.where(on_edge, line * 0.5, line), axis=0, keepdims=True)

    def finish(g, k, base):
        multiply(g, div_ref)

        def third(slot, carry):
            m = base + slot
            h = [u + gout[pl.ds(pl.multiple_of(slot * rows + p * q, q), q), :]
                 for p, u in enumerate(load(w, m))]
            if k < ITERS - 1:
                zh = [u * v for u, v in zip(load(z, m), h)]
                sums[2 * k + 1, pl.ds(m, 1), :] = total_rows(zh)
            return pack((k + 1) * groups + g, m, slot, h, carry)

        tops = lax.fori_loop(0, per, third, (zero, zero), unroll=UNROLL)
        send((k + 1) * groups + g, tops)

    for it in range(ITERS):
        for g in range(groups):
            base = g * per
            k = it * groups + g
            merged = arrive(k)
            if it < ITERS - 1:
                corner_step(it, g, k, merged)
            if it == 0 and g == 0:
                for e in range(2):
                    save(w, modes + e, assembled(k, modes + e, per + e, merged))

            def first(slot, carry, it=it, g=g, k=k, base=base, merged=merged):
                m = base + slot
                uu = assembled(k, m, slot, merged)
                if it == 0:
                    rr = uu
                    inv = [1.0 / (u + scale_ref[m] * v)
                           for u, v in zip(load(w, modes), load(w, modes + 1))]
                    save(invp, m, inv)
                    save(r0, m, rr)
                elif it == 1:
                    rr = [u - v for u, v in zip(uu, load(r0, m))]
                    inv = load(invp, m)
                    save(r1, m, rr)
                else:
                    rr = [2.0 * (u - v) - s for u, v, s in zip(uu, load(r1, m), load(r0, m))]
                    inv = load(invp, m)
                    save(r2, m, rr)
                zz = [u * v for u, v in zip(rr, inv)]
                fill(g, slot, zz)
                sums[2 * it, pl.ds(m, 1), :] = shared_rows([u * v for u, v in zip(uu, zz)])
                f = load2(flux)
                gx = [combo(SLOPES[a], zz) for a in range(4)]
                fg = [f[a] * gx[a] * scale_ref[m] for a in range(4)]
                mz = [u * v for u, v in zip(load2(mass), zz)]
                if it < ITERS - 1:
                    save(z, m, zz)
                else:
                    sums[2 * it + 1, pl.ds(m, 1), :] = total_rows(
                        [u * v + s * t for u, v, s, t in zip(mz, zz, fg, gx)])
                save(w, m, [mz[a] + combo(SLOPES[:, a], fg) for a in range(4)])
                return carry

            lax.fori_loop(0, per, first, 0, unroll=UNROLL)
            multiply(g, grad_ref)

            def second(slot, carry, it=it, g=g, base=base):
                m = base + slot
                grad = [gout[pl.ds(pl.multiple_of(slot * rows + p * q, q), q), :]
                        for p in range(4)]
                fy = [u * v * scale_ref[m] for u, v in zip(load2(flux), grad)]
                if it == ITERS - 1:
                    e = 2 * it + 1
                    sums[e, pl.ds(m, 1), :] = sums[e, pl.ds(m, 1), :] + total_rows(
                        [u * v for u, v in zip(fy, grad)])
                fill(g, slot, fy)
                return carry

            lax.fori_loop(0, per, second, 0, unroll=UNROLL)
            if it < ITERS - 1:
                finish(g, it, base)

    high = lax.broadcasted_iota(jnp.int32, (FIELD, LANES), 0)
    wide = lax.broadcasted_iota(jnp.int32, (FIELD, LANES), 1)
    picks = [(wide == e * FIELD + high) & (high < modes) for e in range(PRODUCTS)]
    spread = jnp.zeros((FIELD, LANES), f32)
    for e in range(PRODUCTS):
        part = jnp.sum(sums[e], axis=1, keepdims=True)
        spread = spread + jnp.where(picks[e], part, 0.0)
    line = jnp.sum(spread, axis=0, keepdims=True)

    def share(stage, line, tx, rx, peers):
        tx[...] = line
        rx[0] = line
        for j, where in enumerate(peers):
            pltpu.make_async_remote_copy(
                src_ref=tx, dst_ref=rx.at[j + 1], send_sem=atx_sem.at[stage],
                recv_sem=arx_sem.at[stage], device_id=where, device_id_type=MESH).start()

    def gather(stage, rx):
        got = rx.at[pl.ds(1, rx.shape[0] - 1)]
        pltpu.make_async_copy(got, got, arx_sem.at[stage]).wait()
        return jnp.sum(rx[...], axis=0)

    share(0, line, near_tx, near_rx, near)
    for g in range(groups):
        finish(g, ITERS - 1, g * per)
    share(1, gather(0, near_rx), far_tx, far_rx, far)
    for g in range(groups):
        k = ITERS * groups + g
        merged = arrive(k)

        def last(slot, carry, g=g, k=k, merged=merged):
            m = g * per + slot
            save(u2, m, assembled(k, m, slot, merged))
            return carry

        lax.fori_loop(0, per, last, 0, unroll=UNROLL)

    total = gather(1, far_rx)
    pad = (high[:, :1] >= modes).astype(f32)
    n0, p00, p01, p11, p12, p22 = [
        jnp.broadcast_to(
            jnp.sum(jnp.where(pick, total, 0.0), axis=1, keepdims=True), (FIELD, LANES))
        for pick in picks]
    pad = jnp.broadcast_to(pad, (FIELD, LANES))
    p00, p11, p22 = p00 + pad, p11 + pad, p22 + 2.0 * pad
    b0 = n0
    b1 = p00 - n0
    b2 = 2.0 * (p01 - b1) - n0
    p02 = 2.0 * p11 - p00
    i0 = 1.0 / p00
    l1, l2 = p01 * i0, p02 * i0
    d1 = p11 - l1 * p01
    t2 = p12 - l2 * p01
    i1 = 1.0 / d1
    l3 = t2 * i1
    d2 = p22 - l2 * p02 - l3 * t2
    y1 = b1 - l1 * b0
    y2 = b2 - l2 * b0 - l3 * y1
    c2 = y2 / d2
    c1 = y1 * i1 - l3 * c2
    c0 = b0 * i0 - l1 * c1 - l2 * c2
    for e, c in enumerate((c0, c1, c2, 1.0 - c0 - 0.5 * c1, c0 + c1, 0.5 * c1)):
        coef[e] = c

    for k in range((ITERS + 1) * groups):
        for copy in halo_copies(k):
            copy.wait_send()
    for stage, rx in enumerate((near_rx, far_rx)):
        sent = rx.at[pl.ds(1, rx.shape[0] - 1)]
        pltpu.make_async_copy(sent, sent, atx_sem.at[stage]).wait()


def node_order(r0, r1, r2, u2, invp, coef, sol_ref, res_ref, sol_buf, res_buf, sem):
    modes, rows, cols = r0.shape
    q, tiles = rows // 4, cols // LANES

    def stores(m):
        return [
            pltpu.make_async_copy(
                buf.at[c, m], out.at[m, :, pl.ds(c * LANES, LANES)], sem.at[k, c, m])
            for k, (buf, out) in enumerate(((sol_buf, sol_ref), (res_buf, res_ref)))
            for c in range(tiles)
        ]

    def body(m, carry):
        c0, c1, c2, e0, e1, e2 = [coef[e, pl.ds(m, 1), :] for e in range(6)]
        for c in range(tiles):
            for p in range(4):
                at = (m, slice(p * q, (p + 1) * q), slice(c * LANES, (c + 1) * LANES))
                a0, a1, a2 = r0[at], r1[at], r2[at]
                sol_buf[c, m, pl.ds(p, q, stride=4), :] = invp[at] * (c0 * a0 + c1 * a1 + c2 * a2)
                res_buf[c, m, pl.ds(p, q, stride=4), :] = (
                    e0 * a0 - e1 * a1 - e2 * a2 - c2 * u2[at])
        for copy in stores(m):
            copy.start()
        return carry

    lax.fori_loop(0, modes, body, 0)

    def drain(m, carry):
        for copy in stores(m):
            copy.wait()
        return carry

    lax.fori_loop(0, modes, drain, 0)


def strided(refs, p, q):
    return jnp.concatenate([ref[pl.ds(p, q, stride=4), :] for ref in refs], axis=1)


def stack_table(table):
    top = table.astype(bf16)
    low = (table - top.astype(np.float32)).astype(bf16)
    return np.concatenate([top, top, low], axis=0)


def shards(nc, ns, forcing, metric, jacobian, mode_scale):
    modes, rows, cols = forcing.shape
    block = np.kron(np.eye(cols // 4), SLOPES).astype(np.float32)
    grad, div = stack_table(block.T), stack_table(block)
    q, tiles = rows // 4, cols // LANES
    groups = GROUPS if modes % GROUPS == 0 else 1
    per = modes // groups
    slots = -(-(per + 2) // 8) * 8
    vm = pl.BlockSpec(memory_space=pltpu.VMEM)
    hbm = pl.BlockSpec(memory_space=pltpu.HBM)
    rounds = (ITERS + 1) * groups
    ny, nz, nk, nx = planes(nc, ns)
    field = pltpu.VMEM((modes, rows, cols), f32)
    split = pltpu.VMEM((tiles, modes, rows, LANES), f32)
    table = pltpu.VMEM(grad.shape, bf16)
    line = pltpu.VMEM((1, LANES), f32)
    shape = jax.ShapeDtypeStruct(forcing.shape, f32)
    kept = pl.pallas_call(
        functools.partial(kernel, nc, ns, modes, groups),
        out_shape=[shape] * 5 + [jax.ShapeDtypeStruct((6, FIELD, LANES), f32)],
        in_specs=[hbm] * 6,
        out_specs=[vm] * 6,
        scratch_shapes=[
            field,
            pltpu.VMEM((modes + 2, rows, cols), f32),
            pltpu.VMEM((rows, cols), f32),
            pltpu.VMEM((rows, cols), f32),
            pltpu.VMEM((groups, per * rows, 2 * cols), bf16),
            pltpu.VMEM((per * rows, cols), f32),
            pltpu.VMEM((PRODUCTS, FIELD, cols), f32),
            pltpu.VMEM((rounds, 2, slots, cols), f32),
            pltpu.VMEM((rounds, 2, slots, cols), f32),
            pltpu.VMEM((rounds, 2, q, LANES), f32),
            pltpu.VMEM((rounds, 2, q, LANES), f32),
            pltpu.VMEM((rounds, 8, LANES), f32),
            pltpu.VMEM((rounds, 4, 1, LANES), f32),
            line,
            pltpu.VMEM((ny * nk * nx, 1, LANES), f32),
            line,
            pltpu.VMEM((nz, 1, LANES), f32),
            split,
            pltpu.VMEM((2, tiles, rows, LANES), f32),
            table, table,
            pltpu.SMEM((modes,), f32),
            pltpu.SemaphoreType.DMA((rounds, 8)),
            pltpu.SemaphoreType.DMA((rounds, 8)),
            pltpu.SemaphoreType.DMA((2,)),
            pltpu.SemaphoreType.DMA((2,)),
            pltpu.SemaphoreType.DMA((3, tiles)),
            pltpu.SemaphoreType.DMA((3,)),
        ],
        compiler_params=pltpu.CompilerParams(
            collective_id=0, has_side_effects=True, vmem_limit_bytes=41943040),
    )(*[pltpu.with_memory_space_constraint(v, pltpu.HBM) for v in (mode_scale, forcing, metric, jacobian, jnp.asarray(grad), jnp.asarray(div))])
    return pl.pallas_call(
        node_order,
        out_shape=[shape] * 2,
        in_specs=[vm] * 6,
        out_specs=[hbm, hbm],
        scratch_shapes=[split, split, pltpu.SemaphoreType.DMA((2, tiles, modes))],
        compiler_params=pltpu.CompilerParams(vmem_limit_bytes=16 * 1024 * 1024),
    )(*kept)


def solution(mesh):
    placed = (P(None, "curve", "sub"), P("curve", "sub"), P("curve", "sub"), P())
    return jax.shard_map(
        functools.partial(shards, mesh.shape["curve"], mesh.shape["sub"]),
        mesh=mesh,
        in_specs=placed,
        out_specs=(P(None, "curve", "sub"), P(None, "curve", "sub")),
        check_vma=False,
    )
```

```python
import functools
import math

import jax
import jax.numpy as jnp
import numpy as np
from jax import lax
from jax.experimental import pallas as pl
from jax.experimental.pallas import tpu as pltpu
from jax.sharding import PartitionSpec as P

ITERS = 3
GROUPS = 2
UNROLL = True
MESH = pl.DeviceIdType.MESH
LANES = 128
f32 = jnp.float32
bf16 = jnp.bfloat16


def gll_tables():
    points = np.array([-1.0, -1.0 / math.sqrt(5.0), 1.0 / math.sqrt(5.0), 1.0])
    weights = np.array([1.0 / 6.0, 5.0 / 6.0, 5.0 / 6.0, 1.0 / 6.0])
    factor = np.array(
        [np.prod([points[j] - points[m] for m in range(4) if m != j]) for j in range(4)]
    )
    slopes = np.zeros((4, 4))
    for i in range(4):
        for j in range(4):
            if i != j:
                slopes[i, j] = factor[i] / (factor[j] * (points[i] - points[j]))
        slopes[i, i] = sum((1.0 / (points[i] - points[m]) for m in range(4) if m != i))
    return (slopes, weights)


SLOPES, WEIGHTS = gll_tables()


def combo(coefs, parts):
    total = None
    for c, v in zip(coefs, parts):
        if abs(c) < 1e-12:
            continue
        term = v * f32(c)
        total = term if total is None else total + term
    return total


PRODUCTS = 6
FIELD = 16


def planes(nc, ns):
    depth = 8 if nc % 16 == 0 else 2
    return nc // (2 * depth), depth, 2, ns


def landed(ref, sem):
    pltpu.make_async_copy(ref, ref, sem).wait()


def kernel(
    nc, ns, modes, groups,
    scale_hbm, forcing_ref, metric_ref, jac_ref, grad_hbm, div_hbm,
    r0, r1, r2, u2, invp, coef,
    z, w, mass, flux, zcat, gout, sums,
    row_tx, row_rx, col_tx, col_rx, cor_tx, cor_rx, near_tx, near_rx, far_tx, far_rx,
    source, factors, gauge, grad_ref, div_ref, scale_ref,
    htx_sem, hrx_sem, atx_sem, arx_sem, in_sem, table_sem,
):
    rows, cols = metric_ref.shape
    q = rows // 4
    half = cols - LANES
    tiles = cols // LANES
    per = modes // groups
    slots = row_tx.shape[2]
    loads, sources = [], []
    for c in range(tiles):
        cut = pl.ds(c * LANES, LANES)
        loads += [
            pltpu.make_async_copy(jac_ref.at[:, cut], factors.at[0, c], in_sem.at[0]),
            pltpu.make_async_copy(metric_ref.at[:, cut], factors.at[1, c], in_sem.at[0]),
        ]
        sources.append(
            pltpu.make_async_copy(forcing_ref.at[:, :, cut], source.at[c], in_sem.at[1]))
    div_load = pltpu.make_async_copy(div_hbm, div_ref, table_sem.at[0])
    grad_load = pltpu.make_async_copy(grad_hbm, grad_ref, table_sem.at[1])
    scale_load = pltpu.make_async_copy(scale_hbm, scale_ref, table_sem.at[2])
    for copy in loads + sources + [div_load, scale_load, grad_load]:
        copy.start()

    me_c, me_s = lax.axis_index("curve"), lax.axis_index("sub")
    up, down = lax.rem(me_c + nc - 1, nc), lax.rem(me_c + 1, nc)
    left, right = lax.rem(me_s + ns - 1, ns), lax.rem(me_s + 1, ns)

    ny, nz, nk, nx = planes(nc, ns)
    core, chip = lax.rem(me_c, nk), me_c // nk
    at_z, at_y = lax.rem(chip, nz), chip // nz
    subs = [me_s if dx == 0 else lax.rem(me_s + dx, nx) for dx in range(nx)]
    ys = [at_y if dy == 0 else lax.rem(at_y + dy, ny) for dy in range(ny)]
    zs = [at_z if dz == 0 else lax.rem(at_z + dz, nz) for dz in range(nz)]

    def ring(step, size):
        return min(step, size - step)

    plane = sorted(
        [(dy, dk, dx) for dy in range(ny) for dk in range(nk) for dx in range(nx)][1:],
        key=lambda o: -(2 * ring(o[0], ny) + o[1] + 2 * ring(o[2], nx)))
    near = [((ys[dy] * nz + at_z) * nk + (1 - core if dk else core), subs[dx])
            for dy, dk, dx in plane]
    line_z = sorted(range(1, nz), key=lambda dz: -ring(dz, nz))
    far = [((at_y * nz + zs[dz]) * nk + core, me_s) for dz in line_z]

    barrier = pltpu.get_barrier_semaphore()
    greeted = [
        (up, left), (up, right), (down, left), (down, right)]
    greeted += [((ys[dy] * nz + at_z) * nk + core, me_s) for dy in range(1, ny)]
    greeted += [((at_y * nz + zs[dz]) * nk + core, me_s)
                for dz in sorted({1, 2, nz - 1, nz - 2} - {0, nz})]
    greeted += [(up, me_s), (down, me_s), (me_c, left), (me_c, right)]
    for where in greeted:
        pl.semaphore_signal(barrier, inc=1, device_id=where, device_id_type=MESH)

    lane_full = lax.broadcasted_iota(jnp.int32, (q, cols), 1)
    lane = lax.broadcasted_iota(jnp.int32, (q, LANES), 1)
    row_at = lax.broadcasted_iota(jnp.int32, (q, cols), 0)
    phase = lane_full % 4
    on_edge = (phase == 0) | (phase == 3)
    take_next = (phase == 3) & (lane_full != cols - 1)
    take_prev = (phase == 0) & (lane_full != 0)

    def load(ref, m):
        return [ref[m, p * q:(p + 1) * q, :] for p in range(4)]

    def save(ref, m, parts):
        for p in range(4):
            ref[m, p * q:(p + 1) * q, :] = parts[p]

    def load2(ref):
        return [ref[p * q:(p + 1) * q, :] for p in range(4)]

    def pack(k, m, slot, h, tops):
        lo, hi = tops
        row_tx[k, 0, pl.ds(slot, 1), :] = h[0][0:1, :]
        row_tx[k, 1, pl.ds(slot, 1), :] = h[3][q - 1:q, :]
        t0 = h[0] + jnp.where(row_at == 0, 0.0, pltpu.roll(h[3], 1, 0))
        t3 = h[3] + jnp.where(row_at == q - 1, 0.0, pltpu.roll(h[0], q - 1, 0))
        t = [t0, h[1], h[2], t3]
        save(w, m, t)
        for p in range(4):
            at = 4 * slot + p
            lo = jnp.where(lane == at, pltpu.roll(t[p][:, :LANES], at, 1), lo)
            hi = jnp.where(lane == at, pltpu.roll(t[p][:, half:], at + 1, 1), hi)
        return lo, hi

    def early(k):
        return groups <= k < ITERS * groups

    def halo_copies(k):
        if early(k):
            corners = [cor_tx.at[k, pl.ds(2 * e, 1)] for e in range(4)]
        else:
            corners = [col_tx.at[k, e % 2, pl.ds(0 if e < 2 else q - 1, 1)] for e in range(4)]
        plan = [
            (corners[0], cor_rx.at[k, 3], (up, left)),
            (corners[1], cor_rx.at[k, 2], (up, right)),
            (corners[2], cor_rx.at[k, 1], (down, left)),
            (corners[3], cor_rx.at[k, 0], (down, right)),
            (row_tx.at[k, 0], row_rx.at[k, 1], (up, me_s)),
            (row_tx.at[k, 1], row_rx.at[k, 0], (down, me_s)),
            (col_tx.at[k, 0], col_rx.at[k, 1], (me_c, left)),
            (col_tx.at[k, 1], col_rx.at[k, 0], (me_c, right)),
        ]
        return [
            pltpu.make_async_remote_copy(
                src_ref=src, dst_ref=dst, send_sem=htx_sem.at[k], recv_sem=hrx_sem.at[k],
                device_id=where, device_id_type=MESH)
            for src, dst, where in plan
        ]

    def send(k, tops):
        col_tx[k, 0], col_tx[k, 1] = tops
        for copy in halo_copies(k)[4 if early(k) else 0:]:
            copy.start()

    def arrive(k):
        landed(gauge, hrx_sem.at[k])
        ph = lax.broadcasted_iota(jnp.int32, (1, LANES), 1) % 4
        edge_row = lax.broadcasted_iota(jnp.int32, (q, LANES), 0)
        merged = []
        for side in range(2):
            above, below = cor_rx[k, side], cor_rx[k, 2 + side]
            above = jnp.where(ph == 0, pltpu.roll(above, LANES - 3, 1), 0.0)
            below = jnp.where(ph == 3, pltpu.roll(below, 3, 1), 0.0)
            c = col_rx[k, side]
            c = c + jnp.where(edge_row == 0, above, 0.0) + jnp.where(edge_row == q - 1, below, 0.0)
            merged.append(c)
        return merged

    def assembled(k, m, slot, merged):
        t = load(w, m)
        t[0] = t[0] + jnp.where(row_at == 0, row_rx[k, 0, pl.ds(slot, 1), :], 0.0)
        t[3] = t[3] + jnp.where(row_at == q - 1, row_rx[k, 1, pl.ds(slot, 1), :], 0.0)
        out = []
        for p in range(4):
            at = 4 * slot + p
            c = t[p] + jnp.where(
                take_next, pltpu.roll(t[p], cols - 1, 1),
                jnp.where(take_prev, pltpu.roll(t[p], 1, 1), 0.0))
            a = jnp.where(lane == 0, pltpu.roll(merged[0], LANES - at, 1), 0.0)
            b = jnp.where(lane == LANES - 1, pltpu.roll(merged[1], LANES - 1 - at, 1), 0.0)
            pieces = [c[:, e * LANES:(e + 1) * LANES] for e in range(tiles)]
            pieces[0] = pieces[0] + a
            pieces[-1] = pieces[-1] + b
            out.append(jnp.concatenate(pieces, axis=1))
        return out

    edge_w, mid_w = f32(1.0 / 6.0), f32(5.0 / 6.0)
    col_w = jnp.where(on_edge, edge_w, mid_w)
    mw, fw = [], []
    landed(factors, in_sem.at[0])
    for p in range(4):
        grid_w = col_w * (edge_w if p in (0, 3) else mid_w)
        mw.append(strided([factors.at[0, c] for c in range(tiles)], p, q) * grid_w)
        fw.append(strided([factors.at[1, c] for c in range(tiles)], p, q) * grid_w)
        mass[p * q:(p + 1) * q, :] = mw[p]
        flux[p * q:(p + 1) * q, :] = fw[p]
    zero = jnp.zeros((q, LANES), f32)
    tops = pack(0, modes, per, mw, (zero, zero))
    div_load.wait()
    table = div_ref[:cols, :].astype(f32) + div_ref[2 * cols:, :].astype(f32)
    by_cols = jnp.dot(flux[...], table * table, precision=lax.Precision.HIGHEST,
                      preferred_element_type=f32)
    squared = SLOPES * SLOPES
    lap = [combo(squared[:, a], fw) + by_cols[a * q:(a + 1) * q, :] for a in range(4)]
    tops = pack(0, modes + 1, per + 1, lap, tops)
    landed(source, in_sem.at[1])
    for g in range(groups):

        def start_body(slot, carry, g=g):
            m = g * per + slot
            h = [strided([source.at[c, m] for c in range(tiles)], p, q)
                 * mass[p * q:(p + 1) * q, :] for p in range(4)]
            return pack(g, m, slot, h, carry)

        tops = lax.fori_loop(0, per, start_body, tops if g == 0 else (zero, zero), unroll=UNROLL)
        if g == 0:
            pl.semaphore_wait(barrier, len(greeted))
        send(g, tops)
    scale_load.wait()
    grad_load.wait()

    at_lane = lax.broadcasted_iota(jnp.int32, (1, LANES), 1)
    of_four = at_lane % 4
    tall = lax.broadcasted_iota(jnp.int32, (slots, LANES), 0)
    flat = lax.broadcasted_iota(jnp.int32, (slots, LANES), 1)
    low_half = tall < 4

    def coefs(values):
        line = jnp.zeros((1, LANES), f32)
        for e, value in enumerate(values):
            line = jnp.where(of_four == e, f32(value), line)
        return line

    def corner_weights(g):
        scale = jnp.zeros((1, LANES), f32)
        for slot in range(per):
            scale = jnp.where(at_lane // 4 == slot, scale_ref[g * per + slot], scale)
        lines = []
        for tb in range(2):
            er, cr = (0, 0) if tb == 0 else (q - 1, 3)
            for side in range(2):
                cc, edge, start = (0, 0, 0) if side == 0 else (3, cols - 1, cols - 4)
                sx = jnp.zeros((1, LANES), f32)
                sy = jnp.zeros((1, LANES), f32)
                own = jnp.zeros((1, 1), f32)
                for e in range(4):
                    fx = flux[e * q + er:e * q + er + 1, edge:edge + 1]
                    fy = flux[cr * q + er:cr * q + er + 1, start + e:start + e + 1]
                    sx = sx + fx * coefs(SLOPES[e, cr] * SLOPES[e])
                    sy = sy + fy * coefs(SLOPES[e, cc] * SLOPES[e])
                    own = own + fy * f32(SLOPES[e, cc] * SLOPES[e, cc])
                here = mass[cr * q + er:cr * q + er + 1, edge:edge + 1]
                lines += [
                    scale * sx + jnp.where(of_four == cr, here + scale * own, 0.0),
                    jnp.where(of_four == cc, 0.0, scale * sy)]
        return scale, jnp.concatenate(lines, axis=0)

    def gathered_rows(x):
        left = x[:, :LANES]
        left = left + jnp.where(flat == 3, pltpu.roll(left, LANES - 1, 1), 0.0)
        right = x[:, half:]
        right = right + jnp.where(flat == LANES - 4, pltpu.roll(right, 1, 1), 0.0)
        left = pltpu.roll(jnp.where(flat < 4, left, 0.0), 0, 1, stride=4, stride_axis=0)
        right = pltpu.roll(
            jnp.where(flat >= LANES - 4, right, 0.0), 4, 1, stride=4, stride_axis=0)
        return [jnp.sum(v, axis=0, keepdims=True) for v in (left, right)]

    def corner_values(k, merged):
        lines = []
        for tb in range(2):
            er, cr = (0, 0) if tb == 0 else (q - 1, 3)
            halo = row_rx[k, tb]
            rows_here = gathered_rows(row_tx[k, tb] + halo)
            for side in range(2):
                edge = 0 if side == 0 else cols - 1
                place = flat == 4 * tall + cr
                extra = jnp.sum(
                    jnp.where(place, halo[:, edge:edge + 1], 0.0), axis=0, keepdims=True)
                col = col_tx[k, side, er:er + 1, :] + merged[side][er:er + 1, :] + extra
                lines += [col, rows_here[side]]
        return jnp.concatenate(lines, axis=0)

    def send_corners(k, weights, v):
        h = weights * v
        fore = h + pltpu.roll(h, LANES - 1, 1)
        fore = fore + pltpu.roll(fore, LANES - 2, 1)
        back = h + pltpu.roll(h, 1, 1)
        back = back + pltpu.roll(back, 2, 1)
        h = jnp.where(low_half, fore, back)
        cor_tx[k] = h + pltpu.roll(h, slots - 1, 0)
        for copy in halo_copies(k)[:4]:
            copy.start()

    def repeat(x, slot):
        x = jnp.where(flat // 4 == slot, x, 0.0)
        x = pltpu.roll(x, LANES - 4 * slot, 1)
        for step in (4, 8, 16):
            x = x + pltpu.roll(x, step, 1)
        return x

    assert slots == 8
    corner = [corner_weights(g) for g in range(groups)]
    corner_r, corner_inv, shared_diag = [None] * groups, [None] * groups, []

    def corner_step(it, g, k, merged):
        u = corner_values(k, merged)
        scale, weights = corner[g]
        if it == 0:
            if g == 0:
                shared_diag.extend([repeat(u, per), repeat(u, per + 1)])
            used = flat < 4 * per
            u = jnp.where(used, u, 0.0)
            corner_r[g] = u
            corner_inv[g] = jnp.where(used, 1.0 / jnp.where(
                used, shared_diag[0] + scale * shared_diag[1], 1.0), 0.0)
            r = u
        else:
            r = jnp.where(flat < 4 * per, u, 0.0) - corner_r[g]
        send_corners(k + groups, weights, r * corner_inv[g])

    def fill(g, slot, parts):
        v = jnp.concatenate(parts, axis=0)
        top = v.astype(bf16)
        at = pl.ds(pl.multiple_of(slot * rows, rows), rows)
        zcat[g, at, :cols] = top
        zcat[g, at, cols:] = (v - top.astype(f32)).astype(bf16)

    def multiply(g, table_ref):
        gout[...] = (
            jnp.dot(zcat[g], table_ref[:2 * cols, :], preferred_element_type=f32)
            + jnp.dot(zcat[g, :, :cols], table_ref[2 * cols:, :], preferred_element_type=f32))

    def total_rows(parts):
        return jnp.sum((parts[0] + parts[3]) + (parts[1] + parts[2]), axis=0, keepdims=True)

    def shared_rows(parts):
        line = (parts[0] + parts[3]) * 0.5 + (parts[1] + parts[2])
        return jnp.sum(jnp.where(on_edge, line * 0.5, line), axis=0, keepdims=True)

    def finish(g, k, base):
        multiply(g, div_ref)

        def third(slot, carry):
            m = base + slot
            h = [u + gout[pl.ds(pl.multiple_of(slot * rows + p * q, q), q), :]
                 for p, u in enumerate(load(w, m))]
            if k < ITERS - 1:
                zh = [u * v for u, v in zip(load(z, m), h)]
                sums[2 * k + 1, pl.ds(m, 1), :] = total_rows(zh)
            return pack((k + 1) * groups + g, m, slot, h, carry)

        tops = lax.fori_loop(0, per, third, (zero, zero), unroll=UNROLL)
        send((k + 1) * groups + g, tops)

    for it in range(ITERS):
        for g in range(groups):
            base = g * per
            k = it * groups + g
            merged = arrive(k)
            if it < ITERS - 1:
                corner_step(it, g, k, merged)
            if it == 0 and g == 0:
                for e in range(2):
                    save(w, modes + e, assembled(k, modes + e, per + e, merged))

            def first(slot, carry, it=it, g=g, k=k, base=base, merged=merged):
                m = base + slot
                uu = assembled(k, m, slot, merged)
                if it == 0:
                    rr = uu
                    inv = [1.0 / (u + scale_ref[m] * v)
                           for u, v in zip(load(w, modes), load(w, modes + 1))]
                    save(invp, m, inv)
                    save(r0, m, rr)
                elif it == 1:
                    rr = [u - v for u, v in zip(uu, load(r0, m))]
                    inv = load(invp, m)
                    save(r1, m, rr)
                else:
                    rr = [2.0 * (u - v) - s for u, v, s in zip(uu, load(r1, m), load(r0, m))]
                    inv = load(invp, m)
                    save(r2, m, rr)
                zz = [u * v for u, v in zip(rr, inv)]
                fill(g, slot, zz)
                sums[2 * it, pl.ds(m, 1), :] = shared_rows([u * v for u, v in zip(uu, zz)])
                f = load2(flux)
                gx = [combo(SLOPES[a], zz) for a in range(4)]
                fg = [f[a] * gx[a] * scale_ref[m] for a in range(4)]
                mz = [u * v for u, v in zip(load2(mass), zz)]
                if it < ITERS - 1:
                    save(z, m, zz)
                else:
                    sums[2 * it + 1, pl.ds(m, 1), :] = total_rows(
                        [u * v + s * t for u, v, s, t in zip(mz, zz, fg, gx)])
                save(w, m, [mz[a] + combo(SLOPES[:, a], fg) for a in range(4)])
                return carry

            lax.fori_loop(0, per, first, 0, unroll=UNROLL)
            multiply(g, grad_ref)

            def second(slot, carry, it=it, g=g, base=base):
                m = base + slot
                grad = [gout[pl.ds(pl.multiple_of(slot * rows + p * q, q), q), :]
                        for p in range(4)]
                fy = [u * v * scale_ref[m] for u, v in zip(load2(flux), grad)]
                if it == ITERS - 1:
                    e = 2 * it + 1
                    sums[e, pl.ds(m, 1), :] = sums[e, pl.ds(m, 1), :] + total_rows(
                        [u * v for u, v in zip(fy, grad)])
                fill(g, slot, fy)
                return carry

            lax.fori_loop(0, per, second, 0, unroll=UNROLL)
            if it < ITERS - 1:
                finish(g, it, base)

    high = lax.broadcasted_iota(jnp.int32, (FIELD, LANES), 0)
    wide = lax.broadcasted_iota(jnp.int32, (FIELD, LANES), 1)
    picks = [(wide == e * FIELD + high) & (high < modes) for e in range(PRODUCTS)]
    spread = jnp.zeros((FIELD, LANES), f32)
    for e in range(PRODUCTS):
        part = jnp.sum(sums[e], axis=1, keepdims=True)
        spread = spread + jnp.where(picks[e], part, 0.0)
    line = jnp.sum(spread, axis=0, keepdims=True)

    def share(stage, line, tx, rx, peers):
        tx[...] = line
        rx[0] = line
        for j, where in enumerate(peers):
            pltpu.make_async_remote_copy(
                src_ref=tx, dst_ref=rx.at[j + 1], send_sem=atx_sem.at[stage],
                recv_sem=arx_sem.at[stage], device_id=where, device_id_type=MESH).start()

    def gather(stage, rx):
        landed(rx.at[pl.ds(1, rx.shape[0] - 1)], arx_sem.at[stage])
        return jnp.sum(rx[...], axis=0)

    share(0, line, near_tx, near_rx, near)
    for g in range(groups):
        finish(g, ITERS - 1, g * per)
    share(1, gather(0, near_rx), far_tx, far_rx, far)
    for g in range(groups):
        k = ITERS * groups + g
        merged = arrive(k)

        def last(slot, carry, g=g, k=k, merged=merged):
            m = g * per + slot
            save(u2, m, assembled(k, m, slot, merged))
            return carry

        lax.fori_loop(0, per, last, 0, unroll=UNROLL)

    total = gather(1, far_rx)
    pad = (high[:, :1] >= modes).astype(f32)
    n0, p00, p01, p11, p12, p22 = [
        jnp.broadcast_to(
            jnp.sum(jnp.where(pick, total, 0.0), axis=1, keepdims=True), (FIELD, LANES))
        for pick in picks]
    pad = jnp.broadcast_to(pad, (FIELD, LANES))
    p00, p11, p22 = p00 + pad, p11 + pad, p22 + 2.0 * pad
    b0 = n0
    b1 = p00 - n0
    b2 = 2.0 * (p01 - b1) - n0
    p02 = 2.0 * p11 - p00
    i0 = 1.0 / p00
    l1, l2 = p01 * i0, p02 * i0
    d1 = p11 - l1 * p01
    t2 = p12 - l2 * p01
    i1 = 1.0 / d1
    l3 = t2 * i1
    d2 = p22 - l2 * p02 - l3 * t2
    y1 = b1 - l1 * b0
    y2 = b2 - l2 * b0 - l3 * y1
    c2 = y2 / d2
    c1 = y1 * i1 - l3 * c2
    c0 = b0 * i0 - l1 * c1 - l2 * c2
    for e, c in enumerate((c0, c1, c2, 1.0 - c0 - 0.5 * c1, c0 + c1, 0.5 * c1)):
        coef[e] = c

    for k in range((ITERS + 1) * groups):
        landed(gauge, htx_sem.at[k])
    for stage, rx in enumerate((near_rx, far_rx)):
        landed(rx.at[pl.ds(1, rx.shape[0] - 1)], atx_sem.at[stage])


def node_order(r0, r1, r2, u2, invp, coef, sol_ref, res_ref, sol_buf, res_buf, sem):
    modes, rows, cols = r0.shape
    q, tiles = rows // 4, cols // LANES

    def stores(m):
        return [
            pltpu.make_async_copy(
                buf.at[c, m], out.at[m, :, pl.ds(c * LANES, LANES)], sem.at[k, c, m])
            for k, (buf, out) in enumerate(((sol_buf, sol_ref), (res_buf, res_ref)))
            for c in range(tiles)
        ]

    def body(m, carry):
        c0, c1, c2, e0, e1, e2 = [coef[e, pl.ds(m, 1), :] for e in range(6)]
        for c in range(tiles):
            for p in range(4):
                at = (m, slice(p * q, (p + 1) * q), slice(c * LANES, (c + 1) * LANES))
                a0, a1, a2 = r0[at], r1[at], r2[at]
                sol_buf[c, m, pl.ds(p, q, stride=4), :] = invp[at] * (c0 * a0 + c1 * a1 + c2 * a2)
                res_buf[c, m, pl.ds(p, q, stride=4), :] = (
                    e0 * a0 - e1 * a1 - e2 * a2 - c2 * u2[at])
        for copy in stores(m):
            copy.start()
        return carry

    lax.fori_loop(0, modes, body, 0)

    def drain(m, carry):
        for copy in stores(m):
            copy.wait()
        return carry

    lax.fori_loop(0, modes, drain, 0)


def strided(refs, p, q):
    return jnp.concatenate([ref[pl.ds(p, q, stride=4), :] for ref in refs], axis=1)


def stack_table(table):
    top = table.astype(bf16)
    low = (table - top.astype(np.float32)).astype(bf16)
    return np.concatenate([top, top, low], axis=0)


def shards(nc, ns, forcing, metric, jacobian, mode_scale):
    modes, rows, cols = forcing.shape
    block = np.kron(np.eye(cols // 4), SLOPES).astype(np.float32)
    grad, div = stack_table(block.T), stack_table(block)
    q, tiles = rows // 4, cols // LANES
    groups = GROUPS if modes % GROUPS == 0 else 1
    per = modes // groups
    slots = -(-(per + 2) // 8) * 8
    vm = pl.BlockSpec(memory_space=pltpu.VMEM)
    hbm = pl.BlockSpec(memory_space=pltpu.HBM)
    rounds = (ITERS + 1) * groups
    ny, nz, nk, nx = planes(nc, ns)
    field = pltpu.VMEM((modes, rows, cols), f32)
    split = pltpu.VMEM((tiles, modes, rows, LANES), f32)
    table = pltpu.VMEM(grad.shape, bf16)
    line = pltpu.VMEM((1, LANES), f32)
    shape = jax.ShapeDtypeStruct(forcing.shape, f32)
    kept = pl.pallas_call(
        functools.partial(kernel, nc, ns, modes, groups),
        out_shape=[shape] * 5 + [jax.ShapeDtypeStruct((6, FIELD, LANES), f32)],
        in_specs=[hbm] * 6,
        out_specs=[vm] * 6,
        scratch_shapes=[
            field,
            pltpu.VMEM((modes + 2, rows, cols), f32),
            pltpu.VMEM((rows, cols), f32),
            pltpu.VMEM((rows, cols), f32),
            pltpu.VMEM((groups, per * rows, 2 * cols), bf16),
            pltpu.VMEM((per * rows, cols), f32),
            pltpu.VMEM((PRODUCTS, FIELD, cols), f32),
            pltpu.VMEM((rounds, 2, slots, cols), f32),
            pltpu.VMEM((rounds, 2, slots, cols), f32),
            pltpu.VMEM((rounds, 2, q, LANES), f32),
            pltpu.VMEM((rounds, 2, q, LANES), f32),
            pltpu.VMEM((rounds, 8, LANES), f32),
            pltpu.VMEM((rounds, 4, 1, LANES), f32),
            line,
            pltpu.VMEM((ny * nk * nx, 1, LANES), f32),
            line,
            pltpu.VMEM((nz, 1, LANES), f32),
            split,
            pltpu.VMEM((2, tiles, rows, LANES), f32),
            pltpu.VMEM((4 + 2 * slots * tiles + 2 * q, LANES), f32),
            table, table,
            pltpu.SMEM((modes,), f32),
            pltpu.SemaphoreType.DMA((rounds,)),
            pltpu.SemaphoreType.DMA((rounds,)),
            pltpu.SemaphoreType.DMA((2,)),
            pltpu.SemaphoreType.DMA((2,)),
            pltpu.SemaphoreType.DMA((2,)),
            pltpu.SemaphoreType.DMA((3,)),
        ],
        compiler_params=pltpu.CompilerParams(
            collective_id=0, has_side_effects=True, vmem_limit_bytes=41943040),
    )(*[pltpu.with_memory_space_constraint(v, pltpu.HBM) for v in (mode_scale, forcing, metric, jacobian, jnp.asarray(grad), jnp.asarray(div))])
    return pl.pallas_call(
        node_order,
        out_shape=[shape] * 2,
        in_specs=[vm] * 6,
        out_specs=[hbm, hbm],
        scratch_shapes=[split, split, pltpu.SemaphoreType.DMA((2, tiles, modes))],
        compiler_params=pltpu.CompilerParams(vmem_limit_bytes=16 * 1024 * 1024),
    )(*kept)


def solution(mesh):
    placed = (P(None, "curve", "sub"), P("curve", "sub"), P("curve", "sub"), P())
    return jax.shard_map(
        functools.partial(shards, mesh.shape["curve"], mesh.shape["sub"]),
        mesh=mesh,
        in_specs=placed,
        out_specs=(P(None, "curve", "sub"), P(None, "curve", "sub")),
        check_vma=False,
    )
```

```python
import functools
import math

import jax
import jax.numpy as jnp
import numpy as np
from jax import lax
from jax.experimental import pallas as pl
from jax.experimental.pallas import tpu as pltpu
from jax.sharding import PartitionSpec as P

ITERS = 3
GROUPS = 2
UNROLL = True
MESH = pl.DeviceIdType.MESH
LANES = 128
f32 = jnp.float32
bf16 = jnp.bfloat16


def gll_tables():
    points = np.array([-1.0, -1.0 / math.sqrt(5.0), 1.0 / math.sqrt(5.0), 1.0])
    weights = np.array([1.0 / 6.0, 5.0 / 6.0, 5.0 / 6.0, 1.0 / 6.0])
    factor = np.array(
        [np.prod([points[j] - points[m] for m in range(4) if m != j]) for j in range(4)]
    )
    slopes = np.zeros((4, 4))
    for i in range(4):
        for j in range(4):
            if i != j:
                slopes[i, j] = factor[i] / (factor[j] * (points[i] - points[j]))
        slopes[i, i] = sum((1.0 / (points[i] - points[m]) for m in range(4) if m != i))
    return (slopes, weights)


SLOPES, WEIGHTS = gll_tables()


def combo(coefs, parts):
    total = None
    for c, v in zip(coefs, parts):
        if abs(c) < 1e-12:
            continue
        term = v * f32(c)
        total = term if total is None else total + term
    return total


PRODUCTS = 6
FIELD = 16


def planes(nc, ns):
    depth = 8 if nc % 16 == 0 else 2
    return nc // (2 * depth), depth, 2, ns


def slope(z):
    even = (z[1] + z[2]) - (z[0] + z[3])
    outer, inner = z[3] - z[0], z[2] - z[1]
    half = 0.5 * (SLOPES[:, ::-1] - SLOPES)
    a = outer * f32(half[0, 0]) + inner * f32(half[0, 1])
    b = outer * f32(half[1, 0]) + inner * f32(half[1, 1])
    e0 = even * f32(0.5 * (SLOPES[0, 1] + SLOPES[0, 2]))
    e1 = even * f32(0.5 * (SLOPES[1, 1] + SLOPES[1, 2]))
    return [a + e0, b + e1, b - e1, a - e0]


def fall(f):
    s0, s1, d0, d1 = f[0] + f[3], f[1] + f[2], f[3] - f[0], f[2] - f[1]
    even = 0.5 * (SLOPES[:, 1] + SLOPES[:, 2])
    half = 0.5 * (SLOPES[:, ::-1] - SLOPES)
    x = d0 * f32(even[0]) + d1 * f32(even[1])
    y = s0 * f32(half[0, 0]) + s1 * f32(half[1, 0])
    v = s0 * f32(half[0, 1]) + s1 * f32(half[1, 1])
    return [x - y, (0.0 - x) - v, v - x, x + y]


def landed(ref, sem):
    pltpu.make_async_copy(ref, ref, sem).wait()


def kernel(
    nc, ns, modes, groups,
    scale_hbm, forcing_ref, metric_ref, jac_ref, grad_hbm, div_hbm,
    r0, r1, r2, u2, invp, coef,
    z, w, mass, flux, zcat, gout, sums,
    row_tx, row_rx, col_tx, col_rx, cor_tx, cor_rx, near_tx, near_rx, far_tx, far_rx,
    source, factors, gauge, grad_ref, div_ref, scale_ref,
    htx_sem, hrx_sem, atx_sem, arx_sem, in_sem, table_sem,
):
    rows, cols = metric_ref.shape
    q = rows // 4
    half = cols - LANES
    tiles = cols // LANES
    per = modes // groups
    slots = row_tx.shape[2]
    loads, sources = [], []
    for c in range(tiles):
        cut = pl.ds(c * LANES, LANES)
        loads += [
            pltpu.make_async_copy(jac_ref.at[:, cut], factors.at[0, c], in_sem.at[0]),
            pltpu.make_async_copy(metric_ref.at[:, cut], factors.at[1, c], in_sem.at[0]),
        ]
        sources.append(
            pltpu.make_async_copy(forcing_ref.at[:, :, cut], source.at[c], in_sem.at[1]))
    div_load = pltpu.make_async_copy(div_hbm, div_ref, table_sem.at[0])
    grad_load = pltpu.make_async_copy(grad_hbm, grad_ref, table_sem.at[1])
    scale_load = pltpu.make_async_copy(scale_hbm, scale_ref, table_sem.at[2])
    for copy in loads + sources + [div_load, scale_load, grad_load]:
        copy.start()

    me_c, me_s = lax.axis_index("curve"), lax.axis_index("sub")
    up, down = lax.rem(me_c + nc - 1, nc), lax.rem(me_c + 1, nc)
    left, right = lax.rem(me_s + ns - 1, ns), lax.rem(me_s + 1, ns)

    ny, nz, nk, nx = planes(nc, ns)
    core, chip = lax.rem(me_c, nk), me_c // nk
    at_z, at_y = lax.rem(chip, nz), chip // nz
    subs = [me_s if dx == 0 else lax.rem(me_s + dx, nx) for dx in range(nx)]
    ys = [at_y if dy == 0 else lax.rem(at_y + dy, ny) for dy in range(ny)]
    zs = [at_z if dz == 0 else lax.rem(at_z + dz, nz) for dz in range(nz)]

    def ring(step, size):
        return min(step, size - step)

    plane = sorted(
        [(dy, dk, dx) for dy in range(ny) for dk in range(nk) for dx in range(nx)][1:],
        key=lambda o: -(2 * ring(o[0], ny) + o[1] + 2 * ring(o[2], nx)))
    near = [((ys[dy] * nz + at_z) * nk + (1 - core if dk else core), subs[dx])
            for dy, dk, dx in plane]
    line_z = sorted(range(1, nz), key=lambda dz: -ring(dz, nz))
    far = [((at_y * nz + zs[dz]) * nk + core, me_s) for dz in line_z]

    barrier = pltpu.get_barrier_semaphore()
    greeted = [
        (up, left), (up, right), (down, left), (down, right)]
    greeted += [((ys[dy] * nz + at_z) * nk + core, me_s) for dy in range(1, ny)]
    greeted += [((at_y * nz + zs[dz]) * nk + core, me_s)
                for dz in sorted({1, 2, nz - 1, nz - 2} - {0, nz})]
    greeted += [(up, me_s), (down, me_s), (me_c, left), (me_c, right)]
    for where in greeted:
        pl.semaphore_signal(barrier, inc=1, device_id=where, device_id_type=MESH)

    lane_full = lax.broadcasted_iota(jnp.int32, (q, cols), 1)
    lane = lax.broadcasted_iota(jnp.int32, (q, LANES), 1)
    row_at = lax.broadcasted_iota(jnp.int32, (q, cols), 0)
    phase = lane_full % 4
    on_edge = (phase == 0) | (phase == 3)
    take_next = (phase == 3) & (lane_full != cols - 1)
    take_prev = (phase == 0) & (lane_full != 0)

    def load(ref, m):
        return [ref[m, p * q:(p + 1) * q, :] for p in range(4)]

    def save(ref, m, parts):
        for p in range(4):
            ref[m, p * q:(p + 1) * q, :] = parts[p]

    def load2(ref):
        return [ref[p * q:(p + 1) * q, :] for p in range(4)]

    def pack(k, m, slot, h, tops):
        lo, hi = tops
        row_tx[k, 0, pl.ds(slot, 1), :] = h[0][0:1, :]
        row_tx[k, 1, pl.ds(slot, 1), :] = h[3][q - 1:q, :]
        t0 = h[0] + jnp.where(row_at == 0, 0.0, pltpu.roll(h[3], 1, 0))
        t3 = h[3] + jnp.where(row_at == q - 1, 0.0, pltpu.roll(h[0], q - 1, 0))
        t = [t0, h[1], h[2], t3]
        save(w, m, t)
        for p in range(4):
            at = 4 * slot + p
            lo = jnp.where(lane == at, pltpu.roll(t[p][:, :LANES], at, 1), lo)
            hi = jnp.where(lane == at, pltpu.roll(t[p][:, half:], at + 1, 1), hi)
        return lo, hi

    def early(k):
        return groups <= k < ITERS * groups

    def halo_copies(k):
        if early(k):
            corners = [cor_tx.at[k, pl.ds(2 * e, 1)] for e in range(4)]
        else:
            corners = [col_tx.at[k, e % 2, pl.ds(0 if e < 2 else q - 1, 1)] for e in range(4)]
        plan = [
            (corners[0], cor_rx.at[k, 3], (up, left)),
            (corners[1], cor_rx.at[k, 2], (up, right)),
            (corners[2], cor_rx.at[k, 1], (down, left)),
            (corners[3], cor_rx.at[k, 0], (down, right)),
            (row_tx.at[k, 0], row_rx.at[k, 1], (up, me_s)),
            (row_tx.at[k, 1], row_rx.at[k, 0], (down, me_s)),
            (col_tx.at[k, 0], col_rx.at[k, 1], (me_c, left)),
            (col_tx.at[k, 1], col_rx.at[k, 0], (me_c, right)),
        ]
        return [
            pltpu.make_async_remote_copy(
                src_ref=src, dst_ref=dst, send_sem=htx_sem.at[k], recv_sem=hrx_sem.at[k],
                device_id=where, device_id_type=MESH)
            for src, dst, where in plan
        ]

    def send(k, tops):
        col_tx[k, 0], col_tx[k, 1] = tops
        for copy in halo_copies(k)[4 if early(k) else 0:]:
            copy.start()

    def arrive(k):
        landed(gauge, hrx_sem.at[k])
        ph = lax.broadcasted_iota(jnp.int32, (1, LANES), 1) % 4
        edge_row = lax.broadcasted_iota(jnp.int32, (q, LANES), 0)
        merged = []
        for side in range(2):
            above, below = cor_rx[k, side], cor_rx[k, 2 + side]
            above = jnp.where(ph == 0, pltpu.roll(above, LANES - 3, 1), 0.0)
            below = jnp.where(ph == 3, pltpu.roll(below, 3, 1), 0.0)
            c = col_rx[k, side]
            c = c + jnp.where(edge_row == 0, above, 0.0) + jnp.where(edge_row == q - 1, below, 0.0)
            merged.append(c)
        return merged

    few_rows = lax.broadcasted_iota(jnp.int32, (8, cols), 0)
    few_at = lax.broadcasted_iota(jnp.int32, (8, cols), 1)
    few_lane = lax.broadcasted_iota(jnp.int32, (8, LANES), 1)
    few_next = (few_at % 4 == 3) & (few_at != cols - 1)
    few_prev = (few_at % 4 == 0) & (few_at != 0)
    few_edge = (few_at % 4 == 3) | (few_at % 4 == 0)
    chunks = q // 8

    def chunk(ref, m, n):
        return [ref[m, p * q + 8 * n:p * q + 8 * n + 8, :] for p in range(4)]

    def chunk2(ref, n):
        return [ref[p * q + 8 * n:p * q + 8 * n + 8, :] for p in range(4)]

    def keep(ref, m, n, parts):
        for p in range(4):
            ref[m, p * q + 8 * n:p * q + 8 * n + 8, :] = parts[p]

    def joined(k, m, slot, merged, n):
        t = chunk(w, m, n)
        if n == 0:
            t[0] = t[0] + jnp.where(few_rows == 0, row_rx[k, 0, pl.ds(slot, 1), :], 0.0)
        if n == chunks - 1:
            t[3] = t[3] + jnp.where(few_rows == 7, row_rx[k, 1, pl.ds(slot, 1), :], 0.0)
        near_side, far_side = [v[8 * n:8 * n + 8] for v in merged]
        out = []
        for p in range(4):
            at = 4 * slot + p
            c = t[p] + jnp.where(
                few_next, pltpu.roll(t[p], cols - 1, 1),
                jnp.where(few_prev, pltpu.roll(t[p], 1, 1), 0.0))
            a = jnp.where(few_lane == 0, pltpu.roll(near_side, LANES - at, 1), 0.0)
            b = jnp.where(few_lane == LANES - 1, pltpu.roll(far_side, LANES - 1 - at, 1), 0.0)
            pieces = [c[:, e * LANES:(e + 1) * LANES] for e in range(tiles)]
            pieces[0] = pieces[0] + a
            pieces[-1] = pieces[-1] + b
            out.append(jnp.concatenate(pieces, axis=1))
        return out

    edge_w, mid_w = f32(1.0 / 6.0), f32(5.0 / 6.0)
    col_w = jnp.where(on_edge, edge_w, mid_w)
    mw, fw = [], []
    landed(factors, in_sem.at[0])
    for p in range(4):
        grid_w = col_w * (edge_w if p in (0, 3) else mid_w)
        mw.append(strided([factors.at[0, c] for c in range(tiles)], p, q) * grid_w)
        fw.append(strided([factors.at[1, c] for c in range(tiles)], p, q) * grid_w)
        mass[p * q:(p + 1) * q, :] = mw[p]
        flux[p * q:(p + 1) * q, :] = fw[p]
    zero = jnp.zeros((q, LANES), f32)
    tops = pack(0, modes, per, mw, (zero, zero))
    div_load.wait()
    table = div_ref[:cols, :].astype(f32) + div_ref[2 * cols:, :].astype(f32)
    by_cols = jnp.dot(flux[...], table * table, precision=lax.Precision.HIGHEST,
                      preferred_element_type=f32)
    squared = SLOPES * SLOPES
    lap = [combo(squared[:, a], fw) + by_cols[a * q:(a + 1) * q, :] for a in range(4)]
    tops = pack(0, modes + 1, per + 1, lap, tops)
    landed(source, in_sem.at[1])
    for g in range(groups):

        def start_body(slot, carry, g=g):
            m = g * per + slot
            h = [strided([source.at[c, m] for c in range(tiles)], p, q)
                 * mass[p * q:(p + 1) * q, :] for p in range(4)]
            return pack(g, m, slot, h, carry)

        tops = lax.fori_loop(0, per, start_body, tops if g == 0 else (zero, zero), unroll=UNROLL)
        if g == 0:
            pl.semaphore_wait(barrier, len(greeted))
        send(g, tops)
    scale_load.wait()
    grad_load.wait()

    at_lane = lax.broadcasted_iota(jnp.int32, (1, LANES), 1)
    of_four = at_lane % 4
    tall = lax.broadcasted_iota(jnp.int32, (slots, LANES), 0)
    flat = lax.broadcasted_iota(jnp.int32, (slots, LANES), 1)
    low_half = tall < 4

    def coefs(values):
        line = jnp.zeros((1, LANES), f32)
        for e, value in enumerate(values):
            line = jnp.where(of_four == e, f32(value), line)
        return line

    def corner_weights(g):
        scale = jnp.zeros((1, LANES), f32)
        for slot in range(per):
            scale = jnp.where(at_lane // 4 == slot, scale_ref[g * per + slot], scale)
        lines = []
        for tb in range(2):
            er, cr = (0, 0) if tb == 0 else (q - 1, 3)
            for side in range(2):
                cc, edge, start = (0, 0, 0) if side == 0 else (3, cols - 1, cols - 4)
                sx = jnp.zeros((1, LANES), f32)
                sy = jnp.zeros((1, LANES), f32)
                own = jnp.zeros((1, 1), f32)
                for e in range(4):
                    fx = flux[e * q + er:e * q + er + 1, edge:edge + 1]
                    fy = flux[cr * q + er:cr * q + er + 1, start + e:start + e + 1]
                    sx = sx + fx * coefs(SLOPES[e, cr] * SLOPES[e])
                    sy = sy + fy * coefs(SLOPES[e, cc] * SLOPES[e])
                    own = own + fy * f32(SLOPES[e, cc] * SLOPES[e, cc])
                here = mass[cr * q + er:cr * q + er + 1, edge:edge + 1]
                lines += [
                    scale * sx + jnp.where(of_four == cr, here + scale * own, 0.0),
                    jnp.where(of_four == cc, 0.0, scale * sy)]
        return scale, jnp.concatenate(lines, axis=0)

    def gathered_rows(x):
        left = x[:, :LANES]
        left = left + jnp.where(flat == 3, pltpu.roll(left, LANES - 1, 1), 0.0)
        right = x[:, half:]
        right = right + jnp.where(flat == LANES - 4, pltpu.roll(right, 1, 1), 0.0)
        left = pltpu.roll(jnp.where(flat < 4, left, 0.0), 0, 1, stride=4, stride_axis=0)
        right = pltpu.roll(
            jnp.where(flat >= LANES - 4, right, 0.0), 4, 1, stride=4, stride_axis=0)
        return [jnp.sum(v, axis=0, keepdims=True) for v in (left, right)]

    def corner_values(k, merged):
        lines = []
        for tb in range(2):
            er, cr = (0, 0) if tb == 0 else (q - 1, 3)
            halo = row_rx[k, tb]
            rows_here = gathered_rows(row_tx[k, tb] + halo)
            for side in range(2):
                edge = 0 if side == 0 else cols - 1
                place = flat == 4 * tall + cr
                extra = jnp.sum(
                    jnp.where(place, halo[:, edge:edge + 1], 0.0), axis=0, keepdims=True)
                col = col_tx[k, side, er:er + 1, :] + merged[side][er:er + 1, :] + extra
                lines += [col, rows_here[side]]
        return jnp.concatenate(lines, axis=0)

    def send_corners(k, weights, v):
        h = weights * v
        fore = h + pltpu.roll(h, LANES - 1, 1)
        fore = fore + pltpu.roll(fore, LANES - 2, 1)
        back = h + pltpu.roll(h, 1, 1)
        back = back + pltpu.roll(back, 2, 1)
        h = jnp.where(low_half, fore, back)
        cor_tx[k] = h + pltpu.roll(h, slots - 1, 0)
        for copy in halo_copies(k)[:4]:
            copy.start()

    def repeat(x, slot):
        x = jnp.where(flat // 4 == slot, x, 0.0)
        x = pltpu.roll(x, LANES - 4 * slot, 1)
        for step in (4, 8, 16):
            x = x + pltpu.roll(x, step, 1)
        return x

    assert slots == 8
    corner = [corner_weights(g) for g in range(groups)]
    corner_r, corner_inv, shared_diag = [None] * groups, [None] * groups, []

    def corner_step(it, g, k, merged):
        u = corner_values(k, merged)
        scale, weights = corner[g]
        if it == 0:
            if g == 0:
                shared_diag.extend([repeat(u, per), repeat(u, per + 1)])
            used = flat < 4 * per
            u = jnp.where(used, u, 0.0)
            corner_r[g] = u
            corner_inv[g] = jnp.where(used, 1.0 / jnp.where(
                used, shared_diag[0] + scale * shared_diag[1], 1.0), 0.0)
            r = u
        else:
            r = jnp.where(flat < 4 * per, u, 0.0) - corner_r[g]
        send_corners(k + groups, weights, r * corner_inv[g])

    def fill(g, slot, n, parts):
        v = jnp.concatenate(parts, axis=0)
        top = v.astype(bf16)
        at = pl.ds(pl.multiple_of(slot * rows + 32 * n, 32), 32)
        zcat[g, at, :cols] = top
        zcat[g, at, cols:] = (v - top.astype(f32)).astype(bf16)

    def taken(slot, n):
        return [gout[pl.ds(pl.multiple_of(slot * rows + 32 * n + 8 * p, 8), 8), :]
                for p in range(4)]

    def multiply(g, table_ref):
        gout[...] = (
            jnp.dot(zcat[g], table_ref[:2 * cols, :], preferred_element_type=f32)
            + jnp.dot(zcat[g, :, :cols], table_ref[2 * cols:, :], preferred_element_type=f32))

    def total(parts):
        return (parts[0] + parts[3]) + (parts[1] + parts[2])

    def shared(parts):
        return (parts[0] + parts[3]) * 0.5 + (parts[1] + parts[2])

    def put(e, m, line):
        sums[e, pl.ds(m, 1), :] = jnp.sum(line, axis=0, keepdims=True)

    def finish(g, k, base):
        multiply(g, div_ref)

        def third(slot, carry):
            m = base + slot
            h, line = [], 0.0
            for n in range(chunks):
                zz = chunk(z, m, n)
                part = [t * u + scale_ref[m] * (v + s) for t, u, v, s in zip(
                    chunk2(mass, n), zz, chunk(w, m, n), taken(slot, n))]
                if k < ITERS - 1:
                    line = line + total([u * v for u, v in zip(zz, part)])
                h.append(part)
            if k < ITERS - 1:
                put(2 * k + 1, m, line)
            h = [jnp.concatenate([part[p] for part in h], axis=0) for p in range(4)]
            return pack((k + 1) * groups + g, m, slot, h, carry)

        tops = lax.fori_loop(0, per, third, (zero, zero), unroll=UNROLL)
        send((k + 1) * groups + g, tops)

    for it in range(ITERS):
        for g in range(groups):
            base = g * per
            k = it * groups + g
            merged = arrive(k)
            if it < ITERS - 1:
                corner_step(it, g, k, merged)
            if it == 0 and g == 0:
                for e in range(2):
                    got = [joined(k, modes + e, per + e, merged, n) for n in range(chunks)]
                    for n in range(chunks):
                        keep(w, modes + e, n, got[n])

            def first(slot, carry, it=it, g=g, k=k, base=base, merged=merged):
                m = base + slot
                line, energy = 0.0, 0.0
                for n in range(chunks):
                    uu = joined(k, m, slot, merged, n)
                    if it == 0:
                        rr = uu
                        inv = [1.0 / (u + scale_ref[m] * v)
                               for u, v in zip(chunk(w, modes, n), chunk(w, modes + 1, n))]
                        keep(invp, m, n, inv)
                    elif it == 1:
                        rr = [u - v for u, v in zip(uu, chunk(r0, m, n))]
                        inv = chunk(invp, m, n)
                    else:
                        rr = [2.0 * (u - v) - s for u, v, s in zip(
                            uu, chunk(r1, m, n), chunk(r0, m, n))]
                        inv = chunk(invp, m, n)
                    keep((r0, r1, r2)[it], m, n, rr)
                    zz = [u * v for u, v in zip(rr, inv)]
                    keep(z, m, n, zz)
                    fill(g, slot, n, zz)
                    line = line + shared([u * v for u, v in zip(uu, zz)])
                    gx = slope(zz)
                    fg = [u * v for u, v in zip(chunk2(flux, n), gx)]
                    keep(w, m, n, fall(fg))
                    if it == ITERS - 1:
                        energy = energy + (
                            total([t * u * u for t, u in zip(chunk2(mass, n), zz)])
                            + scale_ref[m] * total([u * v for u, v in zip(fg, gx)]))
                put(2 * it, m, jnp.where(few_edge, line * 0.5, line))
                if it == ITERS - 1:
                    put(2 * it + 1, m, energy)
                return carry

            lax.fori_loop(0, per, first, 0, unroll=UNROLL)
            multiply(g, grad_ref)

            def second(slot, carry, it=it, g=g, base=base):
                m, e, line = base + slot, 2 * it + 1, 0.0
                for n in range(chunks):
                    grad = taken(slot, n)
                    fy = [u * v for u, v in zip(chunk2(flux, n), grad)]
                    if it == ITERS - 1:
                        line = line + total([u * v for u, v in zip(fy, grad)])
                    fill(g, slot, n, fy)
                if it == ITERS - 1:
                    sums[e, pl.ds(m, 1), :] = sums[e, pl.ds(m, 1), :] + scale_ref[m] * jnp.sum(
                        line, axis=0, keepdims=True)
                return carry

            lax.fori_loop(0, per, second, 0, unroll=UNROLL)
            if it < ITERS - 1:
                finish(g, it, base)

    high = lax.broadcasted_iota(jnp.int32, (FIELD, LANES), 0)
    wide = lax.broadcasted_iota(jnp.int32, (FIELD, LANES), 1)
    picks = [(wide == e * FIELD + high) & (high < modes) for e in range(PRODUCTS)]
    spread = jnp.zeros((FIELD, LANES), f32)
    for e in range(PRODUCTS):
        part = jnp.sum(sums[e], axis=1, keepdims=True)
        spread = spread + jnp.where(picks[e], part, 0.0)
    line = jnp.sum(spread, axis=0, keepdims=True)

    def share(stage, line, tx, rx, peers):
        tx[...] = line
        rx[0] = line
        for j, where in enumerate(peers):
            pltpu.make_async_remote_copy(
                src_ref=tx, dst_ref=rx.at[j + 1], send_sem=atx_sem.at[stage],
                recv_sem=arx_sem.at[stage], device_id=where, device_id_type=MESH).start()

    def gather(stage, rx):
        landed(rx.at[pl.ds(1, rx.shape[0] - 1)], arx_sem.at[stage])
        return jnp.sum(rx[...], axis=0)

    share(0, line, near_tx, near_rx, near)
    for g in range(groups):
        finish(g, ITERS - 1, g * per)
    share(1, gather(0, near_rx), far_tx, far_rx, far)
    for g in range(groups):
        k = ITERS * groups + g
        merged = arrive(k)

        def last(slot, carry, g=g, k=k, merged=merged):
            m = g * per + slot
            for n in range(chunks):
                keep(u2, m, n, joined(k, m, slot, merged, n))
            return carry

        lax.fori_loop(0, per, last, 0, unroll=UNROLL)

    total = gather(1, far_rx)
    pad = (high[:, :1] >= modes).astype(f32)
    n0, p00, p01, p11, p12, p22 = [
        jnp.broadcast_to(
            jnp.sum(jnp.where(pick, total, 0.0), axis=1, keepdims=True), (FIELD, LANES))
        for pick in picks]
    pad = jnp.broadcast_to(pad, (FIELD, LANES))
    p00, p11, p22 = p00 + pad, p11 + pad, p22 + 2.0 * pad
    b0 = n0
    b1 = p00 - n0
    b2 = 2.0 * (p01 - b1) - n0
    p02 = 2.0 * p11 - p00
    i0 = 1.0 / p00
    l1, l2 = p01 * i0, p02 * i0
    d1 = p11 - l1 * p01
    t2 = p12 - l2 * p01
    i1 = 1.0 / d1
    l3 = t2 * i1
    d2 = p22 - l2 * p02 - l3 * t2
    y1 = b1 - l1 * b0
    y2 = b2 - l2 * b0 - l3 * y1
    c2 = y2 / d2
    c1 = y1 * i1 - l3 * c2
    c0 = b0 * i0 - l1 * c1 - l2 * c2
    for e, c in enumerate((c0, c1, c2, 1.0 - c0 - 0.5 * c1, c0 + c1, 0.5 * c1)):
        coef[e] = c

    for k in range((ITERS + 1) * groups):
        landed(gauge, htx_sem.at[k])
    for stage, rx in enumerate((near_rx, far_rx)):
        landed(rx.at[pl.ds(1, rx.shape[0] - 1)], atx_sem.at[stage])


def node_order(r0, r1, r2, u2, invp, coef, sol_ref, res_ref, sol_buf, res_buf, sem):
    modes, rows, cols = r0.shape
    q, tiles = rows // 4, cols // LANES

    def stores(m):
        return [
            pltpu.make_async_copy(
                buf.at[c, m], out.at[m, :, pl.ds(c * LANES, LANES)], sem.at[k, c, m])
            for k, (buf, out) in enumerate(((sol_buf, sol_ref), (res_buf, res_ref)))
            for c in range(tiles)
        ]

    def body(m, carry):
        c0, c1, c2, e0, e1, e2 = [coef[e, pl.ds(m, 1), :] for e in range(6)]
        for c in range(tiles):
            for p in range(4):
                at = (m, slice(p * q, (p + 1) * q), slice(c * LANES, (c + 1) * LANES))
                a0, a1, a2 = r0[at], r1[at], r2[at]
                sol_buf[c, m, pl.ds(p, q, stride=4), :] = invp[at] * (c0 * a0 + c1 * a1 + c2 * a2)
                res_buf[c, m, pl.ds(p, q, stride=4), :] = (
                    e0 * a0 - e1 * a1 - e2 * a2 - c2 * u2[at])
        for copy in stores(m):
            copy.start()
        return carry

    lax.fori_loop(0, modes, body, 0)

    def drain(m, carry):
        for copy in stores(m):
            copy.wait()
        return carry

    lax.fori_loop(0, modes, drain, 0)


def strided(refs, p, q):
    return jnp.concatenate([ref[pl.ds(p, q, stride=4), :] for ref in refs], axis=1)


def stack_table(table):
    top = table.astype(bf16)
    low = (table - top.astype(np.float32)).astype(bf16)
    return np.concatenate([top, top, low], axis=0)


def shards(nc, ns, forcing, metric, jacobian, mode_scale):
    modes, rows, cols = forcing.shape
    block = np.kron(np.eye(cols // 4), SLOPES).astype(np.float32)
    grad, div = stack_table(block.T), stack_table(block)
    q, tiles = rows // 4, cols // LANES
    groups = GROUPS if modes % GROUPS == 0 else 1
    per = modes // groups
    slots = -(-(per + 2) // 8) * 8
    vm = pl.BlockSpec(memory_space=pltpu.VMEM)
    hbm = pl.BlockSpec(memory_space=pltpu.HBM)
    rounds = (ITERS + 1) * groups
    ny, nz, nk, nx = planes(nc, ns)
    field = pltpu.VMEM((modes, rows, cols), f32)
    split = pltpu.VMEM((tiles, modes, rows, LANES), f32)
    table = pltpu.VMEM(grad.shape, bf16)
    line = pltpu.VMEM((1, LANES), f32)
    shape = jax.ShapeDtypeStruct(forcing.shape, f32)
    kept = pl.pallas_call(
        functools.partial(kernel, nc, ns, modes, groups),
        out_shape=[shape] * 5 + [jax.ShapeDtypeStruct((6, FIELD, LANES), f32)],
        in_specs=[hbm] * 6,
        out_specs=[vm] * 6,
        scratch_shapes=[
            field,
            pltpu.VMEM((modes + 2, rows, cols), f32),
            pltpu.VMEM((rows, cols), f32),
            pltpu.VMEM((rows, cols), f32),
            pltpu.VMEM((groups, per * rows, 2 * cols), bf16),
            pltpu.VMEM((per * rows, cols), f32),
            pltpu.VMEM((PRODUCTS, FIELD, cols), f32),
            pltpu.VMEM((rounds, 2, slots, cols), f32),
            pltpu.VMEM((rounds, 2, slots, cols), f32),
            pltpu.VMEM((rounds, 2, q, LANES), f32),
            pltpu.VMEM((rounds, 2, q, LANES), f32),
            pltpu.VMEM((rounds, 8, LANES), f32),
            pltpu.VMEM((rounds, 4, 1, LANES), f32),
            line,
            pltpu.VMEM((ny * nk * nx, 1, LANES), f32),
            line,
            pltpu.VMEM((nz, 1, LANES), f32),
            split,
            pltpu.VMEM((2, tiles, rows, LANES), f32),
            pltpu.VMEM((4 + 2 * slots * tiles + 2 * q, LANES), f32),
            table, table,
            pltpu.SMEM((modes,), f32),
            pltpu.SemaphoreType.DMA((rounds,)),
            pltpu.SemaphoreType.DMA((rounds,)),
            pltpu.SemaphoreType.DMA((2,)),
            pltpu.SemaphoreType.DMA((2,)),
            pltpu.SemaphoreType.DMA((2,)),
            pltpu.SemaphoreType.DMA((3,)),
        ],
        compiler_params=pltpu.CompilerParams(
            collective_id=0, has_side_effects=True, vmem_limit_bytes=41943040),
    )(*[pltpu.with_memory_space_constraint(v, pltpu.HBM) for v in (mode_scale, forcing, metric, jacobian, jnp.asarray(grad), jnp.asarray(div))])
    return pl.pallas_call(
        node_order,
        out_shape=[shape] * 2,
        in_specs=[vm] * 6,
        out_specs=[hbm, hbm],
        scratch_shapes=[split, split, pltpu.SemaphoreType.DMA((2, tiles, modes))],
        compiler_params=pltpu.CompilerParams(vmem_limit_bytes=16 * 1024 * 1024),
    )(*kept)


def solution(mesh):
    placed = (P(None, "curve", "sub"), P("curve", "sub"), P("curve", "sub"), P())
    return jax.shard_map(
        functools.partial(shards, mesh.shape["curve"], mesh.shape["sub"]),
        mesh=mesh,
        in_specs=placed,
        out_specs=(P(None, "curve", "sub"), P(None, "curve", "sub")),
        check_vma=False,
    )
```

```python
import functools
import math

import jax
import jax.numpy as jnp
import numpy as np
from jax import lax
from jax.experimental import pallas as pl
from jax.experimental.pallas import tpu as pltpu
from jax.sharding import PartitionSpec as P

ITERS = 3
GROUPS = 2
UNROLL = True
MESH = pl.DeviceIdType.MESH
LANES = 128
f32 = jnp.float32
bf16 = jnp.bfloat16


def gll_tables():
    points = np.array([-1.0, -1.0 / math.sqrt(5.0), 1.0 / math.sqrt(5.0), 1.0])
    weights = np.array([1.0 / 6.0, 5.0 / 6.0, 5.0 / 6.0, 1.0 / 6.0])
    factor = np.array(
        [np.prod([points[j] - points[m] for m in range(4) if m != j]) for j in range(4)]
    )
    slopes = np.zeros((4, 4))
    for i in range(4):
        for j in range(4):
            if i != j:
                slopes[i, j] = factor[i] / (factor[j] * (points[i] - points[j]))
        slopes[i, i] = sum((1.0 / (points[i] - points[m]) for m in range(4) if m != i))
    return (slopes, weights)


SLOPES, WEIGHTS = gll_tables()


def combo(coefs, parts):
    total = None
    for c, v in zip(coefs, parts):
        if abs(c) < 1e-12:
            continue
        term = v * f32(c)
        total = term if total is None else total + term
    return total


PRODUCTS = 6
FIELD = 16


def planes(nc, ns):
    depth = 8 if nc % 16 == 0 else 2
    return nc // (2 * depth), depth, 2, ns


def slope(z):
    even = (z[1] + z[2]) - (z[0] + z[3])
    outer, inner = z[3] - z[0], z[2] - z[1]
    half = 0.5 * (SLOPES[:, ::-1] - SLOPES)
    a = outer * f32(half[0, 0]) + inner * f32(half[0, 1])
    b = outer * f32(half[1, 0]) + inner * f32(half[1, 1])
    e0 = even * f32(0.5 * (SLOPES[0, 1] + SLOPES[0, 2]))
    e1 = even * f32(0.5 * (SLOPES[1, 1] + SLOPES[1, 2]))
    return [a + e0, b + e1, b - e1, a - e0]


def fall(f):
    s0, s1, d0, d1 = f[0] + f[3], f[1] + f[2], f[3] - f[0], f[2] - f[1]
    even = 0.5 * (SLOPES[:, 1] + SLOPES[:, 2])
    half = 0.5 * (SLOPES[:, ::-1] - SLOPES)
    x = d0 * f32(even[0]) + d1 * f32(even[1])
    y = s0 * f32(half[0, 0]) + s1 * f32(half[1, 0])
    v = s0 * f32(half[0, 1]) + s1 * f32(half[1, 1])
    return [x - y, (0.0 - x) - v, v - x, x + y]


def landed(ref, sem):
    pltpu.make_async_copy(ref, ref, sem).wait()


def kernel(
    nc, ns, modes, groups,
    scale_hbm, forcing_ref, metric_ref, jac_ref, grad_hbm, div_hbm,
    r0, r1, r2, u2, invp, coef,
    z, w, mass, flux, zcat, gout, sums,
    row_tx, row_rx, col_tx, col_rx, cor_tx, cor_rx, near_tx, near_rx, far_tx, far_rx,
    source, factors, gauge, grad_ref, div_ref, scale_ref,
    htx_sem, hrx_sem, crx_sem, atx_sem, arx_sem, in_sem, table_sem,
):
    rows, cols = metric_ref.shape
    q = rows // 4
    half = cols - LANES
    tiles = cols // LANES
    per = modes // groups
    slots = row_tx.shape[2]
    loads, sources = [], []
    for c in range(tiles):
        cut = pl.ds(c * LANES, LANES)
        loads += [
            pltpu.make_async_copy(jac_ref.at[:, cut], factors.at[0, c], in_sem.at[0]),
            pltpu.make_async_copy(metric_ref.at[:, cut], factors.at[1, c], in_sem.at[0]),
        ]
        sources.append(
            pltpu.make_async_copy(forcing_ref.at[:, :, cut], source.at[c], in_sem.at[1]))
    div_load = pltpu.make_async_copy(div_hbm, div_ref, table_sem.at[0])
    grad_load = pltpu.make_async_copy(grad_hbm, grad_ref, table_sem.at[1])
    scale_load = pltpu.make_async_copy(scale_hbm, scale_ref, table_sem.at[2])
    for copy in loads + sources + [div_load, scale_load, grad_load]:
        copy.start()

    me_c, me_s = lax.axis_index("curve"), lax.axis_index("sub")
    up, down = lax.rem(me_c + nc - 1, nc), lax.rem(me_c + 1, nc)
    left, right = lax.rem(me_s + ns - 1, ns), lax.rem(me_s + 1, ns)

    ny, nz, nk, nx = planes(nc, ns)
    core, chip = lax.rem(me_c, nk), me_c // nk
    at_z, at_y = lax.rem(chip, nz), chip // nz
    subs = [me_s if dx == 0 else lax.rem(me_s + dx, nx) for dx in range(nx)]
    ys = [at_y if dy == 0 else lax.rem(at_y + dy, ny) for dy in range(ny)]
    zs = [at_z if dz == 0 else lax.rem(at_z + dz, nz) for dz in range(nz)]

    def ring(step, size):
        return min(step, size - step)

    plane = sorted(
        [(dy, dk, dx) for dy in range(ny) for dk in range(nk) for dx in range(nx)][1:],
        key=lambda o: -(2 * ring(o[0], ny) + o[1] + 2 * ring(o[2], nx)))
    near = [((ys[dy] * nz + at_z) * nk + (1 - core if dk else core), subs[dx])
            for dy, dk, dx in plane]
    line_z = sorted(range(1, nz), key=lambda dz: -ring(dz, nz))
    far = [((at_y * nz + zs[dz]) * nk + core, me_s) for dz in line_z]

    barrier = pltpu.get_barrier_semaphore()
    greeted = [
        (up, left), (up, right), (down, left), (down, right)]
    greeted += [((ys[dy] * nz + at_z) * nk + core, me_s) for dy in range(1, ny)]
    greeted += [((at_y * nz + zs[dz]) * nk + core, me_s)
                for dz in sorted({1, 2, nz - 1, nz - 2} - {0, nz})]
    greeted += [(up, me_s), (down, me_s), (me_c, left), (me_c, right)]
    for where in greeted:
        pl.semaphore_signal(barrier, inc=1, device_id=where, device_id_type=MESH)

    lane_full = lax.broadcasted_iota(jnp.int32, (q, cols), 1)
    lane = lax.broadcasted_iota(jnp.int32, (q, LANES), 1)
    row_at = lax.broadcasted_iota(jnp.int32, (q, cols), 0)
    phase = lane_full % 4
    on_edge = (phase == 0) | (phase == 3)
    take_next = (phase == 3) & (lane_full != cols - 1)
    take_prev = (phase == 0) & (lane_full != 0)

    def load(ref, m):
        return [ref[m, p * q:(p + 1) * q, :] for p in range(4)]

    def save(ref, m, parts):
        for p in range(4):
            ref[m, p * q:(p + 1) * q, :] = parts[p]

    def load2(ref):
        return [ref[p * q:(p + 1) * q, :] for p in range(4)]

    def pack(k, m, slot, h, tops):
        lo, hi = tops
        row_tx[k, 0, pl.ds(slot, 1), :] = h[0][0:1, :]
        row_tx[k, 1, pl.ds(slot, 1), :] = h[3][q - 1:q, :]
        t0 = h[0] + jnp.where(row_at == 0, 0.0, pltpu.roll(h[3], 1, 0))
        t3 = h[3] + jnp.where(row_at == q - 1, 0.0, pltpu.roll(h[0], q - 1, 0))
        t = [t0, h[1], h[2], t3]
        save(w, m, t)
        for p in range(4):
            at = 4 * slot + p
            lo = jnp.where(lane == at, pltpu.roll(t[p][:, :LANES], at, 1), lo)
            hi = jnp.where(lane == at, pltpu.roll(t[p][:, half:], at + 1, 1), hi)
        return lo, hi

    def early(k):
        return groups <= k < ITERS * groups

    def halo_copies(k):
        if early(k):
            corners = [cor_tx.at[k, pl.ds(2 * e, 1)] for e in range(4)]
        else:
            corners = [col_tx.at[k, e % 2, pl.ds(0 if e < 2 else q - 1, 1)] for e in range(4)]
        plan = [
            (corners[0], cor_rx.at[k, 3], (up, left)),
            (corners[1], cor_rx.at[k, 2], (up, right)),
            (corners[2], cor_rx.at[k, 1], (down, left)),
            (corners[3], cor_rx.at[k, 0], (down, right)),
            (row_tx.at[k, 0], row_rx.at[k, 1], (up, me_s)),
            (row_tx.at[k, 1], row_rx.at[k, 0], (down, me_s)),
            (col_tx.at[k, 0], col_rx.at[k, 1], (me_c, left)),
            (col_tx.at[k, 1], col_rx.at[k, 0], (me_c, right)),
        ]
        return [
            pltpu.make_async_remote_copy(
                src_ref=src, dst_ref=dst, send_sem=htx_sem.at[k],
                recv_sem=crx_sem.at[k] if k < groups and e < 4 else hrx_sem.at[k],
                device_id=where, device_id_type=MESH)
            for e, (src, dst, where) in enumerate(plan)
        ]

    def send(k, tops):
        col_tx[k, 0], col_tx[k, 1] = tops
        for copy in halo_copies(k)[4 if early(k) else 0:]:
            copy.start()

    def arrive(k):
        if k < groups:
            landed(gauge.at[pl.ds(0, 4)], crx_sem.at[k])
        else:
            landed(gauge, hrx_sem.at[k])
        ph = lax.broadcasted_iota(jnp.int32, (1, LANES), 1) % 4
        edge_row = lax.broadcasted_iota(jnp.int32, (q, LANES), 0)
        merged = []
        for side in range(2):
            above, below = cor_rx[k, side], cor_rx[k, 2 + side]
            above = jnp.where(ph == 0, pltpu.roll(above, LANES - 3, 1), 0.0)
            below = jnp.where(ph == 3, pltpu.roll(below, 3, 1), 0.0)
            c = col_rx[k, side]
            c = c + jnp.where(edge_row == 0, above, 0.0) + jnp.where(edge_row == q - 1, below, 0.0)
            merged.append(c)
        return merged

    few_rows = lax.broadcasted_iota(jnp.int32, (8, cols), 0)
    few_at = lax.broadcasted_iota(jnp.int32, (8, cols), 1)
    few_lane = lax.broadcasted_iota(jnp.int32, (8, LANES), 1)
    few_next = (few_at % 4 == 3) & (few_at != cols - 1)
    few_prev = (few_at % 4 == 0) & (few_at != 0)
    few_edge = (few_at % 4 == 3) | (few_at % 4 == 0)
    chunks = q // 8

    def chunk(ref, m, n):
        return [ref[m, p * q + 8 * n:p * q + 8 * n + 8, :] for p in range(4)]

    def chunk2(ref, n):
        return [ref[p * q + 8 * n:p * q + 8 * n + 8, :] for p in range(4)]

    def keep(ref, m, n, parts):
        for p in range(4):
            ref[m, p * q + 8 * n:p * q + 8 * n + 8, :] = parts[p]

    def joined(k, m, slot, merged, n):
        t = chunk(w, m, n)
        if n == 0:
            t[0] = t[0] + jnp.where(few_rows == 0, row_rx[k, 0, pl.ds(slot, 1), :], 0.0)
        if n == chunks - 1:
            t[3] = t[3] + jnp.where(few_rows == 7, row_rx[k, 1, pl.ds(slot, 1), :], 0.0)
        near_side, far_side = [v[8 * n:8 * n + 8] for v in merged]
        out = []
        for p in range(4):
            at = 4 * slot + p
            c = t[p] + jnp.where(
                few_next, pltpu.roll(t[p], cols - 1, 1),
                jnp.where(few_prev, pltpu.roll(t[p], 1, 1), 0.0))
            a = jnp.where(few_lane == 0, pltpu.roll(near_side, LANES - at, 1), 0.0)
            b = jnp.where(few_lane == LANES - 1, pltpu.roll(far_side, LANES - 1 - at, 1), 0.0)
            pieces = [c[:, e * LANES:(e + 1) * LANES] for e in range(tiles)]
            pieces[0] = pieces[0] + a
            pieces[-1] = pieces[-1] + b
            out.append(jnp.concatenate(pieces, axis=1))
        return out

    edge_w, mid_w = f32(1.0 / 6.0), f32(5.0 / 6.0)
    col_w = jnp.where(on_edge, edge_w, mid_w)
    mw, fw = [], []
    landed(factors, in_sem.at[0])
    for p in range(4):
        grid_w = col_w * (edge_w if p in (0, 3) else mid_w)
        mw.append(strided([factors.at[0, c] for c in range(tiles)], p, q) * grid_w)
        fw.append(strided([factors.at[1, c] for c in range(tiles)], p, q) * grid_w)
        mass[p * q:(p + 1) * q, :] = mw[p]
        flux[p * q:(p + 1) * q, :] = fw[p]
    zero = jnp.zeros((q, LANES), f32)
    tops = pack(0, modes, per, mw, (zero, zero))
    div_load.wait()
    table = div_ref[:cols, :].astype(f32) + div_ref[2 * cols:, :].astype(f32)
    by_cols = jnp.dot(flux[...], table * table, precision=lax.Precision.HIGHEST,
                      preferred_element_type=f32)
    squared = SLOPES * SLOPES
    lap = [combo(squared[:, a], fw) + by_cols[a * q:(a + 1) * q, :] for a in range(4)]
    tops = pack(0, modes + 1, per + 1, lap, tops)
    landed(source, in_sem.at[1])
    for g in range(groups):

        def start_body(slot, carry, g=g):
            m = g * per + slot
            h = [strided([source.at[c, m] for c in range(tiles)], p, q)
                 * mass[p * q:(p + 1) * q, :] for p in range(4)]
            return pack(g, m, slot, h, carry)

        tops = lax.fori_loop(0, per, start_body, tops if g == 0 else (zero, zero), unroll=UNROLL)
        if g == 0:
            pl.semaphore_wait(barrier, len(greeted))
        send(g, tops)
    scale_load.wait()
    grad_load.wait()

    at_lane = lax.broadcasted_iota(jnp.int32, (1, LANES), 1)
    of_four = at_lane % 4
    tall = lax.broadcasted_iota(jnp.int32, (slots, LANES), 0)
    flat = lax.broadcasted_iota(jnp.int32, (slots, LANES), 1)
    low_half = tall < 4

    def coefs(values):
        line = jnp.zeros((1, LANES), f32)
        for e, value in enumerate(values):
            line = jnp.where(of_four == e, f32(value), line)
        return line

    def corner_weights(g):
        scale = jnp.zeros((1, LANES), f32)
        for slot in range(per):
            scale = jnp.where(at_lane // 4 == slot, scale_ref[g * per + slot], scale)
        lines = []
        for tb in range(2):
            er, cr = (0, 0) if tb == 0 else (q - 1, 3)
            for side in range(2):
                cc, edge, start = (0, 0, 0) if side == 0 else (3, cols - 1, cols - 4)
                sx = jnp.zeros((1, LANES), f32)
                sy = jnp.zeros((1, LANES), f32)
                own = jnp.zeros((1, 1), f32)
                for e in range(4):
                    fx = flux[e * q + er:e * q + er + 1, edge:edge + 1]
                    fy = flux[cr * q + er:cr * q + er + 1, start + e:start + e + 1]
                    sx = sx + fx * coefs(SLOPES[e, cr] * SLOPES[e])
                    sy = sy + fy * coefs(SLOPES[e, cc] * SLOPES[e])
                    own = own + fy * f32(SLOPES[e, cc] * SLOPES[e, cc])
                here = mass[cr * q + er:cr * q + er + 1, edge:edge + 1]
                lines += [
                    scale * sx + jnp.where(of_four == cr, here + scale * own, 0.0),
                    jnp.where(of_four == cc, 0.0, scale * sy)]
        return scale, jnp.concatenate(lines, axis=0)

    def gathered_rows(x):
        left = x[:, :LANES]
        left = left + jnp.where(flat == 3, pltpu.roll(left, LANES - 1, 1), 0.0)
        right = x[:, half:]
        right = right + jnp.where(flat == LANES - 4, pltpu.roll(right, 1, 1), 0.0)
        left = pltpu.roll(jnp.where(flat < 4, left, 0.0), 0, 1, stride=4, stride_axis=0)
        right = pltpu.roll(
            jnp.where(flat >= LANES - 4, right, 0.0), 4, 1, stride=4, stride_axis=0)
        return [jnp.sum(v, axis=0, keepdims=True) for v in (left, right)]

    def corner_values(k, merged):
        lines = []
        for tb in range(2):
            er, cr = (0, 0) if tb == 0 else (q - 1, 3)
            halo = row_rx[k, tb]
            rows_here = gathered_rows(row_tx[k, tb] + halo)
            for side in range(2):
                edge = 0 if side == 0 else cols - 1
                place = flat == 4 * tall + cr
                extra = jnp.sum(
                    jnp.where(place, halo[:, edge:edge + 1], 0.0), axis=0, keepdims=True)
                col = col_tx[k, side, er:er + 1, :] + merged[side][er:er + 1, :] + extra
                lines += [col, rows_here[side]]
        return jnp.concatenate(lines, axis=0)

    def set_corners(k, weights, v):
        h = weights * v
        fore = h + pltpu.roll(h, LANES - 1, 1)
        fore = fore + pltpu.roll(fore, LANES - 2, 1)
        back = h + pltpu.roll(h, 1, 1)
        back = back + pltpu.roll(back, 2, 1)
        h = jnp.where(low_half, fore, back)
        cor_tx[k] = h + pltpu.roll(h, slots - 1, 0)

    def repeat(x, slot):
        x = jnp.where(flat // 4 == slot, x, 0.0)
        x = pltpu.roll(x, LANES - 4 * slot, 1)
        for step in (4, 8, 16):
            x = x + pltpu.roll(x, step, 1)
        return x

    assert slots == 8
    corner = [corner_weights(g) for g in range(groups)]
    corner_r, corner_inv, shared_diag = [None] * groups, [None] * groups, []

    def corner_step(it, g, k, merged):
        u = corner_values(k, merged)
        scale, weights = corner[g]
        if it == 0:
            if g == 0:
                shared_diag.extend([repeat(u, per), repeat(u, per + 1)])
            used = flat < 4 * per
            u = jnp.where(used, u, 0.0)
            corner_r[g] = u
            corner_inv[g] = jnp.where(used, 1.0 / jnp.where(
                used, shared_diag[0] + scale * shared_diag[1], 1.0), 0.0)
            r = u
        else:
            r = jnp.where(flat < 4 * per, u, 0.0) - corner_r[g]
        set_corners(k + groups, weights, r * corner_inv[g])

    def fill(g, slot, n, parts):
        v = jnp.concatenate(parts, axis=0)
        top = v.astype(bf16)
        at = pl.ds(pl.multiple_of(slot * rows + 32 * n, 32), 32)
        zcat[g, at, :cols] = top
        zcat[g, at, cols:] = (v - top.astype(f32)).astype(bf16)

    def taken(slot, n):
        return [gout[pl.ds(pl.multiple_of(slot * rows + 32 * n + 8 * p, 8), 8), :]
                for p in range(4)]

    def multiply(g, table_ref):
        gout[...] = (
            jnp.dot(zcat[g], table_ref[:2 * cols, :], preferred_element_type=f32)
            + jnp.dot(zcat[g, :, :cols], table_ref[2 * cols:, :], preferred_element_type=f32))

    def total(parts):
        return (parts[0] + parts[3]) + (parts[1] + parts[2])

    def shared(parts):
        return (parts[0] + parts[3]) * 0.5 + (parts[1] + parts[2])

    def put(e, m, line):
        sums[e, pl.ds(m, 1), :] = jnp.sum(line, axis=0, keepdims=True)

    def finish(g, k, base):
        multiply(g, div_ref)

        def third(slot, carry):
            m = base + slot
            h, line = [], 0.0
            for n in range(chunks):
                zz = chunk(z, m, n)
                part = [t * u + scale_ref[m] * (v + s) for t, u, v, s in zip(
                    chunk2(mass, n), zz, chunk(w, m, n), taken(slot, n))]
                if k < ITERS - 1:
                    line = line + total([u * v for u, v in zip(zz, part)])
                h.append(part)
            if k < ITERS - 1:
                put(2 * k + 1, m, line)
            h = [jnp.concatenate([part[p] for part in h], axis=0) for p in range(4)]
            return pack((k + 1) * groups + g, m, slot, h, carry)

        tops = lax.fori_loop(0, per, third, (zero, zero), unroll=UNROLL)
        send((k + 1) * groups + g, tops)

    def patched(k, slot, n, parts):
        parts = list(parts)
        for at_n, p, row, lines, at in (
                (0, 0, 0, (0, 1), 4 * slot + 3), (chunks - 1, 3, 7, (2, 3), 4 * slot)):
            if n != at_n:
                continue
            a = pltpu.roll(cor_rx[k, lines[0]], LANES - at, 1)
            b = pltpu.roll(cor_rx[k, lines[1]], LANES - 1 - at, 1)
            here = few_rows[:, :LANES] == row
            pieces = [parts[p][:, e * LANES:(e + 1) * LANES] for e in range(tiles)]
            pieces[0] = pieces[0] + jnp.where(here & (few_lane == 0), a, 0.0)
            pieces[-1] = pieces[-1] + jnp.where(here & (few_lane == LANES - 1), b, 0.0)
            parts[p] = jnp.concatenate(pieces, axis=1)
        return parts

    for g in range(groups):
        landed(gauge.at[pl.ds(0, gauge.shape[0] - 4)], hrx_sem.at[g])
        sides = [col_rx[g, 0], col_rx[g, 1]]
        pairs = [(modes, per), (modes + 1, per + 1)] if g == 0 else []
        for m, slot in pairs + [(g * per + e, e) for e in range(per)]:
            for n in range(chunks):
                keep(w, m, n, joined(g, m, slot, sides, n))

    for it in range(ITERS):
        for g in range(groups):
            base = g * per
            k = it * groups + g
            merged = arrive(k)
            if it < ITERS - 1:
                corner_step(it, g, k, merged)
            if it == 0 and g == 0:
                for e in range(2):
                    for n in (0, chunks - 1):
                        keep(w, modes + e, n, patched(k, per + e, n, chunk(w, modes + e, n)))

            def first(slot, carry, it=it, g=g, k=k, base=base, merged=merged):
                m = base + slot
                line, energy = 0.0, 0.0
                for n in range(chunks):
                    if it == 0:
                        uu = patched(k, slot, n, chunk(w, m, n))
                    else:
                        uu = joined(k, m, slot, merged, n)
                    if it == 0:
                        rr = uu
                        inv = [1.0 / (u + scale_ref[m] * v)
                               for u, v in zip(chunk(w, modes, n), chunk(w, modes + 1, n))]
                        keep(invp, m, n, inv)
                    elif it == 1:
                        rr = [u - v for u, v in zip(uu, chunk(r0, m, n))]
                        inv = chunk(invp, m, n)
                    else:
                        rr = [2.0 * (u - v) - s for u, v, s in zip(
                            uu, chunk(r1, m, n), chunk(r0, m, n))]
                        inv = chunk(invp, m, n)
                    keep((r0, r1, r2)[it], m, n, rr)
                    zz = [u * v for u, v in zip(rr, inv)]
                    keep(z, m, n, zz)
                    fill(g, slot, n, zz)
                    line = line + shared([u * v for u, v in zip(uu, zz)])
                    gx = slope(zz)
                    fg = [u * v for u, v in zip(chunk2(flux, n), gx)]
                    keep(w, m, n, fall(fg))
                    if it == ITERS - 1:
                        energy = energy + (
                            total([t * u * u for t, u in zip(chunk2(mass, n), zz)])
                            + scale_ref[m] * total([u * v for u, v in zip(fg, gx)]))
                put(2 * it, m, jnp.where(few_edge, line * 0.5, line))
                if it == ITERS - 1:
                    put(2 * it + 1, m, energy)
                return carry

            if it < ITERS - 1:
                for copy in halo_copies(k + groups)[:4]:
                    copy.start()
            lax.fori_loop(0, per, first, 0, unroll=UNROLL)
            multiply(g, grad_ref)

            def second(slot, carry, it=it, g=g, base=base):
                m, e, line = base + slot, 2 * it + 1, 0.0
                for n in range(chunks):
                    grad = taken(slot, n)
                    fy = [u * v for u, v in zip(chunk2(flux, n), grad)]
                    if it == ITERS - 1:
                        line = line + total([u * v for u, v in zip(fy, grad)])
                    fill(g, slot, n, fy)
                if it == ITERS - 1:
                    sums[e, pl.ds(m, 1), :] = sums[e, pl.ds(m, 1), :] + scale_ref[m] * jnp.sum(
                        line, axis=0, keepdims=True)
                return carry

            lax.fori_loop(0, per, second, 0, unroll=UNROLL)
            if it < ITERS - 1:
                finish(g, it, base)

    high = lax.broadcasted_iota(jnp.int32, (FIELD, LANES), 0)
    wide = lax.broadcasted_iota(jnp.int32, (FIELD, LANES), 1)
    picks = [(wide == e * FIELD + high) & (high < modes) for e in range(PRODUCTS)]
    spread = jnp.zeros((FIELD, LANES), f32)
    for e in range(PRODUCTS):
        part = jnp.sum(sums[e], axis=1, keepdims=True)
        spread = spread + jnp.where(picks[e], part, 0.0)
    line = jnp.sum(spread, axis=0, keepdims=True)

    def share(stage, line, tx, rx, peers):
        tx[...] = line
        rx[0] = line
        for j, where in enumerate(peers):
            pltpu.make_async_remote_copy(
                src_ref=tx, dst_ref=rx.at[j + 1], send_sem=atx_sem.at[stage],
                recv_sem=arx_sem.at[stage], device_id=where, device_id_type=MESH).start()

    def gather(stage, rx):
        landed(rx.at[pl.ds(1, rx.shape[0] - 1)], arx_sem.at[stage])
        return jnp.sum(rx[...], axis=0)

    share(0, line, near_tx, near_rx, near)
    for g in range(groups):
        finish(g, ITERS - 1, g * per)
    share(1, gather(0, near_rx), far_tx, far_rx, far)
    for g in range(groups):
        k = ITERS * groups + g
        merged = arrive(k)

        def last(slot, carry, g=g, k=k, merged=merged):
            m = g * per + slot
            for n in range(chunks):
                keep(u2, m, n, joined(k, m, slot, merged, n))
            return carry

        lax.fori_loop(0, per, last, 0, unroll=UNROLL)

    total = gather(1, far_rx)
    pad = (high[:, :1] >= modes).astype(f32)
    n0, p00, p01, p11, p12, p22 = [
        jnp.broadcast_to(
            jnp.sum(jnp.where(pick, total, 0.0), axis=1, keepdims=True), (FIELD, LANES))
        for pick in picks]
    pad = jnp.broadcast_to(pad, (FIELD, LANES))
    p00, p11, p22 = p00 + pad, p11 + pad, p22 + 2.0 * pad
    b0 = n0
    b1 = p00 - n0
    b2 = 2.0 * (p01 - b1) - n0
    p02 = 2.0 * p11 - p00
    i0 = 1.0 / p00
    l1, l2 = p01 * i0, p02 * i0
    d1 = p11 - l1 * p01
    t2 = p12 - l2 * p01
    i1 = 1.0 / d1
    l3 = t2 * i1
    d2 = p22 - l2 * p02 - l3 * t2
    y1 = b1 - l1 * b0
    y2 = b2 - l2 * b0 - l3 * y1
    c2 = y2 / d2
    c1 = y1 * i1 - l3 * c2
    c0 = b0 * i0 - l1 * c1 - l2 * c2
    for e, c in enumerate((c0, c1, c2, 1.0 - c0 - 0.5 * c1, c0 + c1, 0.5 * c1)):
        coef[e] = c

    for k in range((ITERS + 1) * groups):
        landed(gauge, htx_sem.at[k])
    for stage, rx in enumerate((near_rx, far_rx)):
        landed(rx.at[pl.ds(1, rx.shape[0] - 1)], atx_sem.at[stage])


def node_order(r0, r1, r2, u2, invp, coef, sol_ref, res_ref, sol_buf, res_buf, sem):
    modes, rows, cols = r0.shape
    q, tiles = rows // 4, cols // LANES

    def stores(m):
        return [
            pltpu.make_async_copy(
                buf.at[c, m], out.at[m, :, pl.ds(c * LANES, LANES)], sem.at[k, c, m])
            for k, (buf, out) in enumerate(((sol_buf, sol_ref), (res_buf, res_ref)))
            for c in range(tiles)
        ]

    def body(m, carry):
        c0, c1, c2, e0, e1, e2 = [coef[e, pl.ds(m, 1), :] for e in range(6)]
        for c in range(tiles):
            for p in range(4):
                at = (m, slice(p * q, (p + 1) * q), slice(c * LANES, (c + 1) * LANES))
                a0, a1, a2 = r0[at], r1[at], r2[at]
                sol_buf[c, m, pl.ds(p, q, stride=4), :] = invp[at] * (c0 * a0 + c1 * a1 + c2 * a2)
                res_buf[c, m, pl.ds(p, q, stride=4), :] = (
                    e0 * a0 - e1 * a1 - e2 * a2 - c2 * u2[at])
        for copy in stores(m):
            copy.start()
        return carry

    lax.fori_loop(0, modes, body, 0)

    def drain(m, carry):
        for copy in stores(m):
            copy.wait()
        return carry

    lax.fori_loop(0, modes, drain, 0)


def strided(refs, p, q):
    return jnp.concatenate([ref[pl.ds(p, q, stride=4), :] for ref in refs], axis=1)


def stack_table(table):
    top = table.astype(bf16)
    low = (table - top.astype(np.float32)).astype(bf16)
    return np.concatenate([top, top, low], axis=0)


def shards(nc, ns, forcing, metric, jacobian, mode_scale):
    modes, rows, cols = forcing.shape
    block = np.kron(np.eye(cols // 4), SLOPES).astype(np.float32)
    grad, div = stack_table(block.T), stack_table(block)
    q, tiles = rows // 4, cols // LANES
    groups = GROUPS if modes % GROUPS == 0 else 1
    per = modes // groups
    slots = -(-(per + 2) // 8) * 8
    vm = pl.BlockSpec(memory_space=pltpu.VMEM)
    hbm = pl.BlockSpec(memory_space=pltpu.HBM)
    rounds = (ITERS + 1) * groups
    ny, nz, nk, nx = planes(nc, ns)
    field = pltpu.VMEM((modes, rows, cols), f32)
    split = pltpu.VMEM((tiles, modes, rows, LANES), f32)
    table = pltpu.VMEM(grad.shape, bf16)
    line = pltpu.VMEM((1, LANES), f32)
    shape = jax.ShapeDtypeStruct(forcing.shape, f32)
    kept = pl.pallas_call(
        functools.partial(kernel, nc, ns, modes, groups),
        out_shape=[shape] * 5 + [jax.ShapeDtypeStruct((6, FIELD, LANES), f32)],
        in_specs=[hbm] * 6,
        out_specs=[vm] * 6,
        scratch_shapes=[
            field,
            pltpu.VMEM((modes + 2, rows, cols), f32),
            pltpu.VMEM((rows, cols), f32),
            pltpu.VMEM((rows, cols), f32),
            pltpu.VMEM((groups, per * rows, 2 * cols), bf16),
            pltpu.VMEM((per * rows, cols), f32),
            pltpu.VMEM((PRODUCTS, FIELD, cols), f32),
            pltpu.VMEM((rounds, 2, slots, cols), f32),
            pltpu.VMEM((rounds, 2, slots, cols), f32),
            pltpu.VMEM((rounds, 2, q, LANES), f32),
            pltpu.VMEM((rounds, 2, q, LANES), f32),
            pltpu.VMEM((rounds, 8, LANES), f32),
            pltpu.VMEM((rounds, 4, 1, LANES), f32),
            line,
            pltpu.VMEM((ny * nk * nx, 1, LANES), f32),
            line,
            pltpu.VMEM((nz, 1, LANES), f32),
            split,
            pltpu.VMEM((2, tiles, rows, LANES), f32),
            pltpu.VMEM((4 + 2 * slots * tiles + 2 * q, LANES), f32),
            table, table,
            pltpu.SMEM((modes,), f32),
            pltpu.SemaphoreType.DMA((rounds,)),
            pltpu.SemaphoreType.DMA((rounds,)),
            pltpu.SemaphoreType.DMA((groups,)),
            pltpu.SemaphoreType.DMA((2,)),
            pltpu.SemaphoreType.DMA((2,)),
            pltpu.SemaphoreType.DMA((2,)),
            pltpu.SemaphoreType.DMA((3,)),
        ],
        compiler_params=pltpu.CompilerParams(
            collective_id=0, has_side_effects=True, vmem_limit_bytes=41943040),
    )(*[pltpu.with_memory_space_constraint(v, pltpu.HBM) for v in (mode_scale, forcing, metric, jacobian, jnp.asarray(grad), jnp.asarray(div))])
    return pl.pallas_call(
        node_order,
        out_shape=[shape] * 2,
        in_specs=[vm] * 6,
        out_specs=[hbm, hbm],
        scratch_shapes=[split, split, pltpu.SemaphoreType.DMA((2, tiles, modes))],
        compiler_params=pltpu.CompilerParams(vmem_limit_bytes=16 * 1024 * 1024),
    )(*kept)


def solution(mesh):
    placed = (P(None, "curve", "sub"), P("curve", "sub"), P("curve", "sub"), P())
    return jax.shard_map(
        functools.partial(shards, mesh.shape["curve"], mesh.shape["sub"]),
        mesh=mesh,
        in_specs=placed,
        out_specs=(P(None, "curve", "sub"), P(None, "curve", "sub")),
        check_vma=False,
    )
```

```python
import functools
import math

import jax
import jax.numpy as jnp
import numpy as np
from jax import lax
from jax.experimental import pallas as pl
from jax.experimental.pallas import tpu as pltpu
from jax.sharding import PartitionSpec as P

ITERS = 3
GROUPS = 2
UNROLL = True
MESH = pl.DeviceIdType.MESH
LANES = 128
f32 = jnp.float32
bf16 = jnp.bfloat16


def gll_tables():
    points = np.array([-1.0, -1.0 / math.sqrt(5.0), 1.0 / math.sqrt(5.0), 1.0])
    weights = np.array([1.0 / 6.0, 5.0 / 6.0, 5.0 / 6.0, 1.0 / 6.0])
    factor = np.array(
        [np.prod([points[j] - points[m] for m in range(4) if m != j]) for j in range(4)]
    )
    slopes = np.zeros((4, 4))
    for i in range(4):
        for j in range(4):
            if i != j:
                slopes[i, j] = factor[i] / (factor[j] * (points[i] - points[j]))
        slopes[i, i] = sum((1.0 / (points[i] - points[m]) for m in range(4) if m != i))
    return (slopes, weights)


SLOPES, WEIGHTS = gll_tables()


def combo(coefs, parts):
    total = None
    for c, v in zip(coefs, parts):
        if abs(c) < 1e-12:
            continue
        term = v * f32(c)
        total = term if total is None else total + term
    return total


PRODUCTS = 6
FIELD = 16


def planes(nc, ns):
    depth = 8 if nc % 16 == 0 else 2
    return nc // (2 * depth), depth, 2, ns


def slope(z):
    even = (z[1] + z[2]) - (z[0] + z[3])
    outer, inner = z[3] - z[0], z[2] - z[1]
    half = 0.5 * (SLOPES[:, ::-1] - SLOPES)
    a = outer * f32(half[0, 0]) + inner * f32(half[0, 1])
    b = outer * f32(half[1, 0]) + inner * f32(half[1, 1])
    e0 = even * f32(0.5 * (SLOPES[0, 1] + SLOPES[0, 2]))
    e1 = even * f32(0.5 * (SLOPES[1, 1] + SLOPES[1, 2]))
    return [a + e0, b + e1, b - e1, a - e0]


def fall(f):
    s0, s1, d0, d1 = f[0] + f[3], f[1] + f[2], f[3] - f[0], f[2] - f[1]
    even = 0.5 * (SLOPES[:, 1] + SLOPES[:, 2])
    half = 0.5 * (SLOPES[:, ::-1] - SLOPES)
    x = d0 * f32(even[0]) + d1 * f32(even[1])
    y = s0 * f32(half[0, 0]) + s1 * f32(half[1, 0])
    v = s0 * f32(half[0, 1]) + s1 * f32(half[1, 1])
    return [x - y, (0.0 - x) - v, v - x, x + y]


def landed(ref, sem):
    pltpu.make_async_copy(ref, ref, sem).wait()


def kernel(
    nc, ns, modes, groups,
    scale_hbm, forcing_ref, metric_ref, jac_ref, grad_hbm, div_hbm,
    r0, r1, r2, u2, invp, coef,
    z, w, mass, flux, zcat, gout, sums,
    row_tx, row_rx, col_tx, col_rx, cor_tx, cor_rx, near_tx, near_rx, far_tx, far_rx,
    source, factors, gauge, grad_ref, div_ref, scale_ref,
    htx_sem, hrx_sem, crx_sem, atx_sem, arx_sem, in_sem, table_sem,
):
    rows, cols = metric_ref.shape
    q = rows // 4
    half = cols - LANES
    tiles = cols // LANES
    per = modes // groups
    slots = row_tx.shape[2]
    loads, sources = [], []
    for c in range(tiles):
        cut = pl.ds(c * LANES, LANES)
        loads += [
            pltpu.make_async_copy(jac_ref.at[:, cut], factors.at[0, c], in_sem.at[0]),
            pltpu.make_async_copy(metric_ref.at[:, cut], factors.at[1, c], in_sem.at[0]),
        ]
        sources.append(
            pltpu.make_async_copy(forcing_ref.at[:, :, cut], source.at[c], in_sem.at[1]))
    div_load = pltpu.make_async_copy(div_hbm, div_ref, table_sem.at[0])
    grad_load = pltpu.make_async_copy(grad_hbm, grad_ref, table_sem.at[1])
    scale_load = pltpu.make_async_copy(scale_hbm, scale_ref, table_sem.at[2])
    for copy in loads + sources + [div_load, scale_load, grad_load]:
        copy.start()

    me_c, me_s = lax.axis_index("curve"), lax.axis_index("sub")
    up, down = lax.rem(me_c + nc - 1, nc), lax.rem(me_c + 1, nc)
    left, right = lax.rem(me_s + ns - 1, ns), lax.rem(me_s + 1, ns)

    ny, nz, nk, nx = planes(nc, ns)
    core, chip = lax.rem(me_c, nk), me_c // nk
    at_z, at_y = lax.rem(chip, nz), chip // nz
    subs = [me_s if dx == 0 else lax.rem(me_s + dx, nx) for dx in range(nx)]
    ys = [at_y if dy == 0 else lax.rem(at_y + dy, ny) for dy in range(ny)]
    zs = [at_z if dz == 0 else lax.rem(at_z + dz, nz) for dz in range(nz)]

    def ring(step, size):
        return min(step, size - step)

    plane = sorted(
        [(dy, dk, dx) for dy in range(ny) for dk in range(nk) for dx in range(nx)][1:],
        key=lambda o: -(2 * ring(o[0], ny) + o[1] + 2 * ring(o[2], nx)))
    near = [((ys[dy] * nz + at_z) * nk + (1 - core if dk else core), subs[dx])
            for dy, dk, dx in plane]
    line_z = sorted(range(1, nz), key=lambda dz: -ring(dz, nz))
    far = [((at_y * nz + zs[dz]) * nk + core, me_s) for dz in line_z]

    barrier = pltpu.get_barrier_semaphore()
    greeted = [
        (up, left), (up, right), (down, left), (down, right)]
    greeted += [((ys[dy] * nz + at_z) * nk + core, me_s) for dy in range(1, ny)]
    greeted += [((at_y * nz + zs[dz]) * nk + core, me_s)
                for dz in sorted({1, 2, nz - 1, nz - 2} - {0, nz})]
    greeted += [(up, me_s), (down, me_s), (me_c, left), (me_c, right)]
    for where in greeted:
        pl.semaphore_signal(barrier, inc=1, device_id=where, device_id_type=MESH)

    lane_full = lax.broadcasted_iota(jnp.int32, (q, cols), 1)
    lane = lax.broadcasted_iota(jnp.int32, (q, LANES), 1)
    row_at = lax.broadcasted_iota(jnp.int32, (q, cols), 0)
    phase = lane_full % 4
    on_edge = (phase == 0) | (phase == 3)
    take_next = (phase == 3) & (lane_full != cols - 1)
    take_prev = (phase == 0) & (lane_full != 0)

    def load(ref, m):
        return [ref[m, p * q:(p + 1) * q, :] for p in range(4)]

    def save(ref, m, parts):
        for p in range(4):
            ref[m, p * q:(p + 1) * q, :] = parts[p]

    def load2(ref):
        return [ref[p * q:(p + 1) * q, :] for p in range(4)]

    def pack(k, m, slot, h, tops):
        lo, hi = tops
        row_tx[k, 0, pl.ds(slot, 1), :] = h[0][0:1, :]
        row_tx[k, 1, pl.ds(slot, 1), :] = h[3][q - 1:q, :]
        t0 = h[0] + jnp.where(row_at == 0, 0.0, pltpu.roll(h[3], 1, 0))
        t3 = h[3] + jnp.where(row_at == q - 1, 0.0, pltpu.roll(h[0], q - 1, 0))
        t = [t0, h[1], h[2], t3]
        save(w, m, t)
        for p in range(4):
            at = 4 * slot + p
            lo = jnp.where(lane == at, pltpu.roll(t[p][:, :LANES], at, 1), lo)
            hi = jnp.where(lane == at, pltpu.roll(t[p][:, half:], at + 1, 1), hi)
        return lo, hi

    def early(k):
        return groups <= k < ITERS * groups

    def halo_copies(k):
        if early(k):
            corners = [cor_tx.at[k, pl.ds(2 * e, 1)] for e in range(4)]
        else:
            corners = [col_tx.at[k, e % 2, pl.ds(0 if e < 2 else q - 1, 1)] for e in range(4)]
        plan = [
            (corners[0], cor_rx.at[k, 3], (up, left)),
            (corners[1], cor_rx.at[k, 2], (up, right)),
            (corners[2], cor_rx.at[k, 1], (down, left)),
            (corners[3], cor_rx.at[k, 0], (down, right)),
            (row_tx.at[k, 0], row_rx.at[k, 1], (up, me_s)),
            (row_tx.at[k, 1], row_rx.at[k, 0], (down, me_s)),
            (col_tx.at[k, 0], col_rx.at[k, 1], (me_c, left)),
            (col_tx.at[k, 1], col_rx.at[k, 0], (me_c, right)),
        ]
        return [
            pltpu.make_async_remote_copy(
                src_ref=src, dst_ref=dst, send_sem=htx_sem.at[k],
                recv_sem=crx_sem.at[k] if k < groups and e < 4 else hrx_sem.at[k],
                device_id=where, device_id_type=MESH)
            for e, (src, dst, where) in enumerate(plan)
        ]

    def send(k, tops):
        col_tx[k, 0], col_tx[k, 1] = tops
        for copy in halo_copies(k)[4 if early(k) else 0:]:
            copy.start()

    def arrive(k):
        if k < groups:
            landed(gauge.at[pl.ds(0, 4)], crx_sem.at[k])
        else:
            landed(gauge, hrx_sem.at[k])
        ph = lax.broadcasted_iota(jnp.int32, (1, LANES), 1) % 4
        edge_row = lax.broadcasted_iota(jnp.int32, (q, LANES), 0)
        merged = []
        for side in range(2):
            above, below = cor_rx[k, side], cor_rx[k, 2 + side]
            above = jnp.where(ph == 0, pltpu.roll(above, LANES - 3, 1), 0.0)
            below = jnp.where(ph == 3, pltpu.roll(below, 3, 1), 0.0)
            c = col_rx[k, side]
            c = c + jnp.where(edge_row == 0, above, 0.0) + jnp.where(edge_row == q - 1, below, 0.0)
            merged.append(c)
        return merged

    few_rows = lax.broadcasted_iota(jnp.int32, (8, cols), 0)
    few_at = lax.broadcasted_iota(jnp.int32, (8, cols), 1)
    few_lane = lax.broadcasted_iota(jnp.int32, (8, LANES), 1)
    few_next = (few_at % 4 == 3) & (few_at != cols - 1)
    few_prev = (few_at % 4 == 0) & (few_at != 0)
    few_edge = (few_at % 4 == 3) | (few_at % 4 == 0)
    chunks = q // 8

    def chunk(ref, m, n):
        return [ref[m, p * q + 8 * n:p * q + 8 * n + 8, :] for p in range(4)]

    def chunk2(ref, n):
        return [ref[p * q + 8 * n:p * q + 8 * n + 8, :] for p in range(4)]

    def keep(ref, m, n, parts):
        for p in range(4):
            ref[m, p * q + 8 * n:p * q + 8 * n + 8, :] = parts[p]

    def joined(k, m, slot, merged, n):
        t = chunk(w, m, n)
        if n == 0:
            t[0] = t[0] + jnp.where(few_rows == 0, row_rx[k, 0, pl.ds(slot, 1), :], 0.0)
        if n == chunks - 1:
            t[3] = t[3] + jnp.where(few_rows == 7, row_rx[k, 1, pl.ds(slot, 1), :], 0.0)
        near_side, far_side = [v[8 * n:8 * n + 8] for v in merged]
        out = []
        for p in range(4):
            at = 4 * slot + p
            c = t[p] + jnp.where(
                few_next, pltpu.roll(t[p], cols - 1, 1),
                jnp.where(few_prev, pltpu.roll(t[p], 1, 1), 0.0))
            a = jnp.where(few_lane == 0, pltpu.roll(near_side, LANES - at, 1), 0.0)
            b = jnp.where(few_lane == LANES - 1, pltpu.roll(far_side, LANES - 1 - at, 1), 0.0)
            pieces = [c[:, e * LANES:(e + 1) * LANES] for e in range(tiles)]
            pieces[0] = pieces[0] + a
            pieces[-1] = pieces[-1] + b
            out.append(jnp.concatenate(pieces, axis=1))
        return out

    edge_w, mid_w = f32(1.0 / 6.0), f32(5.0 / 6.0)
    col_w = jnp.where(on_edge, edge_w, mid_w)
    mw, fw = [], []
    landed(factors, in_sem.at[0])
    for p in range(4):
        grid_w = col_w * (edge_w if p in (0, 3) else mid_w)
        mw.append(strided([factors.at[0, c] for c in range(tiles)], p, q) * grid_w)
        fw.append(strided([factors.at[1, c] for c in range(tiles)], p, q) * grid_w)
        mass[p * q:(p + 1) * q, :] = mw[p]
        flux[p * q:(p + 1) * q, :] = fw[p]
    zero = jnp.zeros((q, LANES), f32)
    tops = pack(0, modes, per, mw, (zero, zero))
    div_load.wait()
    table = div_ref[:cols, :].astype(f32) + div_ref[2 * cols:, :].astype(f32)
    by_cols = jnp.dot(flux[...], table * table, precision=lax.Precision.HIGHEST,
                      preferred_element_type=f32)
    squared = SLOPES * SLOPES
    lap = [combo(squared[:, a], fw) + by_cols[a * q:(a + 1) * q, :] for a in range(4)]
    tops = pack(0, modes + 1, per + 1, lap, tops)
    landed(source, in_sem.at[1])
    for g in range(groups):

        def start_body(slot, carry, g=g):
            m = g * per + slot
            h = [strided([source.at[c, m] for c in range(tiles)], p, q)
                 * mass[p * q:(p + 1) * q, :] for p in range(4)]
            return pack(g, m, slot, h, carry)

        tops = lax.fori_loop(0, per, start_body, tops if g == 0 else (zero, zero), unroll=UNROLL)
        if g == 0:
            pl.semaphore_wait(barrier, len(greeted))
        send(g, tops)
    scale_load.wait()
    grad_load.wait()

    at_lane = lax.broadcasted_iota(jnp.int32, (1, LANES), 1)
    of_four = at_lane % 4
    tall = lax.broadcasted_iota(jnp.int32, (slots, LANES), 0)
    flat = lax.broadcasted_iota(jnp.int32, (slots, LANES), 1)
    low_half = tall < 4

    def coefs(values):
        line = jnp.zeros((1, LANES), f32)
        for e, value in enumerate(values):
            line = jnp.where(of_four == e, f32(value), line)
        return line

    def corner_weights(g):
        scale = jnp.zeros((1, LANES), f32)
        for slot in range(per):
            scale = jnp.where(at_lane // 4 == slot, scale_ref[g * per + slot], scale)
        lines = []
        for tb in range(2):
            er, cr = (0, 0) if tb == 0 else (q - 1, 3)
            for side in range(2):
                cc, edge, start = (0, 0, 0) if side == 0 else (3, cols - 1, cols - 4)
                sx = jnp.zeros((1, LANES), f32)
                sy = jnp.zeros((1, LANES), f32)
                own = jnp.zeros((1, 1), f32)
                for e in range(4):
                    fx = flux[e * q + er:e * q + er + 1, edge:edge + 1]
                    fy = flux[cr * q + er:cr * q + er + 1, start + e:start + e + 1]
                    sx = sx + fx * coefs(SLOPES[e, cr] * SLOPES[e])
                    sy = sy + fy * coefs(SLOPES[e, cc] * SLOPES[e])
                    own = own + fy * f32(SLOPES[e, cc] * SLOPES[e, cc])
                here = mass[cr * q + er:cr * q + er + 1, edge:edge + 1]
                lines += [
                    scale * sx + jnp.where(of_four == cr, here + scale * own, 0.0),
                    jnp.where(of_four == cc, 0.0, scale * sy)]
        return scale, jnp.concatenate(lines, axis=0)

    def gathered_rows(x):
        left = x[:, :LANES]
        left = left + jnp.where(flat == 3, pltpu.roll(left, LANES - 1, 1), 0.0)
        right = x[:, half:]
        right = right + jnp.where(flat == LANES - 4, pltpu.roll(right, 1, 1), 0.0)
        left = pltpu.roll(jnp.where(flat < 4, left, 0.0), 0, 1, stride=4, stride_axis=0)
        right = pltpu.roll(
            jnp.where(flat >= LANES - 4, right, 0.0), 4, 1, stride=4, stride_axis=0)
        return [jnp.sum(v, axis=0, keepdims=True) for v in (left, right)]

    def corner_values(k, merged):
        lines = []
        for tb in range(2):
            er, cr = (0, 0) if tb == 0 else (q - 1, 3)
            halo = row_rx[k, tb]
            rows_here = gathered_rows(row_tx[k, tb] + halo)
            for side in range(2):
                edge = 0 if side == 0 else cols - 1
                place = flat == 4 * tall + cr
                extra = jnp.sum(
                    jnp.where(place, halo[:, edge:edge + 1], 0.0), axis=0, keepdims=True)
                col = col_tx[k, side, er:er + 1, :] + merged[side][er:er + 1, :] + extra
                lines += [col, rows_here[side]]
        return jnp.concatenate(lines, axis=0)

    def set_corners(k, weights, v):
        h = weights * v
        fore = h + pltpu.roll(h, LANES - 1, 1)
        fore = fore + pltpu.roll(fore, LANES - 2, 1)
        back = h + pltpu.roll(h, 1, 1)
        back = back + pltpu.roll(back, 2, 1)
        h = jnp.where(low_half, fore, back)
        cor_tx[k] = h + pltpu.roll(h, slots - 1, 0)

    def repeat(x, slot):
        x = jnp.where(flat // 4 == slot, x, 0.0)
        x = pltpu.roll(x, LANES - 4 * slot, 1)
        for step in (4, 8, 16):
            x = x + pltpu.roll(x, step, 1)
        return x

    assert slots == 8
    corner = [corner_weights(g) for g in range(groups)]
    corner_r, corner_inv, shared_diag = [None] * groups, [None] * groups, []

    def corner_step(it, g, k, merged):
        u = corner_values(k, merged)
        scale, weights = corner[g]
        if it == 0:
            if g == 0:
                shared_diag.extend([repeat(u, per), repeat(u, per + 1)])
            used = flat < 4 * per
            u = jnp.where(used, u, 0.0)
            corner_r[g] = u
            corner_inv[g] = jnp.where(used, 1.0 / jnp.where(
                used, shared_diag[0] + scale * shared_diag[1], 1.0), 0.0)
            r = u
        else:
            r = jnp.where(flat < 4 * per, u, 0.0) - corner_r[g]
        set_corners(k + groups, weights, r * corner_inv[g])

    def fill(g, slot, n, parts):
        v = jnp.concatenate(parts, axis=0)
        top = v.astype(bf16)
        at = pl.ds(pl.multiple_of(slot * rows + 32 * n, 32), 32)
        zcat[g, at, :cols] = top
        zcat[g, at, cols:] = (v - top.astype(f32)).astype(bf16)

    def taken(slot, n):
        return [gout[pl.ds(pl.multiple_of(slot * rows + 32 * n + 8 * p, 8), 8), :]
                for p in range(4)]

    def multiply(g, table_ref, part):
        lo, hi = part[0] * rows, part[1] * rows
        gout[lo:hi] = (
            jnp.dot(zcat[g, lo:hi, :], table_ref[:2 * cols, :], preferred_element_type=f32)
            + jnp.dot(zcat[g, lo:hi, :cols], table_ref[2 * cols:, :],
                      preferred_element_type=f32))

    cut = (per + 1) // 2
    parts_of = [(0, cut), (cut, per)]

    def over(part, body, carry=0):
        return lax.fori_loop(part[0], part[1], body, carry, unroll=UNROLL)

    def total(parts):
        return (parts[0] + parts[3]) + (parts[1] + parts[2])

    def shared(parts):
        return (parts[0] + parts[3]) * 0.5 + (parts[1] + parts[2])

    def put(e, m, line):
        sums[e, pl.ds(m, 1), :] = jnp.sum(line, axis=0, keepdims=True)

    def finish(g, k, base):
        def third(slot, carry):
            m = base + slot
            h, line = [], 0.0
            for n in range(chunks):
                zz = chunk(z, m, n)
                part = [t * u + scale_ref[m] * (v + s) for t, u, v, s in zip(
                    chunk2(mass, n), zz, chunk(w, m, n), taken(slot, n))]
                if k < ITERS - 1:
                    line = line + total([u * v for u, v in zip(zz, part)])
                h.append(part)
            if k < ITERS - 1:
                put(2 * k + 1, m, line)
            h = [jnp.concatenate([part[p] for part in h], axis=0) for p in range(4)]
            return pack((k + 1) * groups + g, m, slot, h, carry)

        return third

    def patched(k, slot, n, parts):
        parts = list(parts)
        for at_n, p, row, lines, at in (
                (0, 0, 0, (0, 1), 4 * slot + 3), (chunks - 1, 3, 7, (2, 3), 4 * slot)):
            if n != at_n:
                continue
            a = pltpu.roll(cor_rx[k, lines[0]], LANES - at, 1)
            b = pltpu.roll(cor_rx[k, lines[1]], LANES - 1 - at, 1)
            here = few_rows[:, :LANES] == row
            pieces = [parts[p][:, e * LANES:(e + 1) * LANES] for e in range(tiles)]
            pieces[0] = pieces[0] + jnp.where(here & (few_lane == 0), a, 0.0)
            pieces[-1] = pieces[-1] + jnp.where(here & (few_lane == LANES - 1), b, 0.0)
            parts[p] = jnp.concatenate(pieces, axis=1)
        return parts

    for g in range(groups):
        landed(gauge.at[pl.ds(0, gauge.shape[0] - 4)], hrx_sem.at[g])
        sides = [col_rx[g, 0], col_rx[g, 1]]
        pairs = [(modes, per), (modes + 1, per + 1)] if g == 0 else []
        for m, slot in pairs + [(g * per + e, e) for e in range(per)]:
            for n in range(chunks):
                keep(w, m, n, joined(g, m, slot, sides, n))

    for it in range(ITERS):
        for g in range(groups):
            base = g * per
            k = it * groups + g
            merged = arrive(k)
            if it < ITERS - 1:
                corner_step(it, g, k, merged)
            if it == 0 and g == 0:
                for e in range(2):
                    for n in (0, chunks - 1):
                        keep(w, modes + e, n, patched(k, per + e, n, chunk(w, modes + e, n)))

            def first(slot, carry, it=it, g=g, k=k, base=base, merged=merged):
                m = base + slot
                line, energy = 0.0, 0.0
                for n in range(chunks):
                    if it == 0:
                        uu = patched(k, slot, n, chunk(w, m, n))
                    else:
                        uu = joined(k, m, slot, merged, n)
                    if it == 0:
                        rr = uu
                        inv = [1.0 / (u + scale_ref[m] * v)
                               for u, v in zip(chunk(w, modes, n), chunk(w, modes + 1, n))]
                        keep(invp, m, n, inv)
                    elif it == 1:
                        rr = [u - v for u, v in zip(uu, chunk(r0, m, n))]
                        inv = chunk(invp, m, n)
                    else:
                        rr = [2.0 * (u - v) - s for u, v, s in zip(
                            uu, chunk(r1, m, n), chunk(r0, m, n))]
                        inv = chunk(invp, m, n)
                    keep((r0, r1, r2)[it], m, n, rr)
                    zz = [u * v for u, v in zip(rr, inv)]
                    keep(z, m, n, zz)
                    fill(g, slot, n, zz)
                    line = line + shared([u * v for u, v in zip(uu, zz)])
                    gx = slope(zz)
                    fg = [u * v for u, v in zip(chunk2(flux, n), gx)]
                    keep(w, m, n, fall(fg))
                    if it == ITERS - 1:
                        energy = energy + (
                            total([t * u * u for t, u in zip(chunk2(mass, n), zz)])
                            + scale_ref[m] * total([u * v for u, v in zip(fg, gx)]))
                put(2 * it, m, jnp.where(few_edge, line * 0.5, line))
                if it == ITERS - 1:
                    put(2 * it + 1, m, energy)
                return carry

            if it < ITERS - 1:
                for copy in halo_copies(k + groups)[:4]:
                    copy.start()
            def second(slot, carry, it=it, g=g, base=base):
                m, e, line = base + slot, 2 * it + 1, 0.0
                for n in range(chunks):
                    grad = taken(slot, n)
                    fy = [u * v for u, v in zip(chunk2(flux, n), grad)]
                    if it == ITERS - 1:
                        line = line + total([u * v for u, v in zip(fy, grad)])
                    fill(g, slot, n, fy)
                if it == ITERS - 1:
                    sums[e, pl.ds(m, 1), :] = sums[e, pl.ds(m, 1), :] + scale_ref[m] * jnp.sum(
                        line, axis=0, keepdims=True)
                return carry

            one, two = parts_of
            over(one, first)
            multiply(g, grad_ref, one)
            over(two, first)
            over(one, second)
            multiply(g, grad_ref, two)
            if it < ITERS - 1:
                third = finish(g, it, base)
                multiply(g, div_ref, one)
                over(two, second)
                tops = over(one, third, (zero, zero))
                multiply(g, div_ref, two)
                send(k + groups, over(two, third, tops))
            else:
                over(two, second)

    high = lax.broadcasted_iota(jnp.int32, (FIELD, LANES), 0)
    wide = lax.broadcasted_iota(jnp.int32, (FIELD, LANES), 1)
    picks = [(wide == e * FIELD + high) & (high < modes) for e in range(PRODUCTS)]
    spread = jnp.zeros((FIELD, LANES), f32)
    for e in range(PRODUCTS):
        part = jnp.sum(sums[e], axis=1, keepdims=True)
        spread = spread + jnp.where(picks[e], part, 0.0)
    line = jnp.sum(spread, axis=0, keepdims=True)

    def share(stage, line, tx, rx, peers):
        tx[...] = line
        rx[0] = line
        for j, where in enumerate(peers):
            pltpu.make_async_remote_copy(
                src_ref=tx, dst_ref=rx.at[j + 1], send_sem=atx_sem.at[stage],
                recv_sem=arx_sem.at[stage], device_id=where, device_id_type=MESH).start()

    def gather(stage, rx):
        landed(rx.at[pl.ds(1, rx.shape[0] - 1)], arx_sem.at[stage])
        return jnp.sum(rx[...], axis=0)

    share(0, line, near_tx, near_rx, near)
    for g in range(groups):
        third = finish(g, ITERS - 1, g * per)
        multiply(g, div_ref, one)
        tops = over(one, third, (zero, zero))
        multiply(g, div_ref, two)
        send(ITERS * groups + g, over(two, third, tops))
    share(1, gather(0, near_rx), far_tx, far_rx, far)
    for g in range(groups):
        k = ITERS * groups + g
        merged = arrive(k)

        def last(slot, carry, g=g, k=k, merged=merged):
            m = g * per + slot
            for n in range(chunks):
                keep(u2, m, n, joined(k, m, slot, merged, n))
            return carry

        lax.fori_loop(0, per, last, 0, unroll=UNROLL)

    total = gather(1, far_rx)
    pad = (high[:, :1] >= modes).astype(f32)
    n0, p00, p01, p11, p12, p22 = [
        jnp.broadcast_to(
            jnp.sum(jnp.where(pick, total, 0.0), axis=1, keepdims=True), (FIELD, LANES))
        for pick in picks]
    pad = jnp.broadcast_to(pad, (FIELD, LANES))
    p00, p11, p22 = p00 + pad, p11 + pad, p22 + 2.0 * pad
    b0 = n0
    b1 = p00 - n0
    b2 = 2.0 * (p01 - b1) - n0
    p02 = 2.0 * p11 - p00
    i0 = 1.0 / p00
    l1, l2 = p01 * i0, p02 * i0
    d1 = p11 - l1 * p01
    t2 = p12 - l2 * p01
    i1 = 1.0 / d1
    l3 = t2 * i1
    d2 = p22 - l2 * p02 - l3 * t2
    y1 = b1 - l1 * b0
    y2 = b2 - l2 * b0 - l3 * y1
    c2 = y2 / d2
    c1 = y1 * i1 - l3 * c2
    c0 = b0 * i0 - l1 * c1 - l2 * c2
    for e, c in enumerate((c0, c1, c2, 1.0 - c0 - 0.5 * c1, c0 + c1, 0.5 * c1)):
        coef[e] = c

    for k in range((ITERS + 1) * groups):
        landed(gauge, htx_sem.at[k])
    for stage, rx in enumerate((near_rx, far_rx)):
        landed(rx.at[pl.ds(1, rx.shape[0] - 1)], atx_sem.at[stage])


def node_order(r0, r1, r2, u2, invp, coef, sol_ref, res_ref, sol_buf, res_buf, sem):
    modes, rows, cols = r0.shape
    q, tiles = rows // 4, cols // LANES

    def stores(m):
        return [
            pltpu.make_async_copy(
                buf.at[c, m], out.at[m, :, pl.ds(c * LANES, LANES)], sem.at[k, c, m])
            for k, (buf, out) in enumerate(((sol_buf, sol_ref), (res_buf, res_ref)))
            for c in range(tiles)
        ]

    def body(m, carry):
        c0, c1, c2, e0, e1, e2 = [coef[e, pl.ds(m, 1), :] for e in range(6)]
        for c in range(tiles):
            for p in range(4):
                at = (m, slice(p * q, (p + 1) * q), slice(c * LANES, (c + 1) * LANES))
                a0, a1, a2 = r0[at], r1[at], r2[at]
                sol_buf[c, m, pl.ds(p, q, stride=4), :] = invp[at] * (c0 * a0 + c1 * a1 + c2 * a2)
                res_buf[c, m, pl.ds(p, q, stride=4), :] = (
                    e0 * a0 - e1 * a1 - e2 * a2 - c2 * u2[at])
        for copy in stores(m):
            copy.start()
        return carry

    lax.fori_loop(0, modes, body, 0)

    def drain(m, carry):
        for copy in stores(m):
            copy.wait()
        return carry

    lax.fori_loop(0, modes, drain, 0)


def strided(refs, p, q):
    return jnp.concatenate([ref[pl.ds(p, q, stride=4), :] for ref in refs], axis=1)


def stack_table(table):
    top = table.astype(bf16)
    low = (table - top.astype(np.float32)).astype(bf16)
    return np.concatenate([top, top, low], axis=0)


def shards(nc, ns, forcing, metric, jacobian, mode_scale):
    modes, rows, cols = forcing.shape
    block = np.kron(np.eye(cols // 4), SLOPES).astype(np.float32)
    grad, div = stack_table(block.T), stack_table(block)
    q, tiles = rows // 4, cols // LANES
    groups = GROUPS if modes % GROUPS == 0 else 1
    per = modes // groups
    slots = -(-(per + 2) // 8) * 8
    vm = pl.BlockSpec(memory_space=pltpu.VMEM)
    hbm = pl.BlockSpec(memory_space=pltpu.HBM)
    rounds = (ITERS + 1) * groups
    ny, nz, nk, nx = planes(nc, ns)
    field = pltpu.VMEM((modes, rows, cols), f32)
    split = pltpu.VMEM((tiles, modes, rows, LANES), f32)
    table = pltpu.VMEM(grad.shape, bf16)
    line = pltpu.VMEM((1, LANES), f32)
    shape = jax.ShapeDtypeStruct(forcing.shape, f32)
    kept = pl.pallas_call(
        functools.partial(kernel, nc, ns, modes, groups),
        out_shape=[shape] * 5 + [jax.ShapeDtypeStruct((6, FIELD, LANES), f32)],
        in_specs=[hbm] * 6,
        out_specs=[vm] * 6,
        scratch_shapes=[
            field,
            pltpu.VMEM((modes + 2, rows, cols), f32),
            pltpu.VMEM((rows, cols), f32),
            pltpu.VMEM((rows, cols), f32),
            pltpu.VMEM((groups, per * rows, 2 * cols), bf16),
            pltpu.VMEM((per * rows, cols), f32),
            pltpu.VMEM((PRODUCTS, FIELD, cols), f32),
            pltpu.VMEM((rounds, 2, slots, cols), f32),
            pltpu.VMEM((rounds, 2, slots, cols), f32),
            pltpu.VMEM((rounds, 2, q, LANES), f32),
            pltpu.VMEM((rounds, 2, q, LANES), f32),
            pltpu.VMEM((rounds, 8, LANES), f32),
            pltpu.VMEM((rounds, 4, 1, LANES), f32),
            line,
            pltpu.VMEM((ny * nk * nx, 1, LANES), f32),
            line,
            pltpu.VMEM((nz, 1, LANES), f32),
            split,
            pltpu.VMEM((2, tiles, rows, LANES), f32),
            pltpu.VMEM((4 + 2 * slots * tiles + 2 * q, LANES), f32),
            table, table,
            pltpu.SMEM((modes,), f32),
            pltpu.SemaphoreType.DMA((rounds,)),
            pltpu.SemaphoreType.DMA((rounds,)),
            pltpu.SemaphoreType.DMA((groups,)),
            pltpu.SemaphoreType.DMA((2,)),
            pltpu.SemaphoreType.DMA((2,)),
            pltpu.SemaphoreType.DMA((2,)),
            pltpu.SemaphoreType.DMA((3,)),
        ],
        compiler_params=pltpu.CompilerParams(
            collective_id=0, has_side_effects=True, vmem_limit_bytes=41943040),
    )(*[pltpu.with_memory_space_constraint(v, pltpu.HBM) for v in (mode_scale, forcing, metric, jacobian, jnp.asarray(grad), jnp.asarray(div))])
    return pl.pallas_call(
        node_order,
        out_shape=[shape] * 2,
        in_specs=[vm] * 6,
        out_specs=[hbm, hbm],
        scratch_shapes=[split, split, pltpu.SemaphoreType.DMA((2, tiles, modes))],
        compiler_params=pltpu.CompilerParams(vmem_limit_bytes=16 * 1024 * 1024),
    )(*kept)


def solution(mesh):
    placed = (P(None, "curve", "sub"), P("curve", "sub"), P("curve", "sub"), P())
    return jax.shard_map(
        functools.partial(shards, mesh.shape["curve"], mesh.shape["sub"]),
        mesh=mesh,
        in_specs=placed,
        out_specs=(P(None, "curve", "sub"), P(None, "curve", "sub")),
        check_vma=False,
    )
```

```python
import functools
import math

import jax
import jax.numpy as jnp
import numpy as np
from jax import lax
from jax.experimental import pallas as pl
from jax.experimental.pallas import tpu as pltpu
from jax.sharding import PartitionSpec as P

ITERS = 3
GROUPS = 2
UNROLL = True
MESH = pl.DeviceIdType.MESH
LANES = 128
f32 = jnp.float32
bf16 = jnp.bfloat16


def gll_tables():
    points = np.array([-1.0, -1.0 / math.sqrt(5.0), 1.0 / math.sqrt(5.0), 1.0])
    weights = np.array([1.0 / 6.0, 5.0 / 6.0, 5.0 / 6.0, 1.0 / 6.0])
    factor = np.array(
        [np.prod([points[j] - points[m] for m in range(4) if m != j]) for j in range(4)]
    )
    slopes = np.zeros((4, 4))
    for i in range(4):
        for j in range(4):
            if i != j:
                slopes[i, j] = factor[i] / (factor[j] * (points[i] - points[j]))
        slopes[i, i] = sum((1.0 / (points[i] - points[m]) for m in range(4) if m != i))
    return (slopes, weights)


SLOPES, WEIGHTS = gll_tables()


def combo(coefs, parts):
    total = None
    for c, v in zip(coefs, parts):
        if abs(c) < 1e-12:
            continue
        term = v * f32(c)
        total = term if total is None else total + term
    return total


PRODUCTS = 6
FIELD = 16


def planes(nc, ns):
    depth = 8 if nc % 16 == 0 else 2
    return nc // (2 * depth), depth, 2, ns


def slope(z):
    even = (z[1] + z[2]) - (z[0] + z[3])
    outer, inner = z[3] - z[0], z[2] - z[1]
    half = 0.5 * (SLOPES[:, ::-1] - SLOPES)
    a = outer * f32(half[0, 0]) + inner * f32(half[0, 1])
    b = outer * f32(half[1, 0]) + inner * f32(half[1, 1])
    e0 = even * f32(0.5 * (SLOPES[0, 1] + SLOPES[0, 2]))
    e1 = even * f32(0.5 * (SLOPES[1, 1] + SLOPES[1, 2]))
    return [a + e0, b + e1, b - e1, a - e0]


def fall(f):
    s0, s1, d0, d1 = f[0] + f[3], f[1] + f[2], f[3] - f[0], f[2] - f[1]
    even = 0.5 * (SLOPES[:, 1] + SLOPES[:, 2])
    half = 0.5 * (SLOPES[:, ::-1] - SLOPES)
    x = d0 * f32(even[0]) + d1 * f32(even[1])
    y = s0 * f32(half[0, 0]) + s1 * f32(half[1, 0])
    v = s0 * f32(half[0, 1]) + s1 * f32(half[1, 1])
    return [x - y, (0.0 - x) - v, v - x, x + y]


def landed(ref, sem):
    pltpu.make_async_copy(ref, ref, sem).wait()


def kernel(
    nc, ns, modes, groups,
    scale_hbm, forcing_ref, metric_ref, jac_ref, grad_hbm, div_hbm,
    r0, r1, r2, u2, invp, coef,
    z, w, mass, flux, zcat, gout, sums,
    row_tx, row_rx, col_tx, col_rx, cor_tx, cor_rx, near_tx, near_rx, far_tx, far_rx,
    source, factors, gauge, grad_ref, div_ref, scale_ref,
    htx_sem, hrx_sem, crx_sem, atx_sem, arx_sem, in_sem, table_sem,
):
    rows, cols = metric_ref.shape
    q = rows // 4
    half = cols - LANES
    tiles = cols // LANES
    per = modes // groups
    slots = row_tx.shape[2]
    loads, sources = [], []
    for c in range(tiles):
        cut = pl.ds(c * LANES, LANES)
        loads += [
            pltpu.make_async_copy(jac_ref.at[:, cut], factors.at[0, c], in_sem.at[0]),
            pltpu.make_async_copy(metric_ref.at[:, cut], factors.at[1, c], in_sem.at[0]),
        ]
        sources.append(
            pltpu.make_async_copy(forcing_ref.at[:, :, cut], source.at[c], in_sem.at[1]))
    div_load = pltpu.make_async_copy(div_hbm, div_ref, table_sem.at[0])
    grad_load = pltpu.make_async_copy(grad_hbm, grad_ref, table_sem.at[1])
    scale_load = pltpu.make_async_copy(scale_hbm, scale_ref, table_sem.at[2])
    for copy in loads + sources + [div_load, scale_load, grad_load]:
        copy.start()

    me_c, me_s = lax.axis_index("curve"), lax.axis_index("sub")
    up, down = lax.rem(me_c + nc - 1, nc), lax.rem(me_c + 1, nc)
    left, right = lax.rem(me_s + ns - 1, ns), lax.rem(me_s + 1, ns)

    ny, nz, nk, nx = planes(nc, ns)
    core, chip = lax.rem(me_c, nk), me_c // nk
    at_z, at_y = lax.rem(chip, nz), chip // nz
    subs = [me_s if dx == 0 else lax.rem(me_s + dx, nx) for dx in range(nx)]
    ys = [at_y if dy == 0 else lax.rem(at_y + dy, ny) for dy in range(ny)]
    zs = [at_z if dz == 0 else lax.rem(at_z + dz, nz) for dz in range(nz)]

    def ring(step, size):
        return min(step, size - step)

    plane = sorted(
        [(dy, dk, dx) for dy in range(ny) for dk in range(nk) for dx in range(nx)][1:],
        key=lambda o: -(2 * ring(o[0], ny) + o[1] + 2 * ring(o[2], nx)))
    near = [((ys[dy] * nz + at_z) * nk + (1 - core if dk else core), subs[dx])
            for dy, dk, dx in plane]
    line_z = sorted(range(1, nz), key=lambda dz: -ring(dz, nz))
    far = [((at_y * nz + zs[dz]) * nk + core, me_s) for dz in line_z]

    barrier = pltpu.get_barrier_semaphore()
    greeted = [
        (up, left), (up, right), (down, left), (down, right)]
    greeted += [((ys[dy] * nz + at_z) * nk + core, me_s) for dy in range(1, ny)]
    greeted += [((at_y * nz + zs[dz]) * nk + core, me_s)
                for dz in sorted({1, 2, nz - 1, nz - 2} - {0, nz})]
    greeted += [(up, me_s), (down, me_s), (me_c, left), (me_c, right)]
    for where in greeted:
        pl.semaphore_signal(barrier, inc=1, device_id=where, device_id_type=MESH)

    lane_full = lax.broadcasted_iota(jnp.int32, (q, cols), 1)
    lane = lax.broadcasted_iota(jnp.int32, (q, LANES), 1)
    row_at = lax.broadcasted_iota(jnp.int32, (q, cols), 0)
    phase = lane_full % 4
    on_edge = (phase == 0) | (phase == 3)
    take_next = (phase == 3) & (lane_full != cols - 1)
    take_prev = (phase == 0) & (lane_full != 0)

    def load(ref, m):
        return [ref[m, p * q:(p + 1) * q, :] for p in range(4)]

    def save(ref, m, parts):
        for p in range(4):
            ref[m, p * q:(p + 1) * q, :] = parts[p]

    def load2(ref):
        return [ref[p * q:(p + 1) * q, :] for p in range(4)]

    def pack(k, m, slot, h, tops):
        lo, hi = tops
        row_tx[k, 0, pl.ds(slot, 1), :] = h[0][0:1, :]
        row_tx[k, 1, pl.ds(slot, 1), :] = h[3][q - 1:q, :]
        t0 = h[0] + jnp.where(row_at == 0, 0.0, pltpu.roll(h[3], 1, 0))
        t3 = h[3] + jnp.where(row_at == q - 1, 0.0, pltpu.roll(h[0], q - 1, 0))
        t = [t0, h[1], h[2], t3]
        save(w, m, t)
        for p in range(4):
            at = 4 * slot + p
            lo = jnp.where(lane == at, pltpu.roll(t[p][:, :LANES], at, 1), lo)
            hi = jnp.where(lane == at, pltpu.roll(t[p][:, half:], at + 1, 1), hi)
        return lo, hi

    def early(k):
        return groups <= k < ITERS * groups

    def halo_copies(k):
        if early(k):
            corners = [cor_tx.at[k, pl.ds(2 * e, 1)] for e in range(4)]
        else:
            corners = [col_tx.at[k, e % 2, pl.ds(0 if e < 2 else q - 1, 1)] for e in range(4)]
        plan = [
            (corners[0], cor_rx.at[k, 3], (up, left)),
            (corners[1], cor_rx.at[k, 2], (up, right)),
            (corners[2], cor_rx.at[k, 1], (down, left)),
            (corners[3], cor_rx.at[k, 0], (down, right)),
            (row_tx.at[k, 0], row_rx.at[k, 1], (up, me_s)),
            (row_tx.at[k, 1], row_rx.at[k, 0], (down, me_s)),
            (col_tx.at[k, 0], col_rx.at[k, 1], (me_c, left)),
            (col_tx.at[k, 1], col_rx.at[k, 0], (me_c, right)),
        ]
        return [
            pltpu.make_async_remote_copy(
                src_ref=src, dst_ref=dst, send_sem=htx_sem.at[k],
                recv_sem=crx_sem.at[k] if k < groups and e < 4 else hrx_sem.at[k],
                device_id=where, device_id_type=MESH)
            for e, (src, dst, where) in enumerate(plan)
        ]

    def send(k, tops):
        col_tx[k, 0], col_tx[k, 1] = tops
        for copy in halo_copies(k)[4 if early(k) else 0:]:
            copy.start()

    def arrive(k):
        if k < groups:
            landed(gauge.at[pl.ds(0, 4)], crx_sem.at[k])
        else:
            landed(gauge, hrx_sem.at[k])
        ph = lax.broadcasted_iota(jnp.int32, (1, LANES), 1) % 4
        edge_row = lax.broadcasted_iota(jnp.int32, (q, LANES), 0)
        merged = []
        for side in range(2):
            above, below = cor_rx[k, side], cor_rx[k, 2 + side]
            above = jnp.where(ph == 0, pltpu.roll(above, LANES - 3, 1), 0.0)
            below = jnp.where(ph == 3, pltpu.roll(below, 3, 1), 0.0)
            c = col_rx[k, side]
            c = c + jnp.where(edge_row == 0, above, 0.0) + jnp.where(edge_row == q - 1, below, 0.0)
            merged.append(c)
        return merged

    few_rows = lax.broadcasted_iota(jnp.int32, (8, cols), 0)
    few_at = lax.broadcasted_iota(jnp.int32, (8, cols), 1)
    few_lane = lax.broadcasted_iota(jnp.int32, (8, LANES), 1)
    few_next = (few_at % 4 == 3) & (few_at != cols - 1)
    few_prev = (few_at % 4 == 0) & (few_at != 0)
    few_edge = (few_at % 4 == 3) | (few_at % 4 == 0)
    chunks = q // 8

    def chunk(ref, m, n):
        return [ref[m, p * q + 8 * n:p * q + 8 * n + 8, :] for p in range(4)]

    def chunk2(ref, n):
        return [ref[p * q + 8 * n:p * q + 8 * n + 8, :] for p in range(4)]

    def keep(ref, m, n, parts):
        for p in range(4):
            ref[m, p * q + 8 * n:p * q + 8 * n + 8, :] = parts[p]

    def joined(k, m, slot, merged, n):
        t = chunk(w, m, n)
        if n == 0:
            t[0] = t[0] + jnp.where(few_rows == 0, row_rx[k, 0, pl.ds(slot, 1), :], 0.0)
        if n == chunks - 1:
            t[3] = t[3] + jnp.where(few_rows == 7, row_rx[k, 1, pl.ds(slot, 1), :], 0.0)
        near_side, far_side = [v[8 * n:8 * n + 8] for v in merged]
        out = []
        for p in range(4):
            at = 4 * slot + p
            c = t[p] + jnp.where(
                few_next, pltpu.roll(t[p], cols - 1, 1),
                jnp.where(few_prev, pltpu.roll(t[p], 1, 1), 0.0))
            a = jnp.where(few_lane == 0, pltpu.roll(near_side, LANES - at, 1), 0.0)
            b = jnp.where(few_lane == LANES - 1, pltpu.roll(far_side, LANES - 1 - at, 1), 0.0)
            pieces = [c[:, e * LANES:(e + 1) * LANES] for e in range(tiles)]
            pieces[0] = pieces[0] + a
            pieces[-1] = pieces[-1] + b
            out.append(jnp.concatenate(pieces, axis=1))
        return out

    edge_w, mid_w = f32(1.0 / 6.0), f32(5.0 / 6.0)
    col_w = jnp.where(on_edge, edge_w, mid_w)
    mw, fw = [], []
    landed(factors, in_sem.at[0])
    for p in range(4):
        grid_w = col_w * (edge_w if p in (0, 3) else mid_w)
        mw.append(strided([factors.at[0, c] for c in range(tiles)], p, q) * grid_w)
        fw.append(strided([factors.at[1, c] for c in range(tiles)], p, q) * grid_w)
        mass[p * q:(p + 1) * q, :] = mw[p]
        flux[p * q:(p + 1) * q, :] = fw[p]
    zero = jnp.zeros((q, LANES), f32)
    tops = pack(0, modes, per, mw, (zero, zero))
    div_load.wait()
    table = div_ref[:cols, :].astype(f32) + div_ref[2 * cols:, :].astype(f32)
    by_cols = jnp.dot(flux[...], table * table, precision=lax.Precision.HIGHEST,
                      preferred_element_type=f32)
    squared = SLOPES * SLOPES
    lap = [combo(squared[:, a], fw) + by_cols[a * q:(a + 1) * q, :] for a in range(4)]
    tops = pack(0, modes + 1, per + 1, lap, tops)
    landed(source, in_sem.at[1])
    for g in range(groups):

        def start_body(slot, carry, g=g):
            m = g * per + slot
            h = [strided([source.at[c, m] for c in range(tiles)], p, q)
                 * mass[p * q:(p + 1) * q, :] for p in range(4)]
            return pack(g, m, slot, h, carry)

        tops = lax.fori_loop(0, per, start_body, tops if g == 0 else (zero, zero), unroll=UNROLL)
        if g == 0:
            pl.semaphore_wait(barrier, len(greeted))
        send(g, tops)
    scale_load.wait()
    grad_load.wait()

    at_lane = lax.broadcasted_iota(jnp.int32, (1, LANES), 1)
    of_four = at_lane % 4
    tall = lax.broadcasted_iota(jnp.int32, (slots, LANES), 0)
    flat = lax.broadcasted_iota(jnp.int32, (slots, LANES), 1)
    low_half = tall < 4

    def coefs(values):
        line = jnp.zeros((1, LANES), f32)
        for e, value in enumerate(values):
            line = jnp.where(of_four == e, f32(value), line)
        return line

    def corner_weights(g):
        scale = jnp.zeros((1, LANES), f32)
        for slot in range(per):
            scale = jnp.where(at_lane // 4 == slot, scale_ref[g * per + slot], scale)
        lines = []
        for tb in range(2):
            er, cr = (0, 0) if tb == 0 else (q - 1, 3)
            for side in range(2):
                cc, edge, start = (0, 0, 0) if side == 0 else (3, cols - 1, cols - 4)
                sx = jnp.zeros((1, LANES), f32)
                sy = jnp.zeros((1, LANES), f32)
                own = jnp.zeros((1, 1), f32)
                for e in range(4):
                    fx = flux[e * q + er:e * q + er + 1, edge:edge + 1]
                    fy = flux[cr * q + er:cr * q + er + 1, start + e:start + e + 1]
                    sx = sx + fx * coefs(SLOPES[e, cr] * SLOPES[e])
                    sy = sy + fy * coefs(SLOPES[e, cc] * SLOPES[e])
                    own = own + fy * f32(SLOPES[e, cc] * SLOPES[e, cc])
                here = mass[cr * q + er:cr * q + er + 1, edge:edge + 1]
                lines += [
                    scale * sx + jnp.where(of_four == cr, here + scale * own, 0.0),
                    jnp.where(of_four == cc, 0.0, scale * sy)]
        return scale, jnp.concatenate(lines, axis=0)

    def gathered_rows(x):
        left = x[:, :LANES]
        left = left + jnp.where(flat == 3, pltpu.roll(left, LANES - 1, 1), 0.0)
        right = x[:, half:]
        right = right + jnp.where(flat == LANES - 4, pltpu.roll(right, 1, 1), 0.0)
        left = pltpu.roll(jnp.where(flat < 4, left, 0.0), 0, 1, stride=4, stride_axis=0)
        right = pltpu.roll(
            jnp.where(flat >= LANES - 4, right, 0.0), 4, 1, stride=4, stride_axis=0)
        return [jnp.sum(v, axis=0, keepdims=True) for v in (left, right)]

    def corner_values(k, merged):
        lines = []
        for tb in range(2):
            er, cr = (0, 0) if tb == 0 else (q - 1, 3)
            halo = row_rx[k, tb]
            rows_here = gathered_rows(row_tx[k, tb] + halo)
            for side in range(2):
                edge = 0 if side == 0 else cols - 1
                place = flat == 4 * tall + cr
                extra = jnp.sum(
                    jnp.where(place, halo[:, edge:edge + 1], 0.0), axis=0, keepdims=True)
                col = col_tx[k, side, er:er + 1, :] + merged[side][er:er + 1, :] + extra
                lines += [col, rows_here[side]]
        return jnp.concatenate(lines, axis=0)

    def set_corners(k, weights, v):
        h = weights * v
        fore = h + pltpu.roll(h, LANES - 1, 1)
        fore = fore + pltpu.roll(fore, LANES - 2, 1)
        back = h + pltpu.roll(h, 1, 1)
        back = back + pltpu.roll(back, 2, 1)
        h = jnp.where(low_half, fore, back)
        cor_tx[k] = h + pltpu.roll(h, slots - 1, 0)

    def repeat(x, slot):
        x = jnp.where(flat // 4 == slot, x, 0.0)
        x = pltpu.roll(x, LANES - 4 * slot, 1)
        for step in (4, 8, 16):
            x = x + pltpu.roll(x, step, 1)
        return x

    assert slots == 8
    corner = [corner_weights(g) for g in range(groups)]
    corner_r, corner_inv, shared_diag = [None] * groups, [None] * groups, []

    def corner_step(it, g, k, merged):
        u = corner_values(k, merged)
        scale, weights = corner[g]
        if it == 0:
            if g == 0:
                shared_diag.extend([repeat(u, per), repeat(u, per + 1)])
            used = flat < 4 * per
            u = jnp.where(used, u, 0.0)
            corner_r[g] = u
            corner_inv[g] = jnp.where(used, 1.0 / jnp.where(
                used, shared_diag[0] + scale * shared_diag[1], 1.0), 0.0)
            r = u
        else:
            r = jnp.where(flat < 4 * per, u, 0.0) - corner_r[g]
        set_corners(k + groups, weights, r * corner_inv[g])

    def fill(g, slot, n, parts):
        v = jnp.concatenate(parts, axis=0)
        top = v.astype(bf16)
        at = pl.ds(pl.multiple_of(slot * rows + 32 * n, 32), 32)
        zcat[g, at, :cols] = top
        zcat[g, at, cols:] = (v - top.astype(f32)).astype(bf16)

    def taken(slot, n):
        return [gout[pl.ds(pl.multiple_of(slot * rows + 32 * n + 8 * p, 8), 8), :]
                for p in range(4)]

    def multiply(g, table_ref, part):
        lo, hi = part[0] * rows, part[1] * rows
        gout[lo:hi] = (
            jnp.dot(zcat[g, lo:hi, :], table_ref[:2 * cols, :], preferred_element_type=f32)
            + jnp.dot(zcat[g, lo:hi, :cols], table_ref[2 * cols:, :],
                      preferred_element_type=f32))

    third_of = per // 3
    parts_of = [(0, third_of), (third_of, 2 * third_of), (2 * third_of, per)]

    def over(part, body, carry=0):
        return lax.fori_loop(part[0], part[1], body, carry, unroll=UNROLL)

    def total(parts):
        return (parts[0] + parts[3]) + (parts[1] + parts[2])

    def shared(parts):
        return (parts[0] + parts[3]) * 0.5 + (parts[1] + parts[2])

    def put(e, m, line):
        sums[e, pl.ds(m, 1), :] = jnp.sum(line, axis=0, keepdims=True)

    def finish(g, k, base):
        def third(slot, carry):
            m = base + slot
            h, line = [], 0.0
            for n in range(chunks):
                zz = chunk(z, m, n)
                part = [t * u + scale_ref[m] * (v + s) for t, u, v, s in zip(
                    chunk2(mass, n), zz, chunk(w, m, n), taken(slot, n))]
                if k < ITERS - 1:
                    line = line + total([u * v for u, v in zip(zz, part)])
                h.append(part)
            if k < ITERS - 1:
                put(2 * k + 1, m, line)
            h = [jnp.concatenate([part[p] for part in h], axis=0) for p in range(4)]
            return pack((k + 1) * groups + g, m, slot, h, carry)

        return third

    def patched(k, slot, n, parts):
        parts = list(parts)
        for at_n, p, row, lines, at in (
                (0, 0, 0, (0, 1), 4 * slot + 3), (chunks - 1, 3, 7, (2, 3), 4 * slot)):
            if n != at_n:
                continue
            a = pltpu.roll(cor_rx[k, lines[0]], LANES - at, 1)
            b = pltpu.roll(cor_rx[k, lines[1]], LANES - 1 - at, 1)
            here = few_rows[:, :LANES] == row
            pieces = [parts[p][:, e * LANES:(e + 1) * LANES] for e in range(tiles)]
            pieces[0] = pieces[0] + jnp.where(here & (few_lane == 0), a, 0.0)
            pieces[-1] = pieces[-1] + jnp.where(here & (few_lane == LANES - 1), b, 0.0)
            parts[p] = jnp.concatenate(pieces, axis=1)
        return parts

    for g in range(groups):
        landed(gauge.at[pl.ds(0, gauge.shape[0] - 4)], hrx_sem.at[g])
        sides = [col_rx[g, 0], col_rx[g, 1]]
        pairs = [(modes, per), (modes + 1, per + 1)] if g == 0 else []
        for m, slot in pairs + [(g * per + e, e) for e in range(per)]:
            for n in range(chunks):
                keep(w, m, n, joined(g, m, slot, sides, n))

    for it in range(ITERS):
        for g in range(groups):
            base = g * per
            k = it * groups + g
            merged = arrive(k)
            if it < ITERS - 1:
                corner_step(it, g, k, merged)
            if it == 0 and g == 0:
                for e in range(2):
                    for n in (0, chunks - 1):
                        keep(w, modes + e, n, patched(k, per + e, n, chunk(w, modes + e, n)))

            def first(slot, carry, it=it, g=g, k=k, base=base, merged=merged):
                m = base + slot
                line, energy = 0.0, 0.0
                for n in range(chunks):
                    if it == 0:
                        uu = patched(k, slot, n, chunk(w, m, n))
                    else:
                        uu = joined(k, m, slot, merged, n)
                    if it == 0:
                        rr = uu
                        inv = [1.0 / (u + scale_ref[m] * v)
                               for u, v in zip(chunk(w, modes, n), chunk(w, modes + 1, n))]
                        keep(invp, m, n, inv)
                    elif it == 1:
                        rr = [u - v for u, v in zip(uu, chunk(r0, m, n))]
                        inv = chunk(invp, m, n)
                    else:
                        rr = [2.0 * (u - v) - s for u, v, s in zip(
                            uu, chunk(r1, m, n), chunk(r0, m, n))]
                        inv = chunk(invp, m, n)
                    keep((r0, r1, r2)[it], m, n, rr)
                    zz = [u * v for u, v in zip(rr, inv)]
                    keep(z, m, n, zz)
                    fill(g, slot, n, zz)
                    line = line + shared([u * v for u, v in zip(uu, zz)])
                    gx = slope(zz)
                    fg = [u * v for u, v in zip(chunk2(flux, n), gx)]
                    keep(w, m, n, fall(fg))
                    if it == ITERS - 1:
                        energy = energy + (
                            total([t * u * u for t, u in zip(chunk2(mass, n), zz)])
                            + scale_ref[m] * total([u * v for u, v in zip(fg, gx)]))
                put(2 * it, m, jnp.where(few_edge, line * 0.5, line))
                if it == ITERS - 1:
                    put(2 * it + 1, m, energy)
                return carry

            if it < ITERS - 1:
                for copy in halo_copies(k + groups)[:4]:
                    copy.start()
            def second(slot, carry, it=it, g=g, base=base):
                m, e, line = base + slot, 2 * it + 1, 0.0
                for n in range(chunks):
                    grad = taken(slot, n)
                    fy = [u * v for u, v in zip(chunk2(flux, n), grad)]
                    if it == ITERS - 1:
                        line = line + total([u * v for u, v in zip(fy, grad)])
                    fill(g, slot, n, fy)
                if it == ITERS - 1:
                    sums[e, pl.ds(m, 1), :] = sums[e, pl.ds(m, 1), :] + scale_ref[m] * jnp.sum(
                        line, axis=0, keepdims=True)
                return carry

            one, two, three = parts_of
            over(one, first)
            multiply(g, grad_ref, one)
            over(two, first)
            over(one, second)
            multiply(g, grad_ref, two)
            over(three, first)
            over(two, second)
            multiply(g, grad_ref, three)
            if it < ITERS - 1:
                third = finish(g, it, base)
                multiply(g, div_ref, one)
                over(three, second)
                tops = over(one, third, (zero, zero))
                multiply(g, div_ref, two)
                tops = over(two, third, tops)
                multiply(g, div_ref, three)
                send(k + groups, over(three, third, tops))
            else:
                over(three, second)

    high = lax.broadcasted_iota(jnp.int32, (FIELD, LANES), 0)
    wide = lax.broadcasted_iota(jnp.int32, (FIELD, LANES), 1)
    picks = [(wide == e * FIELD + high) & (high < modes) for e in range(PRODUCTS)]
    spread = jnp.zeros((FIELD, LANES), f32)
    for e in range(PRODUCTS):
        part = jnp.sum(sums[e], axis=1, keepdims=True)
        spread = spread + jnp.where(picks[e], part, 0.0)
    line = jnp.sum(spread, axis=0, keepdims=True)

    def share(stage, line, tx, rx, peers):
        tx[...] = line
        rx[0] = line
        for j, where in enumerate(peers):
            pltpu.make_async_remote_copy(
                src_ref=tx, dst_ref=rx.at[j + 1], send_sem=atx_sem.at[stage],
                recv_sem=arx_sem.at[stage], device_id=where, device_id_type=MESH).start()

    def gather(stage, rx):
        landed(rx.at[pl.ds(1, rx.shape[0] - 1)], arx_sem.at[stage])
        return jnp.sum(rx[...], axis=0)

    share(0, line, near_tx, near_rx, near)
    for g in range(groups):
        third = finish(g, ITERS - 1, g * per)
        multiply(g, div_ref, (0, per))
        send(ITERS * groups + g, over((0, per), third, (zero, zero)))
    share(1, gather(0, near_rx), far_tx, far_rx, far)
    for g in range(groups):
        k = ITERS * groups + g
        merged = arrive(k)

        def last(slot, carry, g=g, k=k, merged=merged):
            m = g * per + slot
            for n in range(chunks):
                keep(u2, m, n, joined(k, m, slot, merged, n))
            return carry

        lax.fori_loop(0, per, last, 0, unroll=UNROLL)

    total = gather(1, far_rx)
    pad = (high[:, :1] >= modes).astype(f32)
    n0, p00, p01, p11, p12, p22 = [
        jnp.broadcast_to(
            jnp.sum(jnp.where(pick, total, 0.0), axis=1, keepdims=True), (FIELD, LANES))
        for pick in picks]
    pad = jnp.broadcast_to(pad, (FIELD, LANES))
    p00, p11, p22 = p00 + pad, p11 + pad, p22 + 2.0 * pad
    b0 = n0
    b1 = p00 - n0
    b2 = 2.0 * (p01 - b1) - n0
    p02 = 2.0 * p11 - p00
    i0 = 1.0 / p00
    l1, l2 = p01 * i0, p02 * i0
    d1 = p11 - l1 * p01
    t2 = p12 - l2 * p01
    i1 = 1.0 / d1
    l3 = t2 * i1
    d2 = p22 - l2 * p02 - l3 * t2
    y1 = b1 - l1 * b0
    y2 = b2 - l2 * b0 - l3 * y1
    c2 = y2 / d2
    c1 = y1 * i1 - l3 * c2
    c0 = b0 * i0 - l1 * c1 - l2 * c2
    for e, c in enumerate((c0, c1, c2, 1.0 - c0 - 0.5 * c1, c0 + c1, 0.5 * c1)):
        coef[e] = c

    for k in range((ITERS + 1) * groups):
        landed(gauge, htx_sem.at[k])
    for stage, rx in enumerate((near_rx, far_rx)):
        landed(rx.at[pl.ds(1, rx.shape[0] - 1)], atx_sem.at[stage])


def node_order(r0, r1, r2, u2, invp, coef, sol_ref, res_ref, sol_buf, res_buf, sem):
    modes, rows, cols = r0.shape
    q, tiles = rows // 4, cols // LANES

    def stores(m):
        return [
            pltpu.make_async_copy(
                buf.at[c, m], out.at[m, :, pl.ds(c * LANES, LANES)], sem.at[k, c, m])
            for k, (buf, out) in enumerate(((sol_buf, sol_ref), (res_buf, res_ref)))
            for c in range(tiles)
        ]

    def body(m, carry):
        c0, c1, c2, e0, e1, e2 = [coef[e, pl.ds(m, 1), :] for e in range(6)]
        for c in range(tiles):
            for p in range(4):
                at = (m, slice(p * q, (p + 1) * q), slice(c * LANES, (c + 1) * LANES))
                a0, a1, a2 = r0[at], r1[at], r2[at]
                sol_buf[c, m, pl.ds(p, q, stride=4), :] = invp[at] * (c0 * a0 + c1 * a1 + c2 * a2)
                res_buf[c, m, pl.ds(p, q, stride=4), :] = (
                    e0 * a0 - e1 * a1 - e2 * a2 - c2 * u2[at])
        for copy in stores(m):
            copy.start()
        return carry

    lax.fori_loop(0, modes, body, 0)

    def drain(m, carry):
        for copy in stores(m):
            copy.wait()
        return carry

    lax.fori_loop(0, modes, drain, 0)


def strided(refs, p, q):
    return jnp.concatenate([ref[pl.ds(p, q, stride=4), :] for ref in refs], axis=1)


def stack_table(table):
    top = table.astype(bf16)
    low = (table - top.astype(np.float32)).astype(bf16)
    return np.concatenate([top, top, low], axis=0)


def shards(nc, ns, forcing, metric, jacobian, mode_scale):
    modes, rows, cols = forcing.shape
    block = np.kron(np.eye(cols // 4), SLOPES).astype(np.float32)
    grad, div = stack_table(block.T), stack_table(block)
    q, tiles = rows // 4, cols // LANES
    groups = GROUPS if modes % GROUPS == 0 else 1
    per = modes // groups
    slots = -(-(per + 2) // 8) * 8
    vm = pl.BlockSpec(memory_space=pltpu.VMEM)
    hbm = pl.BlockSpec(memory_space=pltpu.HBM)
    rounds = (ITERS + 1) * groups
    ny, nz, nk, nx = planes(nc, ns)
    field = pltpu.VMEM((modes, rows, cols), f32)
    split = pltpu.VMEM((tiles, modes, rows, LANES), f32)
    table = pltpu.VMEM(grad.shape, bf16)
    line = pltpu.VMEM((1, LANES), f32)
    shape = jax.ShapeDtypeStruct(forcing.shape, f32)
    kept = pl.pallas_call(
        functools.partial(kernel, nc, ns, modes, groups),
        out_shape=[shape] * 5 + [jax.ShapeDtypeStruct((6, FIELD, LANES), f32)],
        in_specs=[hbm] * 6,
        out_specs=[vm] * 6,
        scratch_shapes=[
            field,
            pltpu.VMEM((modes + 2, rows, cols), f32),
            pltpu.VMEM((rows, cols), f32),
            pltpu.VMEM((rows, cols), f32),
            pltpu.VMEM((groups, per * rows, 2 * cols), bf16),
            pltpu.VMEM((per * rows, cols), f32),
            pltpu.VMEM((PRODUCTS, FIELD, cols), f32),
            pltpu.VMEM((rounds, 2, slots, cols), f32),
            pltpu.VMEM((rounds, 2, slots, cols), f32),
            pltpu.VMEM((rounds, 2, q, LANES), f32),
            pltpu.VMEM((rounds, 2, q, LANES), f32),
            pltpu.VMEM((rounds, 8, LANES), f32),
            pltpu.VMEM((rounds, 4, 1, LANES), f32),
            line,
            pltpu.VMEM((ny * nk * nx, 1, LANES), f32),
            line,
            pltpu.VMEM((nz, 1, LANES), f32),
            split,
            pltpu.VMEM((2, tiles, rows, LANES), f32),
            pltpu.VMEM((4 + 2 * slots * tiles + 2 * q, LANES), f32),
            table, table,
            pltpu.SMEM((modes,), f32),
            pltpu.SemaphoreType.DMA((rounds,)),
            pltpu.SemaphoreType.DMA((rounds,)),
            pltpu.SemaphoreType.DMA((groups,)),
            pltpu.SemaphoreType.DMA((2,)),
            pltpu.SemaphoreType.DMA((2,)),
            pltpu.SemaphoreType.DMA((2,)),
            pltpu.SemaphoreType.DMA((3,)),
        ],
        compiler_params=pltpu.CompilerParams(
            collective_id=0, has_side_effects=True, vmem_limit_bytes=41943040),
    )(*[pltpu.with_memory_space_constraint(v, pltpu.HBM) for v in (mode_scale, forcing, metric, jacobian, jnp.asarray(grad), jnp.asarray(div))])
    return pl.pallas_call(
        node_order,
        out_shape=[shape] * 2,
        in_specs=[vm] * 6,
        out_specs=[hbm, hbm],
        scratch_shapes=[split, split, pltpu.SemaphoreType.DMA((2, tiles, modes))],
        compiler_params=pltpu.CompilerParams(vmem_limit_bytes=16 * 1024 * 1024),
    )(*kept)


def solution(mesh):
    placed = (P(None, "curve", "sub"), P("curve", "sub"), P("curve", "sub"), P())
    return jax.shard_map(
        functools.partial(shards, mesh.shape["curve"], mesh.shape["sub"]),
        mesh=mesh,
        in_specs=placed,
        out_specs=(P(None, "curve", "sub"), P(None, "curve", "sub")),
        check_vma=False,
    )
```
